32 devices in a mesh: lat: 4 (over y, x), lon: 8 (over z, core).
Axes of the slice: x: 2, y: 2, z: 4, core: 2. Of those that a mesh axis runs over, the one named last changes fastest.
Arguments:
- adjoint_in: bfloat16 [8, 100, 8, 1024], P(None, None, 'lat', 'lon'), may hold values from -6 to 6
- state: bfloat16 [2, 8, 100, 8, 1024], P(None, None, None, 'lat', 'lon'), may hold values from 0.29882812 to 1
- inverses: bfloat16 [3, 8, 100, 100], replicated
- courant_lon: float32 [8, 1024], P('lat', 'lon'), may hold values from 0.1 to 0.4
- courant_lat: float32 [8, 1024], P('lat', 'lon'), may hold values from 0.1 to 0.4
- emission: float32 [100, 8, 1024], P(None, 'lat', 'lon'), may hold values from 0.02 to 0.2
- region_id: int32 [8, 1024], P('lat', 'lon'), may hold values from 0 to 31, as said below
- stiffness: int32 [8, 8, 1024], P(None, 'lat', 'lon'), may hold values from 1 to 3
Outputs:
- adjoint_out: bfloat16 [8, 100, 8, 1024], P(None, None, 'lat', 'lon')
- emission_grad: float32 [32, 100], P(('lat', 'lon'))
The draws below stay inside these ranges and needn't reach their ends.
Inputs may be any that keep to these rules, and one draw needn't show every extreme that they name: `region_id`: constant on aligned tiles of 2 x 2 columns.
All inputs are finite; a program needn't handle non-finite values.
Results may differ from the reference program's by a relative error of at most 0.0048.
Values sent between devices are 32-bit elements; how exact they have to be, the bound alone decides.
A program may use at most 64 MiB of HBM per device.

```python
import math
import jax
import jax.numpy as jnp
from jax import lax

SPEC = 100
LEV = 8
STEPS = 3
NWIN = 2
ADV = 2
CLAT = 2
CLON = 128
NLAT = 8
NLON = 1024
REGIONS = 32


def draw_inverses(key, part):
    key_diag = jax.random.fold_in(key, 11)
    key_off = jax.random.fold_in(key, 12)
    diag = jax.random.uniform(key_diag, (STEPS, LEV, SPEC), jnp.float32, 0.7, 1.2)
    off = jax.random.normal(key_off, (STEPS, LEV, SPEC, SPEC), jnp.float32) * 0.4 * SPEC ** (-0.5)
    eye = jnp.eye(SPEC, dtype=jnp.float32)
    return (off * (1.0 - eye) + diag[..., None] * eye).astype(jnp.bfloat16)


def draw_region_id(key, part):
    tiles = jax.random.randint(jax.random.fold_in(key, 21), (NLAT // 2, NLON // 2), 0, REGIONS)
    return jnp.repeat(jnp.repeat(tiles, 2, axis=0), 2, axis=1).astype(jnp.int32)


def draw_stiffness(key, part):
    tile_cols = CLON // 2
    caps = jax.random.randint(jax.random.fold_in(key, 31), (NLAT // CLAT, NLON // tile_cols), 1, STEPS + 1)
    caps = jnp.repeat(jnp.repeat(caps, CLAT, axis=0), tile_cols, axis=1)
    extra = jax.random.randint(jax.random.fold_in(key, 32), (LEV, NLAT, NLON), 0, STEPS)
    return (1 + extra % caps[None, :, :]).astype(jnp.int32)


def levels(own_key, dims, cuts, least, high):
    loudness = 1.0
    for position, blocks in cuts:
        heights = jax.random.uniform(jax.random.fold_in(jax.random.fold_in(own_key, 6), position), (blocks,), jnp.float32, least / len(cuts), high / len(cuts))
        loudness = loudness * jnp.repeat(jnp.exp(heights), dims[position] // blocks).reshape((-1,) + (1,) * (len(dims) - 1 - position))
    return loudness


def bell_draw(stream_key, shape, scale, reach, shards=(), held_as=jnp.bfloat16):
    level = levels(stream_key, shape, shards, -0.22, 0.18) if shards else 1.0
    values = jax.random.normal(stream_key, shape, jnp.float32) * scale * level
    return jnp.minimum(jnp.maximum(values, -reach), reach).astype(held_as)


def setup_inputs(seed: int = 0) -> dict:
    seeds = jax.random.split(jax.random.key(seed), 9)
    adjoint_in = bell_draw(seeds[0], (LEV, SPEC, NLAT, NLON), 1.0, 6.0, ((2, 4), (3, 8)))
    state = jnp.clip(jnp.exp(math.log(1.0) - 1.2078867 * jax.random.uniform(seeds[1], (NWIN, LEV, SPEC, NLAT, NLON), jnp.float32) ** levels(seeds[1], (NWIN, LEV, SPEC, NLAT, NLON), ((3, 4), (4, 8)), -0.2, 0.2)), 0.29882812, 1.0).astype(jnp.bfloat16)
    inverses = draw_inverses(jax.random.fold_in(seeds[8], 71), 0)
    courant_lon = jnp.clip(0.1 + 0.3 * jax.random.uniform(seeds[3], (NLAT, NLON), jnp.float32) ** levels(seeds[3], (NLAT, NLON), ((0, 4), (1, 8)), -0.2, 0.2), 0.1, 0.4)
    courant_lat = jnp.clip(0.1 + 0.3 * jax.random.uniform(seeds[4], (NLAT, NLON), jnp.float32) ** levels(seeds[4], (NLAT, NLON), ((0, 4), (1, 8)), -0.2, 0.2), 0.1, 0.4)
    emission = jnp.clip(jnp.exp(math.log(0.2) - 2.3025851 * jax.random.uniform(seeds[5], (SPEC, NLAT, NLON), jnp.float32) ** levels(seeds[5], (SPEC, NLAT, NLON), ((1, 4), (2, 8)), -0.2, 0.2)), 0.02, 0.2)
    region_id = draw_region_id(jax.random.fold_in(seeds[8], 71), 0)
    stiffness = draw_stiffness(jax.random.fold_in(seeds[8], 71), 0)
    return {"adjoint_in": adjoint_in, "state": state, "inverses": inverses, "courant_lon": courant_lon, "courant_lat": courant_lat, "emission": emission, "region_id": region_id, "stiffness": stiffness}


def transport(lam, clon, clat):
    right = jnp.roll(lam, -1, axis=2)
    down = jnp.concatenate([lam[:, 1:, :], jnp.zeros_like(lam[:, :1, :])], axis=1)
    return (1.0 - clon - clat) * lam + clat * down + clon * right


def chem_level(lam, factor, mats, klass):
    spec = lam.shape[0]
    flat = lam.reshape(spec, -1)
    yfac = factor.reshape(spec, -1).astype(jnp.float32)
    live = klass.reshape(1, -1)
    for s in reversed(range(STEPS)):
        amat = mats[s].T
        first = jnp.dot(amat, flat.astype(jnp.bfloat16), preferred_element_type=jnp.float32)
        second = jnp.dot(amat, (first * yfac).astype(jnp.bfloat16), preferred_element_type=jnp.float32)
        third = jnp.dot(amat, (second * yfac).astype(jnp.bfloat16), preferred_element_type=jnp.float32)
        cand = 0.4 * flat + 0.3 * first + 0.2 * second + 0.1 * third
        flat = jnp.where(live > s, cand, flat)
    return flat.reshape(lam.shape)


def reference(adjoint_in, state, inverses, courant_lon, courant_lat, emission, region_id, stiffness):
    lam = adjoint_in.astype(jnp.float32)
    surface = jnp.zeros(emission.shape, jnp.float32)
    mats_by_level = jnp.transpose(inverses, (1, 0, 2, 3))
    for window in reversed(range(NWIN)):
        def level_work(items):
            lam_l, factor_l, mats_l, klass_l = items
            for k in range(ADV):
                lam_l = transport(lam_l, courant_lon, courant_lat)
            return chem_level(lam_l, factor_l, mats_l, klass_l)

        lam = lax.map(level_work, (lam, state[window], mats_by_level, stiffness))
        surface = surface + lam[0]
    contrib = (surface * emission).reshape(emission.shape[0], -1).T
    grad = jax.ops.segment_sum(contrib, region_id.reshape(-1), num_segments=REGIONS)
    return lam.astype(jnp.bfloat16), grad.astype(jnp.float32)
```

```python
import functools

import jax
import jax.numpy as jnp
from jax import lax
from jax.experimental import pallas as pl
from jax.experimental.pallas import tpu as pltpu
from jax.sharding import PartitionSpec as P

MESH = pl.DeviceIdType.MESH
LP = 2

OWN1, OWN0, GHOST, FIRST = 0, 1, 2, 3


def orders(per):
    half = per // 2
    first = [(FIRST, g) for g in range(per)]
    last = [(OWN0, g) for g in range(per)]
    even = []
    for g in range(half):
        even += [(OWN1, half + g), (OWN1, g)]
    odd = [(OWN1, 0), (GHOST, half)] + [(OWN1, g) for g in range(1, half)]
    for g in range(half, per):
        odd += ([(GHOST, g)] if g > half else []) + [(OWN1, g)]
    return first + even + last, first + odd + last


def relays(even, per):
    plan = {}
    passed = [g for g in range(per) if g % 2]
    at = [even.index((OWN1, g)) for g in range(len(passed))]
    for n, g in enumerate(passed):
        plan.setdefault(at[n], []).append((0, g))
    at = [even.index((OWN0, g * 2)) for g in range(len(passed))]
    for n, g in enumerate(reversed(passed)):
        plan.setdefault(at[n], []).append((1, g))
    return plan


def kernel(
    n_lat, n_lon,
    adj_hbm, state_hbm, inv_hbm, clon_hbm, clat_hbm, em_hbm, reg_hbm, stiff_hbm,
    outbuf, grad_ref,
    adj, state, inv, clon_ref, clat_ref, em_ref, reg_ref, stiff_ref, tall, mats,
    lamb, pbuf, vout, vin, relay, zin, st_out, st_in, cout, cin, nclon, nclat, neclat, gstiff,
    xbuf, ybuf, lbuf, tmp, fin, coef, part, inbox1, turn, inbox2,
    adj_sem, state_sem, inv_sem, small_sem, vs, vr, rr, fs, zr, ss, sr, cs, cr, ks, kr, s1, r1, s2, r2,
):
    lev, rows2, cols = adj.shape
    nwin = state.shape[0]
    steps = inv.shape[0]
    spec = rows2 // 2
    per = lev // LP
    half = per // 2
    units = nwin * per
    lat, lon = lax.axis_index("lat"), lax.axis_index("lon")
    odd = lax.rem(lat, 2) == 1
    even = lax.rem(lat, 2) == 0
    north = jnp.maximum(lat - 1, 0)
    north2 = jnp.maximum(lat - 2, 0)
    south = jnp.minimum(lat + 1, n_lat - 1)
    west = lax.rem(lon + n_lon - 1, n_lon)
    east = lax.rem(lon + 1, n_lon)
    has_north = lat > 0
    has_south = lat < n_lat - 1
    even_order, odd_order = orders(per)
    relay_plan = relays(even_order, per)

    barrier = pltpu.get_barrier_semaphore()

    def greet(to):
        pl.semaphore_signal(barrier, inc=1, device_id=to, device_id_type=MESH)

    for k in range(1, n_lon):
        greet((lat, lax.rem(lon + k, n_lon)))
    for k in range(1, n_lat):
        greet((lax.rem(lat + k, n_lat), lon))

    @pl.when(has_south)
    def _():
        greet((south, west))

    @pl.when(has_north)
    def _():
        greet((north, east))

    adj_loads = [
        pltpu.make_async_copy(
            adj_hbm.at[pl.ds(u * LP, LP)], adj.at[pl.ds(u * LP, LP)], adj_sem.at[u])
        for u in range(per)
    ]
    small = [
        pltpu.make_async_copy(src, dst, small_sem.at[n])
        for n, (src, dst) in enumerate((
            (clon_hbm, clon_ref), (clat_hbm, clat_ref), (stiff_hbm, stiff_ref),
            (reg_hbm, reg_ref), (em_hbm, em_ref)))
    ]
    state_loads = [
        pltpu.make_async_copy(state_hbm.at[w], state.at[w], state_sem.at[w]) for w in range(nwin)
    ]
    inv_load = pltpu.make_async_copy(inv_hbm, inv, inv_sem)
    for load in small[:2] + adj_loads:
        load.start()
    state_loads[nwin - 1].start()
    inv_load.start()
    for load in small[2:]:
        load.start()
    for w in range(nwin - 1):
        state_loads[w].start()

    lane = lax.broadcasted_iota(jnp.int32, (spec, cols), 1)

    def weights(which, names):
        return [coef[which, k, 0:1, :] for k in names]

    def remote(src, dst, send, recv, to):
        return pltpu.make_async_remote_copy(
            src_ref=src, dst_ref=dst, send_sem=send, recv_sem=recv, device_id=to, device_id_type=MESH)

    def direct(u, p):
        return remote(vout.at[u, p], vin.at[u, p], vs.at[u, p], vr.at[u, p], (north, lon))

    def to_relay(u, p):
        return remote(vout.at[u, p], relay.at[u, p], vs.at[u, p], rr.at[u, p], (north2, lon))

    def forward(u, p):
        return remote(relay.at[u, p], vin.at[u, p], fs.at[u, p], vr.at[u, p], (south, lon))

    def ghost_out(n, p):
        return remote(vout.at[units + n, p], zin.at[n, p], vs.at[units + n, p], zr.at[n, p], (north2, lon))

    def state_out(n, p):
        return remote(st_out.at[n, p], st_in.at[n, p], ss.at[n, p], sr.at[n, p], (south, lon))

    def col_copy(u):
        return remote(cout.at[u], cin.at[u], cs.at[u], cr.at[u], (lat, west))

    rows_out = [
        remote(clon_ref, nclon, ks.at[0], kr.at[0], (south, lon)),
        remote(clat_ref, nclat, ks.at[1], kr.at[1], (south, lon)),
        remote(clat_ref, neclat, ks.at[2], kr.at[2], (south, west)),
    ]
    stiff_out = remote(stiff_ref, gstiff, ks.at[3], kr.at[3], (south, lon))
    mix_out = remote(coef.at[0, pl.ds(5, 4)], coef.at[1, pl.ds(5, 4)], ks.at[4], kr.at[4], (south, lon))

    def after(x):
        return pltpu.roll(x, cols - 1, 1)

    def pack(u, which):
        c0, n0, o0, c1, o1 = weights(which, range(5))
        message = None
        for p in range(LP):
            row0, row1 = lamb[u, p, 0], lamb[u, p, 1]
            new0 = c0 * row0 + n0 * row1 + o0 * after(row0)
            new1 = c1 * row1 + o1 * after(row1)
            for n, x in enumerate((row0, row1, new0, new1)):
                at = 4 * p + n
                message = x if at == 0 else jnp.where(lane == at, pltpu.roll(x, at, 1), message)
        cout[u] = message

    def move(u, which):
        c0, n0, o0, c1, o1, al, be, ga, de = weights(which, range(9))
        for p in range(LP):
            row0, row1, message = lamb[u, p, 0], lamb[u, p, 1], cin[u]

            def shift(x, n):
                edge = message if 4 * p + n == 0 else pltpu.roll(message, cols - 4 * p - n, 1)
                return after(jnp.where(lane == 0, edge, x))

            right0, right1 = shift(row0, 0), shift(row1, 1)
            new0 = c0 * row0 + n0 * row1 + o0 * right0
            new1 = c1 * row1 + o1 * right1
            pbuf[u, p, 0] = c0 * new0 + n0 * new1 + o0 * shift(new0, 2)
            pbuf[u, p, 1] = c1 * new1 + o1 * shift(new1, 3)
            vout[u, p, 0] = al * row0
            vout[u, p, 1] = be * row0 + ga * row1 + de * right0

    def sends_own(u):
        g = lax.rem(u, per)
        plain = jnp.logical_or(u >= per, g < half)
        return (
            jnp.logical_or(jnp.logical_and(odd, plain), jnp.logical_and(jnp.logical_and(even, has_north), lax.rem(g, 2) == 0)),
            jnp.logical_and(jnp.logical_and(even, has_north), lax.rem(g, 2) == 1),
        )

    sends_ghost = jnp.logical_and(odd, lat >= 2)
    passes_on = jnp.logical_and(even, lat + 2 < n_lat)

    def chem(group):
        ys = [ybuf[p] for p in range(LP)]
        flats = [xbuf[p] for p in range(LP)]
        lives = [lbuf[p] for p in range(LP)]
        for s in reversed(range(steps)):
            mat = [mats[s, group * LP + p] for p in range(LP)]
            v1 = [jnp.dot(mat[p], flats[p].astype(jnp.bfloat16), preferred_element_type=jnp.float32) for p in range(LP)]
            v2 = [jnp.dot(mat[p], (v1[p] * ys[p]).astype(jnp.bfloat16), preferred_element_type=jnp.float32) for p in range(LP)]
            v3 = [jnp.dot(mat[p], (v2[p] * ys[p]).astype(jnp.bfloat16), preferred_element_type=jnp.float32) for p in range(LP)]
            flats = [
                jnp.where(lives[p] > s, 0.4 * flats[p] + 0.3 * v1[p] + 0.2 * v2[p] + 0.1 * v3[p], flats[p])
                for p in range(LP)
            ]
        return flats

    def half_of(r):
        return pl.ds(r * cols, cols)

    def spread(k):
        to = lax.rem(lon + k, n_lon)
        return remote(part.at[to], inbox1.at[lon], s1.at[k], r1.at[lon], (lat, to))

    def spread_in(k):
        source = lax.rem(lon + k, n_lon)
        return source, remote(part.at[source], inbox1.at[source], s1.at[k], r1.at[source], (lat, source))

    def spread2(k):
        to = lax.rem(lat + k, n_lat)
        return remote(turn.at[to], inbox2.at[lat], s2.at[k], r2.at[lat], (to, lon))

    def spread2_in(k):
        source = lax.rem(lat + k, n_lat)
        return source, remote(turn.at[source], inbox2.at[source], s2.at[k], r2.at[source], (source, lon))

    def regions():
        lat8 = part.shape[1]
        contrib = jnp.concatenate([
            em_ref[pl.ds(r, spec, stride=2), :]
            * (lamb[units - per, 0, r] + fin[:, r * cols:(r + 1) * cols])
            for r in range(2)], axis=1)
        where_from = jnp.concatenate([reg_ref[0:1, :], reg_ref[1:2, :]], axis=1)
        shape = (n_lon * lat8, 2 * cols)
        column = jnp.concatenate([jnp.full((lat8, 2 * cols), c, jnp.int32) for c in range(n_lon)], axis=0)
        band = lax.broadcasted_iota(jnp.int32, (lat8, 2 * cols), 0)
        band = jnp.concatenate([band] * n_lon, axis=0)
        onehot = (jnp.broadcast_to(where_from, shape) == band * n_lon + column).astype(jnp.float32)
        sums = lax.dot_general(
            onehot, contrib, (((1,), (1,)), ((), ())),
            precision=lax.Precision.HIGHEST, preferred_element_type=jnp.float32)
        for c in range(n_lon):
            part[c] = sums[c * lat8:(c + 1) * lat8]
        for k in range(1, n_lon):
            spread(k).start()

    def regions_turn():
        total = part[lon]
        for k in range(1, n_lon):
            source, copy = spread_in(k)
            copy.wait_recv()
            total = total + inbox1[source]
        for b in range(n_lat):
            turn[b] = total[b:b + 1]
        for k in range(1, n_lat):
            spread2(k).start()

    def regions_end():
        total = turn[lat]
        for k in range(1, n_lat):
            source, copy = spread2_in(k)
            copy.wait_recv()
            total = total + inbox2[source]
        grad_ref[...] = total

    for load in small[:2]:
        load.wait()
    for r in range(2):
        clon, clat = clon_ref[r:r + 1, :], clat_ref[r:r + 1, :]
        coef[0, 3 * r] = jnp.broadcast_to(1.0 - clon - clat, (8, cols))
        if r == 0:
            coef[0, 1] = jnp.broadcast_to(clat, (8, cols))
        coef[0, 2 + 2 * r] = jnp.broadcast_to(clon, (8, cols))

    for load in adj_loads:
        load.wait()

    def take(u, carry):
        for p in range(LP):
            tmp[p] = adj[u * LP + p].astype(jnp.float32)
            for r in range(2):
                lamb[u, p, r] = tmp[p, pl.ds(r, spec, stride=2), :]
        pack(u, 0)
        return carry

    lax.fori_loop(0, per, take, 0)
    state_loads[nwin - 1].wait()

    @pl.when(even)
    def _():
        def widen(n, carry):
            for p in range(LP):
                tmp[p] = state[nwin - 1, (half + n) * LP + p].astype(jnp.float32)
                for r in range(2):
                    st_out[n, p, r] = tmp[p, pl.ds(r, spec, stride=2), :]
            return carry

        lax.fori_loop(0, per - half, widen, 0)

    inv_load.wait()
    for s in range(steps):
        tall[...] = inv[s].astype(jnp.float32)
        for level in range(lev):
            mats[s, level] = tall[pl.ds(level, spec, stride=lev), :].T.astype(jnp.bfloat16)
    for load in small[2:]:
        load.wait()
    for w in range(nwin - 1):
        state_loads[w].wait()

    pl.semaphore_wait(
        barrier, n_lon - 1 + n_lat - 1 + has_north.astype(jnp.int32) + has_south.astype(jnp.int32))

    @pl.when(has_south)
    def _():
        for copy in rows_out:
            copy.start()
    for g in range(per):
        col_copy(g).start()

    @pl.when(even)
    def _():
        stiff_out.start()
        state_out(0, 0).start()

    @pl.when(has_north)
    def _():
        for copy in rows_out:
            copy.wait_recv()
        c0, o0, n0 = coef[0, 0], coef[0, 2], coef[0, 1]
        for r in range(2):
            clon, clat = nclon[r:r + 1, :], nclat[r:r + 1, :]
            coef[1, 3 * r] = jnp.broadcast_to(1.0 - clon - clat, (8, cols))
            if r == 0:
                coef[1, 1] = jnp.broadcast_to(clat, (8, cols))
            coef[1, 2 + 2 * r] = jnp.broadcast_to(clon, (8, cols))
        below = jnp.broadcast_to(nclat[1:2, :], (8, cols))
        beside = jnp.broadcast_to(neclat[1:2, :], (8, cols))
        first_lane = lax.broadcasted_iota(jnp.int32, (8, cols), 1) == 0
        beside = after(jnp.where(first_lane, beside, below))
        coef[0, 5] = coef[1, 1] * below
        coef[0, 6] = below * (coef[1, 3] + c0)
        coef[0, 7] = below * n0
        coef[0, 8] = below * o0 + coef[1, 4] * beside

    @pl.when(jnp.logical_not(has_north))
    def _():
        for k in range(5, 9):
            coef[0, k] = jnp.zeros((8, cols), jnp.float32)

    @pl.when(even)
    def _():
        mix_out.start()

    def pick(k, n):
        value = jnp.int32(0)
        for at in range(max(len(even_order), len(odd_order))):
            a = even_order[at][n] if at < len(even_order) else 0
            b = odd_order[at][n] if at < len(odd_order) else 0
            one = a if a == b else jnp.where(odd, b, a)
            value = jnp.where(k == at, one, value)
        return value

    def body(k, carry):
        kind, g = pick(k, 0), pick(k, 1)
        first, own1, own0, ghost = kind == FIRST, kind == OWN1, kind == OWN0, kind == GHOST
        merged = g >= half

        for at, items in relay_plan.items():
            @pl.when(jnp.logical_and(passes_on, k == at))
            def _(items=items):
                for w, group in items:
                    for p in range(LP):
                        forward_in = to_relay(w * per + group, p)
                        forward_in.wait_recv()
                        forward(w * per + group, p).start()

        @pl.when(jnp.logical_and(even, k == min(relay_plan)))
        def _():
            for n in range(1, per - half):
                for p in range(LP):
                    state_out(n, p).start()

        @pl.when(jnp.logical_not(first))
        def _():
            w = own0.astype(jnp.int32)
            u = w * per + g
            south_adds = jnp.logical_and(has_south, jnp.logical_or(odd, jnp.logical_or(own0, g < half)))
            south_adds = jnp.logical_and(south_adds, jnp.logical_not(ghost))
            ghost_adds = jnp.logical_and(jnp.logical_and(own0, merged), jnp.logical_and(odd, has_south))

            @pl.when(south_adds)
            def _():
                for p in range(LP):
                    direct(u, p).wait_recv()
                    for r in range(2):
                        xbuf[p, :, half_of(r)] = pbuf[u, p, r] + vin[u, p, r]

            @pl.when(ghost_adds)
            def _():
                for p in range(LP):
                    ghost_out(g - half, p).wait_recv()
                    for r in range(2):
                        xbuf[p, :, half_of(r)] = xbuf[p, :, half_of(r)] + zin[g - half, p, r]

            @pl.when(jnp.logical_not(jnp.logical_or(south_adds, ghost)))
            def _():
                for p in range(LP):
                    for r in range(2):
                        xbuf[p, :, half_of(r)] = pbuf[u, p, r]

            @pl.when(ghost)
            def _():
                @pl.when(g == half)
                def _():
                    stiff_out.wait_recv()
                    mix_out.wait_recv()
                for p in range(LP):
                    state_out(g - half, p).wait_recv()
                    for r in range(2):
                        xbuf[p, :, half_of(r)] = vout[g, p, r]
                        ybuf[p, :, half_of(r)] = st_in[g - half, p, r]
                        lbuf[p, :, half_of(r)] = gstiff[g * LP + p, r:r + 1]

            @pl.when(jnp.logical_not(ghost))
            def _():
                for p in range(LP):
                    tmp[p] = state[nwin - 1 - w, g * LP + p].astype(jnp.float32)
                    for r in range(2):
                        ybuf[p, :, half_of(r)] = tmp[p, pl.ds(r, spec, stride=2), :]
                        lbuf[p, :, half_of(r)] = stiff_ref[g * LP + p, r:r + 1]

            flats = chem(g)

            @pl.when(own0)
            def _():
                for p in range(LP):
                    for r in range(2):
                        tmp[p, pl.ds(r, spec, stride=2), :] = flats[p][:, r * cols:(r + 1) * cols]
                    outbuf[g, p] = tmp[p].astype(jnp.bfloat16)

                @pl.when(g == 0)
                def _():
                    fin[...] = flats[0]
                    regions()

                @pl.when(g == 1)
                def _():
                    regions_turn()

            @pl.when(jnp.logical_not(own0))
            def _():
                slot = jnp.where(ghost, units + g - half, per + g)
                for p in range(LP):
                    for r in range(2):
                        lamb[slot, p, r] = flats[p][:, r * cols:(r + 1) * cols]
                pack(slot, jnp.where(ghost, 1, 0))
                col_copy(slot).start()

        @pl.when(jnp.logical_not(own0))
        def _():
            slot = jnp.where(first, g, jnp.where(ghost, units + g - half, per + g))
            col_copy(slot).wait_recv()
            move(slot, jnp.where(ghost, 1, 0))

            @pl.when(jnp.logical_and(own1, jnp.logical_and(odd, merged)))
            def _():
                for p in range(LP):
                    for r in range(2):
                        vout[slot, p, r] = vout[slot, p, r] + pbuf[units + g - half, p, r]

            @pl.when(jnp.logical_not(ghost))
            def _():
                to_north, to_pass = sends_own(slot)

                @pl.when(to_north)
                def _():
                    for p in range(LP):
                        direct(slot, p).start()

                @pl.when(to_pass)
                def _():
                    for p in range(LP):
                        to_relay(slot, p).start()

            @pl.when(jnp.logical_and(ghost, sends_ghost))
            def _():
                for p in range(LP):
                    ghost_out(g - half, p).start()

        @pl.when(jnp.logical_and(even, k == 0))
        def _():
            for p in range(1, LP):
                state_out(0, p).start()
        return carry

    lax.fori_loop(0, jnp.where(odd, len(odd_order), len(even_order)), body, 0)
    regions_end()

    def drain(u, carry):
        col_copy(u).wait_send()
        to_north, to_pass = sends_own(u)

        @pl.when(to_north)
        def _():
            for p in range(LP):
                direct(u, p).wait_send()

        @pl.when(to_pass)
        def _():
            for p in range(LP):
                to_relay(u, p).wait_send()

        @pl.when(jnp.logical_and(passes_on, lax.rem(u, 2) == 1))
        def _():
            for p in range(LP):
                forward(u, p).wait_send()
        return carry

    lax.fori_loop(0, units, drain, 0)

    @pl.when(has_south)
    def _():
        for copy in rows_out:
            copy.wait_send()

    @pl.when(even)
    def _():
        stiff_out.wait_send()
        mix_out.wait_send()
        for n in range(per - half):
            for p in range(LP):
                state_out(n, p).wait_send()

    @pl.when(odd)
    def _():
        for n in range(per - half):
            col_copy(units + n).wait_send()

    @pl.when(sends_ghost)
    def _():
        for n in range(per - half):
            for p in range(LP):
                ghost_out(n, p).wait_send()
    for k in range(1, n_lon):
        spread(k).wait_send()
    for k in range(1, n_lat):
        spread2(k).wait_send()


def finish(held_ref, grad_ref, out_hbm, grad_hbm, sems):
    copies = [
        pltpu.make_async_copy(held_ref, out_hbm, sems.at[0]),
        pltpu.make_async_copy(grad_ref, grad_hbm, sems.at[1]),
    ]
    for copy in copies:
        copy.start()
    for copy in copies:
        copy.wait()


def solution(mesh):
    n_lat, n_lon = mesh.shape["lat"], mesh.shape["lon"]
    assert n_lat % 2 == 0

    def per_device(adjoint_in, state, inverses, courant_lon, courant_lat, emission, region_id, stiffness):
        lev, spec, rows, cols = adjoint_in.shape
        nwin, steps = state.shape[0], inverses.shape[0]
        per = lev // LP
        units = nwin * per
        kept = per - per // 2
        lat8 = -(-n_lat // 8) * 8
        f32, bf16 = jnp.float32, jnp.bfloat16
        any_space = pl.BlockSpec(memory_space=pl.ANY)
        vmem = pl.BlockSpec(memory_space=pltpu.VMEM)
        dma = pltpu.SemaphoreType.DMA

        def blocks(n):
            return pltpu.VMEM((n, LP, rows, spec, cols), f32)

        out, grad = pl.pallas_call(
            functools.partial(kernel, n_lat, n_lon),
            out_shape=(
                pltpu.VMEM((per, LP, rows * spec, cols), bf16),
                pltpu.VMEM((1, spec), f32),
            ),
            in_specs=[any_space] * 8,
            out_specs=(vmem, vmem),
            scratch_shapes=[
                pltpu.VMEM((lev, rows * spec, cols), bf16),
                pltpu.VMEM((nwin, lev, rows * spec, cols), bf16),
                pltpu.VMEM((steps, spec * lev, spec), bf16),
                pltpu.VMEM(courant_lon.shape, f32),
                pltpu.VMEM(courant_lat.shape, f32),
                pltpu.VMEM((spec * rows, cols), f32),
                pltpu.VMEM(region_id.shape, jnp.int32),
                pltpu.VMEM(stiffness.shape, jnp.int32),
                pltpu.VMEM((spec * lev, spec), f32),
                pltpu.VMEM(inverses.shape, bf16),
                blocks(units + kept), blocks(units + kept), blocks(units + kept),
                blocks(units), blocks(units), blocks(kept), blocks(kept), blocks(kept),
                pltpu.VMEM((units + kept, spec, cols), f32),
                pltpu.VMEM((units + kept, spec, cols), f32),
                pltpu.VMEM(courant_lon.shape, f32),
                pltpu.VMEM(courant_lat.shape, f32),
                pltpu.VMEM(courant_lat.shape, f32),
                pltpu.VMEM(stiffness.shape, jnp.int32),
                pltpu.VMEM((LP, spec, rows * cols), f32),
                pltpu.VMEM((LP, spec, rows * cols), f32),
                pltpu.VMEM((LP, 1, rows * cols), jnp.int32),
                pltpu.VMEM((LP, rows * spec, cols), f32),
                pltpu.VMEM((spec, rows * cols), f32),
                pltpu.VMEM((2, 9, 8, cols), f32),
                pltpu.VMEM((n_lon, lat8, spec), f32),
                pltpu.VMEM((n_lon, lat8, spec), f32),
                pltpu.VMEM((n_lat, 1, spec), f32),
                pltpu.VMEM((n_lat, 1, spec), f32),
                dma((per,)), dma((nwin,)), dma, dma((5,)),
                dma((units + kept, LP)), dma((units, LP)), dma((units, LP)), dma((units, LP)), dma((kept, LP)),
                dma((kept, LP)), dma((kept, LP)),
                dma((units + kept,)), dma((units + kept,)), dma((5,)), dma((5,)),
                dma((n_lon,)), dma((n_lon,)), dma((n_lat,)), dma((n_lat,)),
            ],
            compiler_params=pltpu.CompilerParams(collective_id=0, has_side_effects=True),
        )(
            adjoint_in.reshape(lev, spec * rows, cols),
            state.reshape(nwin, lev, spec * rows, cols),
            inverses.transpose(0, 2, 1, 3).reshape(steps, spec * lev, spec), courant_lon, courant_lat,
            emission.reshape(spec * rows, cols), region_id, stiffness,
        )
        out, grad = pl.pallas_call(
            finish,
            out_shape=(
                jax.ShapeDtypeStruct(out.shape, bf16),
                jax.ShapeDtypeStruct(grad.shape, f32),
            ),
            in_specs=[any_space] * 2,
            out_specs=(any_space, any_space),
            scratch_shapes=[dma((2,))],
        )(*(pltpu.with_memory_space_constraint(x, pltpu.VMEM) for x in (out, grad)))
        return out.reshape(adjoint_in.shape), grad

    in_specs = (
        P(None, None, "lat", "lon"),
        P(None, None, None, "lat", "lon"),
        P(),
        P("lat", "lon"),
        P("lat", "lon"),
        P(None, "lat", "lon"),
        P("lat", "lon"),
        P(None, "lat", "lon"),
    )
    out_specs = (P(None, None, "lat", "lon"), P(("lat", "lon"), None))
    return jax.shard_map(
        per_device, mesh=mesh, in_specs=in_specs, out_specs=out_specs, check_vma=False
    )
```

```python
import functools

import jax
import jax.numpy as jnp
from jax import lax
from jax.experimental import pallas as pl
from jax.experimental.pallas import tpu as pltpu
from jax.sharding import PartitionSpec as P

MESH = pl.DeviceIdType.MESH
OWN1, OWN0, GHOST = 0, 1, 2


def relayed(level):
    return level // 2 % 2 == 1


def even_order(lev):
    half = lev // 2
    passed = [l for l in range(half) if relayed(l)]
    passed_merged = [l for l in range(half, lev) if relayed(l)]
    return [
        ("chem", 1, [(OWN1, l) for l in range(half, lev)]),
        ("relay", 0, passed),
        ("state", 2, half),
        ("chem", 2, [(OWN1, l) for l in range(half) if not relayed(l)]),
        ("relay", 0, passed_merged),
        ("move", 2),
        ("move", 1),
        ("chem", 3, [(OWN1, l) for l in passed]),
        ("relay", 1, passed_merged),
        ("move", 3),
        ("chem", 0, [(OWN0, l) for l in range(half) if not relayed(l)]),
        ("chem", 0, [(OWN0, l) for l in passed]),
        ("turn",),
        ("relay", 1, passed),
        ("chem", 0, [(OWN0, l) for l in range(half, lev) if not relayed(l)]),
        ("chem", 0, [(OWN0, l) for l in passed_merged]),
    ]


def odd_order(lev):
    half = lev // 2
    assert half == 4
    m = half
    batches = [
        [(GHOST, m)], [(OWN1, 0)], [(OWN1, 1)], [(OWN1, 2), (GHOST, m + 1)], [(OWN1, 3), (OWN1, m)],
        [(OWN1, m + 1), (GHOST, m + 2)], [(OWN1, m + 2), (GHOST, m + 3)], [(OWN1, m + 3)],
    ]

    def chem(n):
        return ("chem", n, batches[n - 1])

    return [
        chem(1), chem(2), ("move", 1), chem(3), ("move", 2), chem(4), ("move", 3), chem(5), ("move", 4),
        chem(6), ("move", 5), ("move", 6), chem(7), chem(8), ("move", 7), ("move", 8),
        ("chem", 0, [(OWN0, 0), (OWN0, 1)]),
        ("chem", 0, [(OWN0, m), (OWN0, m + 1)]),
        ("turn",),
        ("chem", 0, [(OWN0, m + 2), (OWN0, m + 3)]),
        ("chem", 0, [(OWN0, 2), (OWN0, 3)]),
    ]


def messages(lev):
    return 1 + max(op[1] for op in even_order(lev) + odd_order(lev) if op[0] == "chem")


def kernel(
    n_lat, n_lon,
    adj_hbm, state_hbm, inv_hbm, clon_hbm, clat_hbm, em_hbm, reg_hbm, stiff_hbm,
    outbuf, grad_ref,
    adj, state, inv, clon_ref, clat_ref, em_ref, reg_ref, stiff_ref, tall, mats,
    lamb, pbuf, vout, vin, relay, zin, st_out, st_in, cout, cin, nclon, nclat, neclat, gstiff,
    tmp, fin, coef, part, inbox1, turn, inbox2,
    adj_sem, state_sem, inv_sem, small_sem, vs, vr, rr, fs, zr, ss, sr, cs, cr, ks, kr, s1, r1, s2, r2,
):
    lev, rows2, cols = adj.shape
    nwin = state.shape[0]
    steps = inv.shape[0]
    spec = rows2 // 2
    half = lev // 2
    lat, lon = lax.axis_index("lat"), lax.axis_index("lon")
    odd = lax.rem(lat, 2) == 1
    even = lax.rem(lat, 2) == 0
    north = jnp.maximum(lat - 1, 0)
    north2 = jnp.maximum(lat - 2, 0)
    south = jnp.minimum(lat + 1, n_lat - 1)
    west = lax.rem(lon + n_lon - 1, n_lon)
    east = lax.rem(lon + 1, n_lon)
    has_north = lat > 0
    has_south = lat < n_lat - 1
    sends_ghost = lat >= 2
    passes_on = lat + 2 < n_lat
    plans = {0: even_order(lev), 1: odd_order(lev)}

    barrier = pltpu.get_barrier_semaphore()

    def greet(to):
        pl.semaphore_signal(barrier, inc=1, device_id=to, device_id_type=MESH)

    for k in range(1, n_lon):
        greet((lat, lax.rem(lon + k, n_lon)))
    for k in range(1, n_lat):
        greet((lax.rem(lat + k, n_lat), lon))

    @pl.when(has_south)
    def _():
        greet((south, west))

    @pl.when(has_north)
    def _():
        greet((north, east))

    adj_load = pltpu.make_async_copy(adj_hbm, adj, adj_sem)
    small = [
        pltpu.make_async_copy(src, dst, small_sem.at[n])
        for n, (src, dst) in enumerate((
            (clon_hbm, clon_ref), (clat_hbm, clat_ref), (stiff_hbm, stiff_ref),
            (reg_hbm, reg_ref), (em_hbm, em_ref)))
    ]
    state_loads = [
        pltpu.make_async_copy(state_hbm.at[w], state.at[w], state_sem.at[w]) for w in range(nwin)
    ]
    inv_load = pltpu.make_async_copy(inv_hbm, inv, inv_sem)
    for load in small[:2] + [adj_load, state_loads[nwin - 1], inv_load] + small[2:] + state_loads[:nwin - 1]:
        load.start()

    lane = lax.broadcasted_iota(jnp.int32, (spec, cols), 1)

    def slot_of(kind, level):
        return {OWN1: level, OWN0: lev + level, GHOST: 2 * lev + level - half}[kind]

    def after_chem(kind, level):
        return slot_of(OWN0 if kind == OWN1 else GHOST, level)

    def weights(which, names):
        return [coef[which, k, 0:1, :] for k in names]

    def remote(src, dst, send, recv, to):
        return pltpu.make_async_remote_copy(
            src_ref=src, dst_ref=dst, send_sem=send, recv_sem=recv, device_id=to, device_id_type=MESH)

    def direct(u):
        return remote(vout.at[u], vin.at[u], vs.at[u], vr.at[u], (north, lon))

    def to_relay(u):
        return remote(vout.at[u], relay.at[u], vs.at[u], rr.at[u], (north2, lon))

    def forward(u):
        return remote(relay.at[u], vin.at[u], fs.at[u], vr.at[u], (south, lon))

    def ghost_out(level):
        u, n = slot_of(GHOST, level), level - half
        return remote(vout.at[u], zin.at[n], vs.at[u], zr.at[n], (north2, lon))

    def state_out(n):
        return remote(st_out.at[n], st_in.at[n], ss.at[n], sr.at[n], (south, lon))

    def col_copy(n):
        return remote(cout.at[n], cin.at[n], cs.at[n], cr.at[n], (lat, west))

    rows_out = [
        remote(clon_ref, nclon, ks.at[0], kr.at[0], (south, lon)),
        remote(clat_ref, nclat, ks.at[1], kr.at[1], (south, lon)),
        remote(clat_ref, neclat, ks.at[2], kr.at[2], (south, west)),
    ]
    stiff_out = remote(stiff_ref, gstiff, ks.at[3], kr.at[3], (south, lon))
    mix_out = remote(coef.at[0, pl.ds(5, 4)], coef.at[1, pl.ds(5, 4)], ks.at[4], kr.at[4], (south, lon))

    def after(x):
        return pltpu.roll(x, cols - 1, 1)

    def pack(n, slots):
        message = None
        for i, (u, which) in enumerate(slots):
            c0, n0, o0, c1, o1 = weights(which, range(5))
            row0, row1 = lamb[u, 0], lamb[u, 1]
            new0 = c0 * row0 + n0 * row1 + o0 * after(row0)
            new1 = c1 * row1 + o1 * after(row1)
            for j, x in enumerate((row0, row1, new0, new1)):
                at = 4 * i + j
                message = x if at == 0 else jnp.where(lane == at, pltpu.roll(x, at, 1), message)
        cout[n] = message

    def move(u, which, n, i):
        c0, n0, o0, c1, o1, al, be, ga, de = weights(which, range(9))
        row0, row1, message = lamb[u, 0], lamb[u, 1], cin[n]

        def shift(x, j):
            edge = message if 4 * i + j == 0 else pltpu.roll(message, cols - 4 * i - j, 1)
            return after(jnp.where(lane == 0, edge, x))

        right0, right1 = shift(row0, 0), shift(row1, 1)
        new0 = c0 * row0 + n0 * row1 + o0 * right0
        new1 = c1 * row1 + o1 * right1
        pbuf[u, 0] = c0 * new0 + n0 * new1 + o0 * shift(new0, 2)
        pbuf[u, 1] = c1 * new1 + o1 * shift(new1, 3)
        v0 = al * row0
        v1 = be * row0 + ga * row1 + de * right0
        return v0, v1

    def own_sends(side, u):
        level = u % lev
        if side == 1:
            return None if u < lev and level >= half else (direct(u), None)
        return (to_relay(u) if relayed(level) else direct(u)), has_north

    def when(condition, do):
        if condition is None:
            do()
        else:
            pl.when(condition)(do)

    def transport(side, n, i, kind, level):
        u = slot_of(kind, level)
        with jax.named_scope("move"):
            v0, v1 = move(u, 1 if kind == GHOST else 0, n, i)
            if side == 1 and kind == OWN0 and level >= half:
                ghost = slot_of(GHOST, level)
                v0, v1 = v0 + pbuf[ghost, 0], v1 + pbuf[ghost, 1]
            vout[u, 0], vout[u, 1] = v0, v1
        if kind == GHOST:
            when(sends_ghost, lambda: ghost_out(level).start())
        else:
            leaving = own_sends(side, u)
            if leaving is not None:
                when(leaving[1], lambda: leaving[0].start())

    def gather(side, kind, level, i):
        u = slot_of(kind, level)
        if kind == GHOST:
            n = level - half
            with jax.named_scope("w_st"):
                state_out(n).wait_recv()
            x, y, live = [vout[level, r] for r in range(2)], [st_in[n, r] for r in range(2)], gstiff[level]
        else:
            if side == 1:
                @pl.when(has_south)
                def _():
                    with jax.named_scope("w_vin"):
                        direct(u).wait_recv()
                    extra = kind == OWN0 and level >= half
                    if extra:
                        with jax.named_scope("w_z"):
                            ghost_out(level).wait_recv()
                    for r in range(2):
                        both = vin[u, r] + zin[level - half, r] if extra else vin[u, r]
                        pbuf[u, r] = pbuf[u, r] + both
                x = [pbuf[u, r] for r in range(2)]
            elif kind == OWN0 or level < half:
                with jax.named_scope("w_vin"):
                    direct(u).wait_recv()
                x = [pbuf[u, r] + vin[u, r] for r in range(2)]
            else:
                x = [pbuf[u, r] for r in range(2)]
            tmp[i] = state[nwin - 1 if kind == OWN1 else 0, level].astype(jnp.float32)
            y, live = [tmp[i, pl.ds(r, spec, stride=2), :] for r in range(2)], stiff_ref[level]
        return (
            jnp.concatenate(x, axis=1), jnp.concatenate(y, axis=1),
            jnp.concatenate([live[0:1], live[1:2]], axis=1),
        )

    def chem(levels, gathered):
        flats, ys, lives = zip(*gathered)
        for s in reversed(range(steps)):
            mat = [mats[s, level] for level in levels]

            def dot(xs):
                return [jnp.dot(a, x.astype(jnp.bfloat16), preferred_element_type=jnp.float32) for a, x in zip(mat, xs)]

            v1 = dot(flats)
            v2 = dot([v * y for v, y in zip(v1, ys)])
            v3 = dot([v * y for v, y in zip(v2, ys)])
            flats = [
                jnp.where(live > s, 0.4 * x + 0.3 * a + 0.2 * b + 0.1 * c, x)
                for x, a, b, c, live in zip(flats, v1, v2, v3, lives)
            ]
        return flats

    def spread(k):
        to = lax.rem(lon + k, n_lon)
        return remote(part.at[to], inbox1.at[lon], s1.at[k], r1.at[lon], (lat, to))

    def spread_in(k):
        source = lax.rem(lon + k, n_lon)
        return source, remote(part.at[source], inbox1.at[source], s1.at[k], r1.at[source], (lat, source))

    def spread2(k):
        to = lax.rem(lat + k, n_lat)
        return remote(turn.at[to], inbox2.at[lat], s2.at[k], r2.at[lat], (to, lon))

    def spread2_in(k):
        source = lax.rem(lat + k, n_lat)
        return source, remote(turn.at[source], inbox2.at[source], s2.at[k], r2.at[source], (source, lon))

    def regions():
        lat8 = part.shape[1]
        contrib = jnp.concatenate([
            em_ref[pl.ds(r, spec, stride=2), :]
            * (lamb[lev, r] + fin[:, r * cols:(r + 1) * cols])
            for r in range(2)], axis=1)
        where_from = jnp.concatenate([reg_ref[0:1, :], reg_ref[1:2, :]], axis=1)
        shape = (n_lon * lat8, 2 * cols)
        column = jnp.concatenate([jnp.full((lat8, 2 * cols), c, jnp.int32) for c in range(n_lon)], axis=0)
        band = lax.broadcasted_iota(jnp.int32, (lat8, 2 * cols), 0)
        band = jnp.concatenate([band] * n_lon, axis=0)
        onehot = (jnp.broadcast_to(where_from, shape) == band * n_lon + column).astype(jnp.float32)
        sums = lax.dot_general(
            onehot, contrib, (((1,), (1,)), ((), ())),
            precision=lax.Precision.HIGHEST, preferred_element_type=jnp.float32)
        for c in range(n_lon):
            part[c] = sums[c * lat8:(c + 1) * lat8]
        for k in range(1, n_lon):
            spread(k).start()

    def regions_turn():
        total = part[lon]
        for k in range(1, n_lon):
            source, copy = spread_in(k)
            copy.wait_recv()
            total = total + inbox1[source]
        for b in range(n_lat):
            turn[b] = total[b:b + 1]
        for k in range(1, n_lat):
            spread2(k).start()

    def regions_end():
        total = turn[lat]
        for k in range(1, n_lat):
            source, copy = spread2_in(k)
            copy.wait_recv()
            total = total + inbox2[source]
        grad_ref[...] = total


    def play(side):
        sent = {}
        for op in plans[side]:
            if op[0] == "chem":
                n, items = op[1:]
                gathered = [gather(side, kind, level, i) for i, (kind, level) in enumerate(items)]
                with jax.named_scope("chem"):
                    flats = chem([level for _, level in items], gathered)
                if n:
                    slots = []
                    for (kind, level), flat in zip(items, flats):
                        u = after_chem(kind, level)
                        for r in range(2):
                            lamb[u, r] = flat[:, r * cols:(r + 1) * cols]
                        slots.append((u, 1 if kind == GHOST else 0))
                    with jax.named_scope("pack"):
                        pack(n, slots)
                    col_copy(n).start()
                    sent[n] = [(OWN0 if kind == OWN1 else GHOST, level) for kind, level in items]
                else:
                    for i, ((kind, level), flat) in enumerate(zip(items, flats)):
                        for r in range(2):
                            tmp[i, pl.ds(r, spec, stride=2), :] = flat[:, r * cols:(r + 1) * cols]
                        outbuf[level] = tmp[i].astype(jnp.bfloat16)
                        if level == 0:
                            fin[...] = flat
                            with jax.named_scope("regions"):
                                regions()
            elif op[0] == "move":
                n = op[1]
                with jax.named_scope("w_col"):
                    col_copy(n).wait_recv()
                if side == 1 and n == 1:
                    mix_out.wait_recv()
                for i, (kind, level) in enumerate(sent[n]):
                    transport(side, n, i, kind, level)
            elif op[0] == "relay":
                w, passed = op[1:]

                @pl.when(passes_on)
                def _(w=w, passed=passed):
                    for level in passed:
                        u = w * lev + level
                        with jax.named_scope("w_relay"):
                            to_relay(u).wait_recv()
                        forward(u).start()
            elif op[0] == "state":
                for k in range(op[1], op[2]):
                    state_out(k).start()
            else:
                with jax.named_scope("turn"):
                    regions_turn()

        for n in [0] + sorted(sent):
            col_copy(n).wait_send()
        for u in range(2 * lev):
            leaving = own_sends(side, u)
            if leaving is not None:
                when(leaving[1], lambda: leaving[0].wait_send())
        if side == 1:
            @pl.when(sends_ghost)
            def _():
                for level in range(half, lev):
                    ghost_out(level).wait_send()
        else:
            @pl.when(passes_on)
            def _():
                for u in range(2 * lev):
                    if relayed(u % lev):
                        forward(u).wait_send()
            stiff_out.wait_send()
            mix_out.wait_send()
            for k in range(half):
                state_out(k).wait_send()

    for load in small[:2]:
        load.wait()
    for r in range(2):
        clon, clat = clon_ref[r:r + 1, :], clat_ref[r:r + 1, :]
        coef[0, 3 * r] = jnp.broadcast_to(1.0 - clon - clat, (8, cols))
        if r == 0:
            coef[0, 1] = jnp.broadcast_to(clat, (8, cols))
        coef[0, 2 + 2 * r] = jnp.broadcast_to(clon, (8, cols))

    adj_load.wait()
    for level in range(lev):
        tmp[level % 4] = adj[level].astype(jnp.float32)
        for r in range(2):
            lamb[level, r] = tmp[level % 4, pl.ds(r, spec, stride=2), :]
    pack(0, [(level, 0) for level in range(lev)])
    state_loads[nwin - 1].wait()

    @pl.when(even)
    def _():
        for n in range(half):
            tmp[n % 4] = state[nwin - 1, half + n].astype(jnp.float32)
            for r in range(2):
                st_out[n, r] = tmp[n % 4, pl.ds(r, spec, stride=2), :]

    inv_load.wait()
    for s in range(steps):
        tall[...] = inv[s].astype(jnp.float32)
        for level in range(lev):
            mats[s, level] = tall[pl.ds(level, spec, stride=lev), :].T.astype(jnp.bfloat16)
    for load in small[2:]:
        load.wait()
    for w in range(nwin - 1):
        state_loads[w].wait()

    with jax.named_scope("w_barrier"):
        pl.semaphore_wait(
            barrier, n_lon - 1 + n_lat - 1 + has_north.astype(jnp.int32) + has_south.astype(jnp.int32))

    @pl.when(has_south)
    def _():
        for copy in rows_out:
            copy.start()
    col_copy(0).start()

    @pl.when(even)
    def _():
        stiff_out.start()
        state_out(0).start()

    @pl.when(has_north)
    def _():
        for copy in rows_out:
            copy.wait_recv()
        c0, o0, n0 = coef[0, 0], coef[0, 2], coef[0, 1]
        for r in range(2):
            clon, clat = nclon[r:r + 1, :], nclat[r:r + 1, :]
            coef[1, 3 * r] = jnp.broadcast_to(1.0 - clon - clat, (8, cols))
            if r == 0:
                coef[1, 1] = jnp.broadcast_to(clat, (8, cols))
            coef[1, 2 + 2 * r] = jnp.broadcast_to(clon, (8, cols))
        below = jnp.broadcast_to(nclat[1:2, :], (8, cols))
        beside = jnp.broadcast_to(neclat[1:2, :], (8, cols))
        first_lane = lax.broadcasted_iota(jnp.int32, (8, cols), 1) == 0
        beside = after(jnp.where(first_lane, beside, below))
        coef[0, 5] = coef[1, 1] * below
        coef[0, 6] = below * (coef[1, 3] + c0)
        coef[0, 7] = below * n0
        coef[0, 8] = below * o0 + coef[1, 4] * beside

    @pl.when(jnp.logical_not(has_north))
    def _():
        for k in range(5, 9):
            coef[0, k] = jnp.zeros((8, cols), jnp.float32)

    with jax.named_scope("w_col"):
        col_copy(0).wait_recv()

    @pl.when(even)
    def _():
        mix_out.start()
        for level in range(lev):
            transport(0, 0, level, OWN1, level)
            if level == 1:
                state_out(1).start()
        play(0)

    @pl.when(odd)
    def _():
        for level in range(lev):
            transport(1, 0, level, OWN1, level)
        stiff_out.wait_recv()
        play(1)

    @pl.when(has_south)
    def _():
        for copy in rows_out:
            copy.wait_send()
    with jax.named_scope("reg_end"):
        regions_end()
    for k in range(1, n_lon):
        spread(k).wait_send()
    for k in range(1, n_lat):
        spread2(k).wait_send()


def finish(held_ref, grad_ref, out_hbm, grad_hbm, sems):
    copies = [
        pltpu.make_async_copy(held_ref, out_hbm, sems.at[0]),
        pltpu.make_async_copy(grad_ref, grad_hbm, sems.at[1]),
    ]
    for copy in copies:
        copy.start()
    for copy in copies:
        copy.wait()


def solution(mesh):
    n_lat, n_lon = mesh.shape["lat"], mesh.shape["lon"]
    assert n_lat % 2 == 0

    def per_device(adjoint_in, state, inverses, courant_lon, courant_lat, emission, region_id, stiffness):
        lev, spec, rows, cols = adjoint_in.shape
        nwin, steps = state.shape[0], inverses.shape[0]
        assert nwin == 2 and rows == 2
        half = lev // 2
        slots = nwin * lev + half
        lat8 = -(-n_lat // 8) * 8
        f32, bf16 = jnp.float32, jnp.bfloat16
        any_space = pl.BlockSpec(memory_space=pl.ANY)
        vmem = pl.BlockSpec(memory_space=pltpu.VMEM)
        dma = pltpu.SemaphoreType.DMA

        def blocks(n):
            return pltpu.VMEM((n, rows, spec, cols), f32)

        out, grad = pl.pallas_call(
            functools.partial(kernel, n_lat, n_lon),
            out_shape=(
                pltpu.VMEM((lev, rows * spec, cols), bf16),
                pltpu.VMEM((1, spec), f32),
            ),
            in_specs=[any_space] * 8,
            out_specs=(vmem, vmem),
            scratch_shapes=[
                pltpu.VMEM((lev, rows * spec, cols), bf16),
                pltpu.VMEM((nwin, lev, rows * spec, cols), bf16),
                pltpu.VMEM((steps, spec * lev, spec), bf16),
                pltpu.VMEM(courant_lon.shape, f32),
                pltpu.VMEM(courant_lat.shape, f32),
                pltpu.VMEM((spec * rows, cols), f32),
                pltpu.VMEM(region_id.shape, jnp.int32),
                pltpu.VMEM(stiffness.shape, jnp.int32),
                pltpu.VMEM((spec * lev, spec), f32),
                pltpu.VMEM(inverses.shape, bf16),
                blocks(slots), blocks(slots), blocks(slots),
                blocks(nwin * lev), blocks(nwin * lev), blocks(half), blocks(half), blocks(half),
                pltpu.VMEM((messages(lev), spec, cols), f32),
                pltpu.VMEM((messages(lev), spec, cols), f32),
                pltpu.VMEM(courant_lon.shape, f32),
                pltpu.VMEM(courant_lat.shape, f32),
                pltpu.VMEM(courant_lat.shape, f32),
                pltpu.VMEM(stiffness.shape, jnp.int32),
                pltpu.VMEM((4, rows * spec, cols), f32),
                pltpu.VMEM((spec, rows * cols), f32),
                pltpu.VMEM((2, 9, 8, cols), f32),
                pltpu.VMEM((n_lon, lat8, spec), f32),
                pltpu.VMEM((n_lon, lat8, spec), f32),
                pltpu.VMEM((n_lat, 1, spec), f32),
                pltpu.VMEM((n_lat, 1, spec), f32),
                dma, dma((nwin,)), dma, dma((5,)),
                dma((slots,)), dma((nwin * lev,)), dma((nwin * lev,)), dma((nwin * lev,)), dma((half,)),
                dma((half,)), dma((half,)),
                dma((messages(lev),)), dma((messages(lev),)), dma((5,)), dma((5,)),
                dma((n_lon,)), dma((n_lon,)), dma((n_lat,)), dma((n_lat,)),
            ],
            compiler_params=pltpu.CompilerParams(collective_id=0, has_side_effects=True),
        )(
            adjoint_in.reshape(lev, spec * rows, cols),
            state.reshape(nwin, lev, spec * rows, cols),
            inverses.transpose(0, 2, 1, 3).reshape(steps, spec * lev, spec), courant_lon, courant_lat,
            emission.reshape(spec * rows, cols), region_id, stiffness,
        )
        out, grad = pl.pallas_call(
            finish,
            out_shape=(
                jax.ShapeDtypeStruct(out.shape, bf16),
                jax.ShapeDtypeStruct(grad.shape, f32),
            ),
            in_specs=[any_space] * 2,
            out_specs=(any_space, any_space),
            scratch_shapes=[dma((2,))],
        )(*(pltpu.with_memory_space_constraint(x, pltpu.VMEM) for x in (out, grad)))
        return out.reshape(adjoint_in.shape), grad

    in_specs = (
        P(None, None, "lat", "lon"),
        P(None, None, None, "lat", "lon"),
        P(),
        P("lat", "lon"),
        P("lat", "lon"),
        P(None, "lat", "lon"),
        P("lat", "lon"),
        P(None, "lat", "lon"),
    )
    out_specs = (P(None, None, "lat", "lon"), P(("lat", "lon"), None))
    return jax.shard_map(
        per_device, mesh=mesh, in_specs=in_specs, out_specs=out_specs, check_vma=False
    )
```

```python
import functools

import jax
import jax.numpy as jnp
from jax import lax
from jax.experimental import pallas as pl
from jax.experimental.pallas import tpu as pltpu
from jax.sharding import PartitionSpec as P

MESH = pl.DeviceIdType.MESH
OWN1, OWN0, GHOST = 0, 1, 2


def relayed(level, window=0):
    return level // 2 % 2 == 1 or (window == 1 and level == 1)


def even_order(lev):
    half = lev // 2
    passed = [l for l in range(half) if relayed(l)]
    passed_merged = [l for l in range(half, lev) if relayed(l)]
    return [
        ("first", list(range(half, lev))),
        ("relay", 0, passed[:1]),
        ("chem", 1, [(OWN1, l) for l in range(half, lev)]),
        ("relay", 0, passed[1:]),
        ("state", 2, half - 1),
        ("first", list(range(half))),
        ("chem", 2, [(OWN1, l) for l in range(half) if not relayed(l)]),
        ("relay", 0, passed_merged),
        ("state", half - 1, half),
        ("chem", 3, [(OWN1, l) for l in passed]),
        ("move", 2),
        ("move", 1),
        ("move", 3),
        ("chem", 0, [(OWN0, l) for l in range(half) if not relayed(l)]),
        ("relay", 1, [l for l in range(half) if relayed(l, 1) and not relayed(l)]),
        ("relay", 1, passed_merged),
        ("chem", 0, [(OWN0, l) for l in passed]),
        ("turn",),
        ("relay", 1, passed),
        ("chem", 0, [(OWN0, l) for l in range(half, lev) if not relayed(l)]),
        ("chem", 0, [(OWN0, l) for l in passed_merged]),
    ]


def odd_order(lev):
    half = lev // 2
    assert half == 4
    m = half
    batches = [
        [(OWN1, 0)], [(OWN1, 1)], [(GHOST, m), (OWN1, 2)], [(OWN1, 3), (OWN1, m)],
        [(GHOST, m + 1), (OWN1, m + 1)], [(GHOST, m + 2), (OWN1, m + 2)], [(GHOST, m + 3), (OWN1, m + 3)],
    ]

    def chem(n):
        return ("chem", n, batches[n - 1])

    return [
        ("first", [0]), chem(1), ("first", [1]), chem(2), ("first", list(range(2, lev))),
        ("move", 1), chem(3), ("move", 2), chem(4), ("move", 3), chem(5), ("move", 4),
        chem(6), ("move", 5), chem(7), ("move", 6),
        ("chem", 0, [(OWN0, 0)]),
        ("move", 7),
        ("chem", 0, [(OWN0, 1), (OWN0, m)]),
        ("turn",),
        ("chem", 0, [(OWN0, m + 1), (OWN0, m + 2)]),
        ("chem", 0, [(OWN0, 2), (OWN0, 3), (OWN0, m + 3)]),
    ]


def messages(lev):
    return 1 + max(op[1] for op in even_order(lev) + odd_order(lev) if op[0] == "chem")


def kernel(
    n_lat, n_lon,
    adj_hbm, state_hbm, inv_hbm, clon_hbm, clat_hbm, em_hbm, reg_hbm, stiff_hbm,
    outbuf, grad_ref,
    adj, state, inv, clon_ref, clat_ref, em_ref, reg_ref, stiff_ref, tall, mats,
    lamb, pbuf, vout, vin, relay, zin, st_out, st_in, cout, cin, nclon, nclat, neclat, sclon, sclat, eclat, gstiff, corner_end, corner_in, corner,
    tmp, fin, coef, mixed, part, inbox1, turn, inbox2,
    adj_sem, state_sem, inv_sem, small_sem, vs, vr, rr, fs, zr, ss, sr, cs, cr, ks, kr, ds, dr, s1, r1, s2, r2,
):
    lev, rows2, cols = adj.shape
    nwin = state.shape[0]
    steps = inv.shape[0]
    spec = rows2 // 2
    half = lev // 2
    lat, lon = lax.axis_index("lat"), lax.axis_index("lon")
    odd = lax.rem(lat, 2) == 1
    even = lax.rem(lat, 2) == 0
    north = jnp.maximum(lat - 1, 0)
    north2 = jnp.maximum(lat - 2, 0)
    south = jnp.minimum(lat + 1, n_lat - 1)
    west = lax.rem(lon + n_lon - 1, n_lon)
    east = lax.rem(lon + 1, n_lon)
    has_north = lat > 0
    has_south = lat < n_lat - 1
    sends_ghost = lat >= 2
    passes_on = lat + 2 < n_lat
    plans = {0: even_order(lev), 1: odd_order(lev)}

    barrier = pltpu.get_barrier_semaphore()

    def greet(to):
        pl.semaphore_signal(barrier, inc=1, device_id=to, device_id_type=MESH)

    for k in range(1, n_lon):
        greet((lat, lax.rem(lon + k, n_lon)))
    for k in range(1, n_lat):
        greet((lax.rem(lat + k, n_lat), lon))

    @pl.when(has_south)
    def _():
        greet((south, west))
        greet((south, east))

    @pl.when(has_north)
    def _():
        greet((north, east))
        greet((north, west))

    adj_load = pltpu.make_async_copy(adj_hbm, adj, adj_sem)
    small = [
        pltpu.make_async_copy(src, dst, small_sem.at[n])
        for n, (src, dst) in enumerate((
            (clon_hbm, clon_ref), (clat_hbm, clat_ref), (stiff_hbm, stiff_ref),
            (reg_hbm, reg_ref), (em_hbm, em_ref)))
    ]
    state_loads = [
        pltpu.make_async_copy(state_hbm.at[w], state.at[w], state_sem.at[w]) for w in range(nwin)
    ]
    inv_load = pltpu.make_async_copy(inv_hbm, inv, inv_sem)
    for load in small[:2] + [adj_load, state_loads[nwin - 1], inv_load] + small[2:] + state_loads[:nwin - 1]:
        load.start()

    lane = lax.broadcasted_iota(jnp.int32, (spec, cols), 1)

    def slot_of(kind, level):
        return {OWN1: level, OWN0: lev + level, GHOST: 2 * lev + level - half}[kind]

    def after_chem(kind, level):
        return slot_of(OWN0 if kind == OWN1 else GHOST, level)

    def weights(which, names):
        return [coef[which, k, 0:1, :] for k in names]

    def remote(src, dst, send, recv, to):
        return pltpu.make_async_remote_copy(
            src_ref=src, dst_ref=dst, send_sem=send, recv_sem=recv, device_id=to, device_id_type=MESH)

    def leaves(u):
        return (lamb if u < lev else vout).at[u]

    def direct(u):
        return remote(leaves(u), vin.at[u], vs.at[u], vr.at[u], (north, lon))

    def to_relay(u):
        return remote(leaves(u), relay.at[u], vs.at[u], rr.at[u], (north2, lon))

    def forward(u):
        return remote(relay.at[u], vin.at[u], fs.at[u], vr.at[u], (south, lon))

    def ghost_out(level):
        u, n = slot_of(GHOST, level), level - half
        return remote(vout.at[u], zin.at[n], vs.at[u], zr.at[n], (north2, lon))

    def state_out(n):
        return remote(st_out.at[n], st_in.at[n], ss.at[n], sr.at[n], (south, lon))

    def col_copy(n):
        return remote(cout.at[n], cin.at[n], cs.at[n], cr.at[n], (lat, west))

    rows_out = [
        remote(clon_ref, nclon, ks.at[0], kr.at[0], (south, lon)),
        remote(clat_ref, nclat, ks.at[1], kr.at[1], (south, lon)),
        remote(clat_ref, neclat, ks.at[2], kr.at[2], (south, west)),
    ]
    rows_north = [
        remote(clon_ref, sclon, ks.at[5], kr.at[5], (north, lon)),
        remote(clat_ref, sclat, ks.at[6], kr.at[6], (north, lon)),
    ]
    rows_west = remote(clat_ref, eclat, ks.at[7], kr.at[7], (lat, west))
    corner_out = remote(corner_end, corner_in, ds, dr, (north, west))
    stiff_out = remote(stiff_ref, gstiff, ks.at[3], kr.at[3], (south, lon))
    mix_out = remote(coef.at[0, pl.ds(5, 4)], coef.at[1, pl.ds(5, 4)], ks.at[4], kr.at[4], (south, lon))

    def after(x):
        return pltpu.roll(x, cols - 1, 1)

    def pack(n, slots):
        message = None
        for i, (u, which) in enumerate(slots):
            c0, n0, o0, c1, o1 = weights(which, range(5))
            row0, row1 = lamb[u, 0], lamb[u, 1]
            new0 = c0 * row0 + n0 * row1 + o0 * after(row0)
            new1 = c1 * row1 + o1 * after(row1)
            for j, x in enumerate((row0, row1, new0, new1)):
                at = 4 * i + j
                message = x if at == 0 else jnp.where(lane == at, pltpu.roll(x, at, 1), message)
        cout[n] = message

    def move(u, which, n, i, combine):
        c0, n0, o0, c1, o1, al, be, ga, de = weights(which, range(9))
        row0, row1, message = lamb[u, 0], lamb[u, 1], cin[n]

        def shift(x, j):
            edge = message if 4 * i + j == 0 else pltpu.roll(message, cols - 4 * i - j, 1)
            return after(jnp.where(lane == 0, edge, x))

        right0, right1 = shift(row0, 0), shift(row1, 1)
        new0 = c0 * row0 + n0 * row1 + o0 * right0
        new1 = c1 * row1 + o1 * right1
        pbuf[u, 0] = c0 * new0 + n0 * new1 + o0 * shift(new0, 2)
        pbuf[u, 1] = c1 * new1 + o1 * shift(new1, 3)
        if not combine:
            return None
        v0 = al * row0
        v1 = be * row0 + ga * row1 + de * right0
        return v0, v1

    def own_sends(side, u):
        level = u % lev
        if side == 1:
            return None if u < lev and level >= half else (direct(u), None)
        return (to_relay(u) if relayed(level, u // lev) else direct(u)), has_north

    def when(condition, do):
        if condition is None:
            do()
        else:
            pl.when(condition)(do)

    def transport(side, n, i, kind, level):
        u = slot_of(kind, level)
        combine = kind != OWN1 or (side == 1 and level >= half)
        with jax.named_scope("move"):
            both = move(u, 1 if kind == GHOST else 0, n, i, combine)
            if combine:
                if side == 1 and kind == OWN0 and level >= half:
                    ghost = slot_of(GHOST, level)
                    both = both[0] + pbuf[ghost, 0], both[1] + pbuf[ghost, 1]
                vout[u, 0], vout[u, 1] = both
        if kind == GHOST:
            when(sends_ghost, lambda: ghost_out(level).start())
        elif kind == OWN0:
            send(side, u)

    def send(side, u):
        leaving = own_sends(side, u)
        if leaving is not None:
            when(leaving[1], lambda: leaving[0].start())

    def arrived(level):
        al, be, ga, de = [mixed[k, 0:1, :] for k in range(4)]
        row0, row1, message = vin[level, 0], vin[level, 1], corner[...]
        edge = message if level == 0 else pltpu.roll(message, cols - 4 * level, 1)
        right0 = after(jnp.where(lane == 0, edge, row0))
        return al * row0, be * row0 + ga * row1 + de * right0

    def gather(side, kind, level, i):
        u = slot_of(kind, level)
        if kind == GHOST:
            n = level - half
            with jax.named_scope("w_st"):
                state_out(n).wait_recv()
            if n == 0:
                stiff_out.wait_recv()
            x, y, live = [vout[level, r] for r in range(2)], [st_in[n, r] for r in range(2)], gstiff[level]
        else:
            if side == 1:
                @pl.when(has_south)
                def _():
                    with jax.named_scope("w_vin"):
                        direct(u).wait_recv()
                    extra = kind == OWN0 and level >= half
                    if extra:
                        with jax.named_scope("w_z"):
                            ghost_out(level).wait_recv()
                    adds = arrived(level) if kind == OWN1 else [vin[u, r] for r in range(2)]
                    for r in range(2):
                        both = adds[r] + zin[level - half, r] if extra else adds[r]
                        pbuf[u, r] = pbuf[u, r] + both
                x = [pbuf[u, r] for r in range(2)]
            elif kind == OWN0 or level < half:
                with jax.named_scope("w_vin"):
                    direct(u).wait_recv()
                adds = arrived(level) if kind == OWN1 else [vin[u, r] for r in range(2)]
                x = [pbuf[u, r] + adds[r] for r in range(2)]
            else:
                x = [pbuf[u, r] for r in range(2)]
            tmp[i] = state[nwin - 1 if kind == OWN1 else 0, level].astype(jnp.float32)
            y, live = [tmp[i, pl.ds(r, spec, stride=2), :] for r in range(2)], stiff_ref[level]
        return (
            jnp.concatenate(x, axis=1), jnp.concatenate(y, axis=1),
            jnp.concatenate([live[0:1], live[1:2]], axis=1),
        )

    def chem(levels, gathered):
        flats, ys, lives = zip(*gathered)
        for s in reversed(range(steps)):
            mat = [mats[s, level] for level in levels]

            def dot(xs):
                return [jnp.dot(a, x.astype(jnp.bfloat16), preferred_element_type=jnp.float32) for a, x in zip(mat, xs)]

            v1 = dot(flats)
            v2 = dot([v * y for v, y in zip(v1, ys)])
            v3 = dot([v * y for v, y in zip(v2, ys)])
            flats = [
                jnp.where(live > s, 0.4 * x + 0.3 * a + 0.2 * b + 0.1 * c, x)
                for x, a, b, c, live in zip(flats, v1, v2, v3, lives)
            ]
        return flats

    def spread(k):
        to = lax.rem(lon + k, n_lon)
        return remote(part.at[to], inbox1.at[lon], s1.at[k], r1.at[lon], (lat, to))

    def spread_in(k):
        source = lax.rem(lon + k, n_lon)
        return source, remote(part.at[source], inbox1.at[source], s1.at[k], r1.at[source], (lat, source))

    def spread2(k):
        to = lax.rem(lat + k, n_lat)
        return remote(turn.at[to], inbox2.at[lat], s2.at[k], r2.at[lat], (to, lon))

    def spread2_in(k):
        source = lax.rem(lat + k, n_lat)
        return source, remote(turn.at[source], inbox2.at[source], s2.at[k], r2.at[source], (source, lon))

    def regions():
        lat8 = part.shape[1]
        contrib = jnp.concatenate([
            em_ref[pl.ds(r, spec, stride=2), :]
            * (lamb[lev, r] + fin[:, r * cols:(r + 1) * cols])
            for r in range(2)], axis=1)
        where_from = jnp.concatenate([reg_ref[0:1, :], reg_ref[1:2, :]], axis=1)
        shape = (n_lon * lat8, 2 * cols)
        column = jnp.concatenate([jnp.full((lat8, 2 * cols), c, jnp.int32) for c in range(n_lon)], axis=0)
        band = lax.broadcasted_iota(jnp.int32, (lat8, 2 * cols), 0)
        band = jnp.concatenate([band] * n_lon, axis=0)
        onehot = (jnp.broadcast_to(where_from, shape) == band * n_lon + column).astype(jnp.float32)
        sums = lax.dot_general(
            onehot, contrib, (((1,), (1,)), ((), ())),
            precision=lax.Precision.HIGHEST, preferred_element_type=jnp.float32)
        for c in range(n_lon):
            part[c] = sums[c * lat8:(c + 1) * lat8]
        for k in range(1, n_lon):
            spread(k).start()

    def regions_turn():
        total = part[lon]
        for k in range(1, n_lon):
            source, copy = spread_in(k)
            copy.wait_recv()
            total = total + inbox1[source]
        for b in range(n_lat):
            turn[b] = total[b:b + 1]
        for k in range(1, n_lat):
            spread2(k).start()

    def regions_end():
        total = turn[lat]
        for k in range(1, n_lat):
            source, copy = spread2_in(k)
            copy.wait_recv()
            total = total + inbox2[source]
        grad_ref[...] = total


    def play(side):
        sent = {}
        for op in plans[side]:
            if op[0] == "chem":
                n, items = op[1:]
                gathered = [gather(side, kind, level, i) for i, (kind, level) in enumerate(items)]
                with jax.named_scope("chem"):
                    flats = chem([level for _, level in items], gathered)
                if n:
                    slots = []
                    for (kind, level), flat in zip(items, flats):
                        u = after_chem(kind, level)
                        for r in range(2):
                            lamb[u, r] = flat[:, r * cols:(r + 1) * cols]
                        slots.append((u, 1 if kind == GHOST else 0))
                    with jax.named_scope("pack"):
                        pack(n, slots)
                    col_copy(n).start()
                    sent[n] = [(OWN0 if kind == OWN1 else GHOST, level) for kind, level in items]
                else:
                    for i, ((kind, level), flat) in enumerate(zip(items, flats)):
                        for r in range(2):
                            tmp[i, pl.ds(r, spec, stride=2), :] = flat[:, r * cols:(r + 1) * cols]
                        outbuf[level] = tmp[i].astype(jnp.bfloat16)
                        if level == 0:
                            fin[...] = flat
                            with jax.named_scope("regions"):
                                regions()
            elif op[0] == "first":
                for level in op[1]:
                    transport(side, 0, level, OWN1, level)
            elif op[0] == "move":
                n = op[1]
                with jax.named_scope("w_col"):
                    col_copy(n).wait_recv()
                if side == 1 and n == 3:
                    mix_out.wait_recv()
                for i, (kind, level) in enumerate(sent[n]):
                    transport(side, n, i, kind, level)
            elif op[0] == "relay":
                w, passed = op[1:]

                @pl.when(passes_on)
                def _(w=w, passed=passed):
                    for level in passed:
                        u = w * lev + level
                        with jax.named_scope("w_relay"):
                            to_relay(u).wait_recv()
                        forward(u).start()
            elif op[0] == "state":
                for k in range(op[1], op[2]):
                    give_state(k)
            else:
                with jax.named_scope("turn"):
                    regions_turn()

        for n in [0] + sorted(sent):
            col_copy(n).wait_send()
        for u in range(2 * lev):
            leaving = own_sends(side, u)
            if leaving is not None:
                when(leaving[1], lambda: leaving[0].wait_send())
        if side == 1:
            @pl.when(sends_ghost)
            def _():
                for level in range(half, lev):
                    ghost_out(level).wait_send()
        else:
            @pl.when(passes_on)
            def _():
                for u in range(2 * lev):
                    if relayed(u % lev, u // lev):
                        forward(u).wait_send()
            stiff_out.wait_send()
            mix_out.wait_send()
            for k in range(half):
                state_out(k).wait_send()

    for load in small[:2]:
        load.wait()
    for r in range(2):
        clon, clat = clon_ref[r:r + 1, :], clat_ref[r:r + 1, :]
        coef[0, 3 * r] = jnp.broadcast_to(1.0 - clon - clat, (8, cols))
        if r == 0:
            coef[0, 1] = jnp.broadcast_to(clat, (8, cols))
        coef[0, 2 + 2 * r] = jnp.broadcast_to(clon, (8, cols))

    adj_load.wait()
    for level in range(lev):
        tmp[level % 4] = adj[level].astype(jnp.float32)
        for r in range(2):
            lamb[level, r] = tmp[level % 4, pl.ds(r, spec, stride=2), :]
    with jax.named_scope("pack"):
        pack(0, [(level, 0) for level in range(lev)])
        corner_end[...] = jnp.concatenate(
            [cout[0], jnp.zeros((cols - spec, cols), jnp.float32)], axis=0).T[:4 * lev]
    with jax.named_scope("w_barrier"):
        pl.semaphore_wait(
            barrier, n_lon - 1 + n_lat - 1 + 2 * has_north.astype(jnp.int32) + 2 * has_south.astype(jnp.int32))

    @pl.when(has_south)
    def _():
        for copy in rows_out:
            copy.start()

    @pl.when(has_north)
    def _():
        for copy in rows_north:
            copy.start()
    rows_west.start()

    @pl.when(even)
    def _():
        send(0, 0)
        send(0, 2)

    @pl.when(odd)
    def _():
        send(1, 0)
    col_copy(0).start()

    @pl.when(has_north)
    def _():
        corner_out.start()

    def give_state(n):
        tmp[n % 4] = state[nwin - 1, half + n].astype(jnp.float32)
        for r in range(2):
            st_out[n, r] = tmp[n % 4, pl.ds(r, spec, stride=2), :]
        state_out(n).start()

    state_loads[nwin - 1].wait()

    @pl.when(even)
    def _():
        for level in range(1, half):
            if level != 2:
                send(0, level)
        give_state(0)
        send(0, half)
        for level in range(half, lev):
            if relayed(level):
                send(0, level)

    @pl.when(odd)
    def _():
        for level in range(1, half):
            send(1, level)

    inv_load.wait()
    with jax.named_scope("mats"):
        for s in range(steps):
            tall[...] = inv[s].astype(jnp.float32)
            for level in range(lev):
                mats[s, level] = tall[pl.ds(level, spec, stride=lev), :].T.astype(jnp.bfloat16)
    for load in small[2:]:
        load.wait()
    for w in range(nwin - 1):
        state_loads[w].wait()
    first_lane = lax.broadcasted_iota(jnp.int32, (8, cols), 1) == 0

    def beside(row, next_row):
        row, next_row = jnp.broadcast_to(row, (8, cols)), jnp.broadcast_to(next_row, (8, cols))
        return after(jnp.where(first_lane, next_row, row))

    @pl.when(has_north)
    def _():
        for copy in rows_out:
            copy.wait_recv()
        c0, o0, n0 = coef[0, 0], coef[0, 2], coef[0, 1]
        for r in range(2):
            clon, clat = nclon[r:r + 1, :], nclat[r:r + 1, :]
            coef[1, 3 * r] = jnp.broadcast_to(1.0 - clon - clat, (8, cols))
            if r == 0:
                coef[1, 1] = jnp.broadcast_to(clat, (8, cols))
            coef[1, 2 + 2 * r] = jnp.broadcast_to(clon, (8, cols))
        below = jnp.broadcast_to(nclat[1:2, :], (8, cols))
        coef[0, 5] = coef[1, 1] * below
        coef[0, 6] = below * (coef[1, 3] + c0)
        coef[0, 7] = below * n0
        coef[0, 8] = below * o0 + coef[1, 4] * beside(nclat[1:2, :], neclat[1:2, :])

    @pl.when(jnp.logical_not(has_north))
    def _():
        for k in range(5, 9):
            coef[0, k] = jnp.zeros((8, cols), jnp.float32)

    rows_west.wait_recv()

    @pl.when(has_south)
    def _():
        for copy in rows_north:
            copy.wait_recv()
        clon, clat = sclon[0:1, :], sclat[0:1, :]
        below = jnp.broadcast_to(clat_ref[1:2, :], (8, cols))
        mixed[0] = coef[0, 1] * below
        mixed[1] = below * (coef[0, 3] + jnp.broadcast_to(1.0 - clon - clat, (8, cols)))
        mixed[2] = below * jnp.broadcast_to(clat, (8, cols))
        mixed[3] = below * jnp.broadcast_to(clon, (8, cols)) + coef[0, 4] * beside(clat_ref[1:2, :], eclat[1:2, :])

    @pl.when(even)
    def _():
        mix_out.start()
        stiff_out.start()
        give_state(1)
        for level in range(half + 1, lev):
            if not relayed(level):
                send(0, level)

    @pl.when(has_south)
    def _():
        with jax.named_scope("w_corner"):
            corner_out.wait_recv()
        corner[...] = jnp.concatenate(
            [corner_in[...], jnp.zeros((cols - 4 * lev, cols), jnp.float32)], axis=0).T[:spec]

    with jax.named_scope("w_col"):
        col_copy(0).wait_recv()

    @pl.when(even)
    def _():
        play(0)

    @pl.when(odd)
    def _():
        play(1)

    rows_west.wait_send()

    @pl.when(has_north)
    def _():
        corner_out.wait_send()
        for copy in rows_north:
            copy.wait_send()

    @pl.when(has_south)
    def _():
        for copy in rows_out:
            copy.wait_send()
    with jax.named_scope("reg_end"):
        regions_end()
    for k in range(1, n_lon):
        spread(k).wait_send()
    for k in range(1, n_lat):
        spread2(k).wait_send()


def finish(held_ref, grad_ref, out_hbm, grad_hbm, sems):
    copies = [
        pltpu.make_async_copy(held_ref, out_hbm, sems.at[0]),
        pltpu.make_async_copy(grad_ref, grad_hbm, sems.at[1]),
    ]
    for copy in copies:
        copy.start()
    for copy in copies:
        copy.wait()


def solution(mesh):
    n_lat, n_lon = mesh.shape["lat"], mesh.shape["lon"]
    assert n_lat % 2 == 0

    def per_device(adjoint_in, state, inverses, courant_lon, courant_lat, emission, region_id, stiffness):
        lev, spec, rows, cols = adjoint_in.shape
        nwin, steps = state.shape[0], inverses.shape[0]
        assert nwin == 2 and rows == 2
        half = lev // 2
        slots = nwin * lev + half
        lat8 = -(-n_lat // 8) * 8
        f32, bf16 = jnp.float32, jnp.bfloat16
        any_space = pl.BlockSpec(memory_space=pl.ANY)
        vmem = pl.BlockSpec(memory_space=pltpu.VMEM)
        dma = pltpu.SemaphoreType.DMA

        def blocks(n):
            return pltpu.VMEM((n, rows, spec, cols), f32)

        out, grad = pl.pallas_call(
            functools.partial(kernel, n_lat, n_lon),
            out_shape=(
                pltpu.VMEM((lev, rows * spec, cols), bf16),
                pltpu.VMEM((1, spec), f32),
            ),
            in_specs=[any_space] * 8,
            out_specs=(vmem, vmem),
            scratch_shapes=[
                pltpu.VMEM((lev, rows * spec, cols), bf16),
                pltpu.VMEM((nwin, lev, rows * spec, cols), bf16),
                pltpu.VMEM((steps, spec * lev, spec), bf16),
                pltpu.VMEM(courant_lon.shape, f32),
                pltpu.VMEM(courant_lat.shape, f32),
                pltpu.VMEM((spec * rows, cols), f32),
                pltpu.VMEM(region_id.shape, jnp.int32),
                pltpu.VMEM(stiffness.shape, jnp.int32),
                pltpu.VMEM((spec * lev, spec), f32),
                pltpu.VMEM(inverses.shape, bf16),
                blocks(slots), blocks(slots), blocks(slots),
                blocks(nwin * lev), blocks(nwin * lev), blocks(half), blocks(half), blocks(half),
                pltpu.VMEM((messages(lev), spec, cols), f32),
                pltpu.VMEM((messages(lev), spec, cols), f32),
                pltpu.VMEM(courant_lon.shape, f32),
                pltpu.VMEM(courant_lat.shape, f32),
                pltpu.VMEM(courant_lat.shape, f32),
                pltpu.VMEM(courant_lon.shape, f32),
                pltpu.VMEM(courant_lat.shape, f32),
                pltpu.VMEM(courant_lat.shape, f32),
                pltpu.VMEM(stiffness.shape, jnp.int32),
                pltpu.VMEM((4 * lev, cols), f32),
                pltpu.VMEM((4 * lev, cols), f32),
                pltpu.VMEM((spec, cols), f32),
                pltpu.VMEM((4, rows * spec, cols), f32),
                pltpu.VMEM((spec, rows * cols), f32),
                pltpu.VMEM((2, 9, 8, cols), f32),
                pltpu.VMEM((4, 8, cols), f32),
                pltpu.VMEM((n_lon, lat8, spec), f32),
                pltpu.VMEM((n_lon, lat8, spec), f32),
                pltpu.VMEM((n_lat, 1, spec), f32),
                pltpu.VMEM((n_lat, 1, spec), f32),
                dma, dma((nwin,)), dma, dma((5,)),
                dma((slots,)), dma((nwin * lev,)), dma((nwin * lev,)), dma((nwin * lev,)), dma((half,)),
                dma((half,)), dma((half,)),
                dma((messages(lev),)), dma((messages(lev),)), dma((8,)), dma((8,)), dma, dma,
                dma((n_lon,)), dma((n_lon,)), dma((n_lat,)), dma((n_lat,)),
            ],
            compiler_params=pltpu.CompilerParams(collective_id=0, has_side_effects=True),
        )(
            adjoint_in.reshape(lev, spec * rows, cols),
            state.reshape(nwin, lev, spec * rows, cols),
            inverses.transpose(0, 2, 1, 3).reshape(steps, spec * lev, spec), courant_lon, courant_lat,
            emission.reshape(spec * rows, cols), region_id, stiffness,
        )
        out, grad = pl.pallas_call(
            finish,
            out_shape=(
                jax.ShapeDtypeStruct(out.shape, bf16),
                jax.ShapeDtypeStruct(grad.shape, f32),
            ),
            in_specs=[any_space] * 2,
            out_specs=(any_space, any_space),
            scratch_shapes=[dma((2,))],
        )(*(pltpu.with_memory_space_constraint(x, pltpu.VMEM) for x in (out, grad)))
        return out.reshape(adjoint_in.shape), grad

    in_specs = (
        P(None, None, "lat", "lon"),
        P(None, None, None, "lat", "lon"),
        P(),
        P("lat", "lon"),
        P("lat", "lon"),
        P(None, "lat", "lon"),
        P("lat", "lon"),
        P(None, "lat", "lon"),
    )
    out_specs = (P(None, None, "lat", "lon"), P(("lat", "lon"), None))
    return jax.shard_map(
        per_device, mesh=mesh, in_specs=in_specs, out_specs=out_specs, check_vma=False
    )
```

```python
import functools

import jax
import jax.numpy as jnp
from jax import lax
from jax.experimental import pallas as pl
from jax.experimental.pallas import tpu as pltpu
from jax.sharding import PartitionSpec as P

MESH = pl.DeviceIdType.MESH
OWN1, OWN0, GHOST = 0, 1, 2


def relayed(level, window=0):
    return level // 2 % 2 == 1 or (window == 1 and level == 1)


def even_order(lev):
    half = lev // 2
    passed = [l for l in range(half) if relayed(l)]
    passed_merged = [l for l in range(half, lev) if relayed(l)]
    return [
        ("first", list(range(half, lev))),
        ("relay", 0, passed[:1]),
        ("chem", 1, [(OWN1, l) for l in range(half, lev)]),
        ("relay", 0, passed[1:]),
        ("state", 2, half - 1),
        ("first", list(range(half))),
        ("chem", 2, [(OWN1, l) for l in range(half) if not relayed(l)]),
        ("relay", 0, passed_merged),
        ("state", half - 1, half),
        ("move", 1),
        ("chem", 3, [(OWN1, l) for l in passed]),
        ("move", 2),
        ("send", [l for l in range(half, lev) if not relayed(l)]),
        ("move", 3),
        ("chem", 0, [(OWN0, l) for l in range(half) if not relayed(l)]),
        ("relay", 1, [l for l in range(half) if relayed(l, 1) and not relayed(l)]),
        ("relay", 1, passed_merged),
        ("chem", 0, [(OWN0, l) for l in passed]),
        ("turn",),
        ("relay", 1, passed),
        ("chem", 0, [(OWN0, l) for l in range(half, lev) if not relayed(l)]),
        ("drain",),
        ("chem", 0, [(OWN0, l) for l in passed_merged]),
    ]


def odd_order(lev):
    half = lev // 2
    assert half == 4
    m = half
    batches = [
        [(OWN1, 0)], [(OWN1, 1)], [(GHOST, m), (OWN1, 2)], [(OWN1, 3), (OWN1, m)],
        [(GHOST, m + 1), (OWN1, m + 1)], [(GHOST, m + 2), (OWN1, m + 2)], [(GHOST, m + 3), (OWN1, m + 3)],
    ]

    def chem(n):
        return ("chem", n, batches[n - 1])

    return [
        ("first", [0]), chem(1), ("first", [1]), chem(2), ("first", [2, m]), chem(3), ("move", 1),
        ("first", [3]), chem(4), ("move", 2), ("first", [m + 1, m + 2, m + 3]), ("move", 3),
        chem(5), ("move", 4),        chem(6), chem(7), ("move", 5),
        ("chem", 0, [(OWN0, 0)]),
        ("move", 6), ("move", 7),
        ("chem", 0, [(OWN0, 1), (OWN0, m)]),
        ("turn",),
        ("chem", 0, [(OWN0, m + 1), (OWN0, m + 2)]),
        ("drain",),
        ("chem", 0, [(OWN0, 2), (OWN0, 3), (OWN0, m + 3)]),
    ]


def messages(lev):
    return 1 + max(op[1] for op in even_order(lev) + odd_order(lev) if op[0] == "chem")


def kernel(
    n_lat, n_lon,
    adj_hbm, state_hbm, inv_hbm, clon_hbm, clat_hbm, em_hbm, reg_hbm, stiff_hbm,
    outbuf, grad_ref,
    adj, state, inv, clon_ref, clat_ref, em_ref, reg_ref, stiff_ref, tall, mats,
    lamb, pbuf, vout, vin, relay, zin, st_out, st_in, cout, cin, nclon, nclat, neclat, sclon, sclat, eclat, gstiff, corner_end, corner_in, corner,
    tmp, fin, coef, mixed, part, inbox1, turn, inbox2,
    adj_sem, state_sem, inv_sem, small_sem, vs, vr, rr, fs, zr, ss, sr, cs, cr, ks, kr, ds, dr, s1, r1, s2, r2,
):
    lev, rows2, cols = adj.shape
    nwin = state.shape[0]
    steps = inv.shape[0]
    spec = rows2 // 2
    half = lev // 2
    lat, lon = lax.axis_index("lat"), lax.axis_index("lon")
    odd = lax.rem(lat, 2) == 1
    even = lax.rem(lat, 2) == 0
    north = jnp.maximum(lat - 1, 0)
    north2 = jnp.maximum(lat - 2, 0)
    south = jnp.minimum(lat + 1, n_lat - 1)
    west = lax.rem(lon + n_lon - 1, n_lon)
    east = lax.rem(lon + 1, n_lon)
    has_north = lat > 0
    has_south = lat < n_lat - 1
    sends_ghost = lat >= 2
    passes_on = lat + 2 < n_lat
    passing = [u for u in range(2 * lev) if relayed(u % lev, u // lev)]
    plans = {0: even_order(lev), 1: odd_order(lev)}

    barrier = pltpu.get_barrier_semaphore()

    def greet(to):
        pl.semaphore_signal(barrier, inc=1, device_id=to, device_id_type=MESH)

    for k in range(1, n_lon):
        greet((lat, lax.rem(lon + k, n_lon)))
    for k in range(1, n_lat):
        greet((lax.rem(lat + k, n_lat), lon))

    @pl.when(has_south)
    def _():
        greet((south, west))
        greet((south, east))

    @pl.when(has_north)
    def _():
        greet((north, east))
        greet((north, west))

    adj_load = pltpu.make_async_copy(adj_hbm, adj, adj_sem)
    small = [
        pltpu.make_async_copy(src, dst, small_sem.at[n])
        for n, (src, dst) in enumerate((
            (clon_hbm, clon_ref), (clat_hbm, clat_ref), (stiff_hbm, stiff_ref),
            (reg_hbm, reg_ref), (em_hbm, em_ref)))
    ]
    state_loads = [
        pltpu.make_async_copy(state_hbm.at[w], state.at[w], state_sem.at[w]) for w in range(nwin)
    ]
    inv_load = pltpu.make_async_copy(inv_hbm, inv, inv_sem)
    for load in small[:2] + [adj_load, state_loads[nwin - 1], inv_load] + small[2:] + state_loads[:nwin - 1]:
        load.start()

    lane = lax.broadcasted_iota(jnp.int32, (spec, cols), 1)

    def slot_of(kind, level):
        return {OWN1: level, OWN0: lev + level, GHOST: 2 * lev + level - half}[kind]

    def after_chem(kind, level):
        return slot_of(OWN0 if kind == OWN1 else GHOST, level)

    def weights(which, names):
        return [coef[which, k, 0:1, :] for k in names]

    def remote(src, dst, send, recv, to):
        return pltpu.make_async_remote_copy(
            src_ref=src, dst_ref=dst, send_sem=send, recv_sem=recv, device_id=to, device_id_type=MESH)

    def leaves(u):
        return (lamb if u < lev else vout).at[u]

    def direct(u):
        return remote(leaves(u), vin.at[u], vs, vr.at[u], (north, lon))

    def to_relay(u):
        n = passing.index(u)
        return remote(leaves(u), relay.at[n], vs, rr.at[n], (north2, lon))

    def forward(u):
        return remote(relay.at[passing.index(u)], vin.at[u], fs, vr.at[u], (south, lon))

    def ghost_out(level):
        u, n = slot_of(GHOST, level), level - half
        return remote(vout.at[u], zin.at[n], vs, zr.at[n], (north2, lon))

    def state_out(n):
        return remote(st_out.at[n], st_in.at[n], ss, sr.at[n], (south, lon))

    def col_copy(n):
        return remote(cout.at[n], cin.at[n], cs, cr.at[n], (lat, west))

    rows_out = [
        remote(clon_ref, nclon, ks.at[0], kr.at[0], (south, lon)),
        remote(clat_ref, nclat, ks.at[1], kr.at[1], (south, lon)),
        remote(clat_ref, neclat, ks.at[2], kr.at[2], (south, west)),
    ]
    rows_north = [
        remote(clon_ref, sclon, ks.at[5], kr.at[5], (north, lon)),
        remote(clat_ref, sclat, ks.at[6], kr.at[6], (north, lon)),
    ]
    rows_west = remote(clat_ref, eclat, ks.at[7], kr.at[7], (lat, west))
    corner_out = remote(corner_end, corner_in, ds, dr, (north, west))
    stiff_out = remote(stiff_ref, gstiff, ks.at[3], kr.at[3], (south, lon))
    mix_out = remote(coef.at[0, pl.ds(5, 4)], coef.at[1, pl.ds(5, 4)], ks.at[4], kr.at[4], (south, lon))

    def after(x):
        return pltpu.roll(x, cols - 1, 1)

    def pack(n, slots):
        message = None
        for i, (u, which) in enumerate(slots):
            c0, n0, o0, c1, o1 = weights(which, range(5))
            row0, row1 = lamb[u, 0], lamb[u, 1]
            new0 = c0 * row0 + n0 * row1 + o0 * after(row0)
            new1 = c1 * row1 + o1 * after(row1)
            for j, x in enumerate((row0, row1, new0, new1)):
                at = 4 * i + j
                message = x if at == 0 else jnp.where(lane == at, pltpu.roll(x, at, 1), message)
        cout[n] = message

    def move(u, which, n, i, combine):
        c0, n0, o0, c1, o1, al, be, ga, de = weights(which, range(9))
        row0, row1, message = lamb[u, 0], lamb[u, 1], cin[n]

        def shift(x, j):
            edge = message if 4 * i + j == 0 else pltpu.roll(message, cols - 4 * i - j, 1)
            return after(jnp.where(lane == 0, edge, x))

        right0, right1 = shift(row0, 0), shift(row1, 1)
        new0 = c0 * row0 + n0 * row1 + o0 * right0
        new1 = c1 * row1 + o1 * right1
        pbuf[u, 0] = c0 * new0 + n0 * new1 + o0 * shift(new0, 2)
        pbuf[u, 1] = c1 * new1 + o1 * shift(new1, 3)
        if not combine:
            return None
        v0 = al * row0
        v1 = be * row0 + ga * row1 + de * right0
        return v0, v1

    def own_sends(side, u):
        level = u % lev
        if side == 1:
            return None if u < lev and level >= half else (direct(u), None)
        return (to_relay(u) if relayed(level, u // lev) else direct(u)), has_north

    def when(condition, do):
        if condition is None:
            do()
        else:
            pl.when(condition)(do)

    def transport(side, n, i, kind, level):
        u = slot_of(kind, level)
        combine = kind != OWN1 or (side == 1 and level >= half)
        with jax.named_scope("move"):
            both = move(u, 1 if kind == GHOST else 0, n, i, combine)
            if combine:
                if side == 1 and kind == OWN0 and level >= half:
                    ghost = slot_of(GHOST, level)
                    both = both[0] + pbuf[ghost, 0], both[1] + pbuf[ghost, 1]
                vout[u, 0], vout[u, 1] = both
        if kind == GHOST:
            when(sends_ghost, lambda: ghost_out(level).start())
        elif kind == OWN0 and not (side == 0 and level >= half and not relayed(level)):
            send(side, u)

    def send(side, u):
        leaving = own_sends(side, u)
        if leaving is not None:
            when(leaving[1], lambda: leaving[0].start())

    def arrived(level):
        al, be, ga, de = [mixed[k, 0:1, :] for k in range(4)]
        row0, row1, message = vin[level, 0], vin[level, 1], corner[...]
        edge = message if level == 0 else pltpu.roll(message, cols - 4 * level, 1)
        right0 = after(jnp.where(lane == 0, edge, row0))
        return al * row0, be * row0 + ga * row1 + de * right0

    def gather(side, kind, level, i):
        u = slot_of(kind, level)
        if kind == GHOST:
            n = level - half
            with jax.named_scope("w_st"):
                state_out(n).wait_recv()
            if n == 0:
                stiff_out.wait_recv()
            x, y, live = [vout[level, r] for r in range(2)], [st_in[n, r] for r in range(2)], gstiff[level]
        else:
            if side == 1:
                @pl.when(has_south)
                def _():
                    with jax.named_scope("w_vin"):
                        direct(u).wait_recv()
                    extra = kind == OWN0 and level >= half
                    if extra:
                        with jax.named_scope("w_z"):
                            ghost_out(level).wait_recv()
                    adds = arrived(level) if kind == OWN1 else [vin[u, r] for r in range(2)]
                    for r in range(2):
                        both = adds[r] + zin[level - half, r] if extra else adds[r]
                        pbuf[u, r] = pbuf[u, r] + both
                x = [pbuf[u, r] for r in range(2)]
            elif kind == OWN0 or level < half:
                with jax.named_scope("w_vin"):
                    direct(u).wait_recv()
                adds = arrived(level) if kind == OWN1 else [vin[u, r] for r in range(2)]
                x = [pbuf[u, r] + adds[r] for r in range(2)]
            else:
                x = [pbuf[u, r] for r in range(2)]
            tmp[i] = state[nwin - 1 if kind == OWN1 else 0, level].astype(jnp.float32)
            y, live = [tmp[i, pl.ds(r, spec, stride=2), :] for r in range(2)], stiff_ref[level]
        return (
            jnp.concatenate(x, axis=1), jnp.concatenate(y, axis=1),
            jnp.concatenate([live[0:1], live[1:2]], axis=1),
        )

    def chem(levels, gathered):
        flats, ys, lives = zip(*gathered)
        for s in reversed(range(steps)):
            mat = [mats[s, level] for level in levels]

            def dot(xs):
                return [jnp.dot(a, x.astype(jnp.bfloat16), preferred_element_type=jnp.float32) for a, x in zip(mat, xs)]

            v1 = dot(flats)
            v2 = dot([v * y for v, y in zip(v1, ys)])
            v3 = dot([v * y for v, y in zip(v2, ys)])
            flats = [
                jnp.where(live > s, 0.4 * x + 0.3 * a + 0.2 * b + 0.1 * c, x)
                for x, a, b, c, live in zip(flats, v1, v2, v3, lives)
            ]
        return flats

    def spread(k):
        to = lax.rem(lon + k, n_lon)
        return remote(part.at[to], inbox1.at[k - 1], s1, r1, (lat, to))

    def spread_all():
        n = pl.ds(0, n_lon - 1)
        return remote(part.at[n], inbox1.at[n], s1, r1, (lat, west))

    def spread2(k):
        to = lax.rem(lat + k, n_lat)
        return remote(turn.at[to], inbox2.at[k - 1], s2, r2, (to, lon))

    def spread2_all():
        n = pl.ds(0, n_lat - 1)
        return remote(turn.at[n], inbox2.at[n], s2, r2, (north, lon))

    def regions():
        lat8 = part.shape[1]
        contrib = jnp.concatenate([
            em_ref[pl.ds(r, spec, stride=2), :]
            * (lamb[lev, r] + fin[:, r * cols:(r + 1) * cols])
            for r in range(2)], axis=1)
        where_from = jnp.concatenate([reg_ref[0:1, :], reg_ref[1:2, :]], axis=1)
        shape = (n_lon * lat8, 2 * cols)
        column = jnp.concatenate([jnp.full((lat8, 2 * cols), c, jnp.int32) for c in range(n_lon)], axis=0)
        band = lax.broadcasted_iota(jnp.int32, (lat8, 2 * cols), 0)
        band = jnp.concatenate([band] * n_lon, axis=0)
        onehot = (jnp.broadcast_to(where_from, shape) == band * n_lon + column).astype(jnp.float32)
        sums = lax.dot_general(
            onehot, contrib, (((1,), (1,)), ((), ())),
            precision=lax.Precision.HIGHEST, preferred_element_type=jnp.float32)
        for c in range(n_lon):
            part[c] = sums[c * lat8:(c + 1) * lat8]
        for k in range(1, n_lon):
            spread(k).start()

    def regions_turn():
        total = part[lon]
        spread_all().wait_recv()
        for k in range(n_lon - 1):
            total = total + inbox1[k]
        for b in range(n_lat):
            turn[b] = total[b:b + 1]
        for k in range(1, n_lat):
            spread2(k).start()

    def regions_end():
        total = turn[lat]
        spread2_all().wait_recv()
        for k in range(n_lat - 1):
            total = total + inbox2[k]
        grad_ref[...] = total

    def drain(side, sent):
        n = 1 + len(sent)
        remote(cout.at[pl.ds(0, n)], cin.at[pl.ds(0, n)], cs, cr.at[0], (lat, west)).wait_send()

        def left(n):
            remote(lamb.at[pl.ds(0, n)], vin.at[pl.ds(0, n)], vs, vr.at[0], (north, lon)).wait_send()

        if side == 1:
            left(lev + half)

            @pl.when(sends_ghost)
            def _():
                left(half)
        else:
            @pl.when(has_north)
            def _():
                left(2 * lev)
            stiff_out.wait_send()
            mix_out.wait_send()
            remote(st_out, st_in, ss, sr.at[0], (south, lon)).wait_send()
        rows_west.wait_send()

        @pl.when(has_north)
        def _():
            corner_out.wait_send()
            for copy in rows_north:
                copy.wait_send()

        @pl.when(has_south)
        def _():
            for copy in rows_out:
                copy.wait_send()

    def play(side):
        sent = {}
        for op in plans[side]:
            if op[0] == "chem":
                n, items = op[1:]
                gathered = [gather(side, kind, level, i) for i, (kind, level) in enumerate(items)]
                with jax.named_scope("chem"):
                    flats = chem([level for _, level in items], gathered)
                if n:
                    slots = []
                    for (kind, level), flat in zip(items, flats):
                        u = after_chem(kind, level)
                        for r in range(2):
                            lamb[u, r] = flat[:, r * cols:(r + 1) * cols]
                        slots.append((u, 1 if kind == GHOST else 0))
                    with jax.named_scope("pack"):
                        pack(n, slots)
                    col_copy(n).start()
                    sent[n] = [(OWN0 if kind == OWN1 else GHOST, level) for kind, level in items]
                else:
                    for i, ((kind, level), flat) in enumerate(zip(items, flats)):
                        for r in range(2):
                            tmp[i, pl.ds(r, spec, stride=2), :] = flat[:, r * cols:(r + 1) * cols]
                        outbuf[level] = tmp[i].astype(jnp.bfloat16)
                        if level == 0:
                            fin[...] = flat
                            with jax.named_scope("regions"):
                                regions()
            elif op[0] == "send":
                for level in op[1]:
                    send(side, lev + level)
            elif op[0] == "first":
                for level in op[1]:
                    transport(side, 0, level, OWN1, level)
            elif op[0] == "move":
                n = op[1]
                with jax.named_scope("w_col"):
                    col_copy(n).wait_recv()
                if side == 1 and n == 3:
                    mix_out.wait_recv()
                for i, (kind, level) in enumerate(sent[n]):
                    transport(side, n, i, kind, level)
            elif op[0] == "relay":
                w, passed = op[1:]

                @pl.when(passes_on)
                def _(w=w, passed=passed):
                    for level in passed:
                        u = w * lev + level
                        with jax.named_scope("w_relay"):
                            to_relay(u).wait_recv()
                        forward(u).start()
            elif op[0] == "state":
                for k in range(op[1], op[2]):
                    give_state(k)
            elif op[0] == "drain":
                drain(side, sent)
            else:
                with jax.named_scope("turn"):
                    regions_turn()

        if side == 0:
            @pl.when(passes_on)
            def _():
                remote(relay, relay, fs, rr.at[0], (south, lon)).wait_send()

    for load in small[:2]:
        load.wait()
    for r in range(2):
        clon, clat = clon_ref[r:r + 1, :], clat_ref[r:r + 1, :]
        coef[0, 3 * r] = jnp.broadcast_to(1.0 - clon - clat, (8, cols))
        if r == 0:
            coef[0, 1] = jnp.broadcast_to(clat, (8, cols))
        coef[0, 2 + 2 * r] = jnp.broadcast_to(clon, (8, cols))

    adj_load.wait()
    small[2].wait()
    for level in range(lev):
        tmp[level % 4] = adj[level].astype(jnp.float32)
        for r in range(2):
            lamb[level, r] = tmp[level % 4, pl.ds(r, spec, stride=2), :]
    with jax.named_scope("pack"):
        pack(0, [(level, 0) for level in range(lev)])
        corner_end[...] = jnp.concatenate(
            [cout[0], jnp.zeros((cols - spec, cols), jnp.float32)], axis=0).T[:4 * lev]
    with jax.named_scope("w_barrier"):
        pl.semaphore_wait(
            barrier, n_lon - 1 + n_lat - 1 + 2 * has_north.astype(jnp.int32) + 2 * has_south.astype(jnp.int32))

    @pl.when(has_south)
    def _():
        for copy in rows_out:
            copy.start()

    @pl.when(has_north)
    def _():
        for copy in rows_north:
            copy.start()
    rows_west.start()

    @pl.when(even)
    def _():
        stiff_out.start()
        when(has_north, lambda: corner_out.start())
        send(0, 0)
        send(0, 2)

    @pl.when(odd)
    def _():
        corner_out.start()
        send(1, 0)
    col_copy(0).start()

    def give_state(n, condition=None):
        def do():
            tmp[n % 4] = state[nwin - 1, half + n].astype(jnp.float32)
            for r in range(2):
                st_out[n, r] = tmp[n % 4, pl.ds(r, spec, stride=2), :]
            state_out(n).start()

        when(condition, do)

    state_loads[nwin - 1].wait()

    @pl.when(even)
    def _():
        for level in range(1, half):
            if level != 2:
                send(0, level)
        give_state(0)
        give_state(1, jnp.logical_not(has_north))
        send(0, half)
        for level in range(half, lev):
            if relayed(level):
                send(0, level)

    @pl.when(odd)
    def _():
        for level in range(1, half):
            send(1, level)

    inv_load.wait()
    with jax.named_scope("mats"):
        for s in range(steps):
            tall[...] = inv[s].astype(jnp.float32)
            for level in range(lev):
                mats[s, level] = tall[pl.ds(level, spec, stride=lev), :].T.astype(jnp.bfloat16)
    for load in small[3:]:
        load.wait()
    for w in range(nwin - 1):
        state_loads[w].wait()
    first_lane = lax.broadcasted_iota(jnp.int32, (8, cols), 1) == 0

    def beside(row, next_row):
        row, next_row = jnp.broadcast_to(row, (8, cols)), jnp.broadcast_to(next_row, (8, cols))
        return after(jnp.where(first_lane, next_row, row))

    @pl.when(has_north)
    def _():
        for copy in rows_out:
            copy.wait_recv()
        c0, o0, n0 = coef[0, 0], coef[0, 2], coef[0, 1]
        for r in range(2):
            clon, clat = nclon[r:r + 1, :], nclat[r:r + 1, :]
            coef[1, 3 * r] = jnp.broadcast_to(1.0 - clon - clat, (8, cols))
            if r == 0:
                coef[1, 1] = jnp.broadcast_to(clat, (8, cols))
            coef[1, 2 + 2 * r] = jnp.broadcast_to(clon, (8, cols))
        below = jnp.broadcast_to(nclat[1:2, :], (8, cols))
        coef[0, 5] = coef[1, 1] * below
        coef[0, 6] = below * (coef[1, 3] + c0)
        coef[0, 7] = below * n0
        coef[0, 8] = below * o0 + coef[1, 4] * beside(nclat[1:2, :], neclat[1:2, :])

    @pl.when(jnp.logical_not(has_north))
    def _():
        for k in range(5, 9):
            coef[0, k] = jnp.zeros((8, cols), jnp.float32)

    rows_west.wait_recv()

    @pl.when(has_south)
    def _():
        for copy in rows_north:
            copy.wait_recv()
        clon, clat = sclon[0:1, :], sclat[0:1, :]
        below = jnp.broadcast_to(clat_ref[1:2, :], (8, cols))
        mixed[0] = coef[0, 1] * below
        mixed[1] = below * (coef[0, 3] + jnp.broadcast_to(1.0 - clon - clat, (8, cols)))
        mixed[2] = below * jnp.broadcast_to(clat, (8, cols))
        mixed[3] = below * jnp.broadcast_to(clon, (8, cols)) + coef[0, 4] * beside(clat_ref[1:2, :], eclat[1:2, :])

    @pl.when(even)
    def _():
        mix_out.start()
        give_state(1, has_north)
        for level in range(half + 1, lev):
            if not relayed(level):
                send(0, level)

    @pl.when(has_south)
    def _():
        with jax.named_scope("w_corner"):
            corner_out.wait_recv()
        corner[...] = jnp.concatenate(
            [corner_in[...], jnp.zeros((cols - 4 * lev, cols), jnp.float32)], axis=0).T[:spec]

    with jax.named_scope("w_col"):
        col_copy(0).wait_recv()

    @pl.when(even)
    def _():
        play(0)

    @pl.when(odd)
    def _():
        play(1)

    with jax.named_scope("reg_end"):
        regions_end()
    spread_all().wait_send()
    spread2_all().wait_send()


def finish(held_ref, grad_ref, out_hbm, grad_hbm, sems):
    copies = [
        pltpu.make_async_copy(held_ref, out_hbm, sems.at[0]),
        pltpu.make_async_copy(grad_ref, grad_hbm, sems.at[1]),
    ]
    for copy in copies:
        copy.start()
    for copy in copies:
        copy.wait()


def solution(mesh):
    n_lat, n_lon = mesh.shape["lat"], mesh.shape["lon"]
    assert n_lat % 2 == 0

    def per_device(adjoint_in, state, inverses, courant_lon, courant_lat, emission, region_id, stiffness):
        lev, spec, rows, cols = adjoint_in.shape
        nwin, steps = state.shape[0], inverses.shape[0]
        assert nwin == 2 and rows == 2
        half = lev // 2
        slots = nwin * lev + half
        passed = sum(relayed(level, w) for level in range(lev) for w in range(nwin))
        lat8 = -(-n_lat // 8) * 8
        f32, bf16 = jnp.float32, jnp.bfloat16
        any_space = pl.BlockSpec(memory_space=pl.ANY)
        vmem = pl.BlockSpec(memory_space=pltpu.VMEM)
        dma = pltpu.SemaphoreType.DMA

        def blocks(n):
            return pltpu.VMEM((n, rows, spec, cols), f32)

        out, grad = pl.pallas_call(
            functools.partial(kernel, n_lat, n_lon),
            out_shape=(
                pltpu.VMEM((lev, rows * spec, cols), bf16),
                pltpu.VMEM((1, spec), f32),
            ),
            in_specs=[any_space] * 8,
            out_specs=(vmem, vmem),
            scratch_shapes=[
                pltpu.VMEM((lev, rows * spec, cols), bf16),
                pltpu.VMEM((nwin, lev, rows * spec, cols), bf16),
                pltpu.VMEM((steps, spec * lev, spec), bf16),
                pltpu.VMEM(courant_lon.shape, f32),
                pltpu.VMEM(courant_lat.shape, f32),
                pltpu.VMEM((spec * rows, cols), f32),
                pltpu.VMEM(region_id.shape, jnp.int32),
                pltpu.VMEM(stiffness.shape, jnp.int32),
                pltpu.VMEM((spec * lev, spec), f32),
                pltpu.VMEM(inverses.shape, bf16),
                blocks(slots), blocks(slots), blocks(slots),
                blocks(nwin * lev), blocks(passed), blocks(half), blocks(half), blocks(half),
                pltpu.VMEM((messages(lev), spec, cols), f32),
                pltpu.VMEM((messages(lev), spec, cols), f32),
                pltpu.VMEM(courant_lon.shape, f32),
                pltpu.VMEM(courant_lat.shape, f32),
                pltpu.VMEM(courant_lat.shape, f32),
                pltpu.VMEM(courant_lon.shape, f32),
                pltpu.VMEM(courant_lat.shape, f32),
                pltpu.VMEM(courant_lat.shape, f32),
                pltpu.VMEM(stiffness.shape, jnp.int32),
                pltpu.VMEM((4 * lev, cols), f32),
                pltpu.VMEM((4 * lev, cols), f32),
                pltpu.VMEM((spec, cols), f32),
                pltpu.VMEM((4, rows * spec, cols), f32),
                pltpu.VMEM((spec, rows * cols), f32),
                pltpu.VMEM((2, 9, 8, cols), f32),
                pltpu.VMEM((4, 8, cols), f32),
                pltpu.VMEM((n_lon, lat8, spec), f32),
                pltpu.VMEM((n_lon, lat8, spec), f32),
                pltpu.VMEM((n_lat, 1, spec), f32),
                pltpu.VMEM((n_lat, 1, spec), f32),
                dma, dma((nwin,)), dma, dma((5,)),
                dma, dma((nwin * lev,)), dma((passed,)), dma, dma((half,)),
                dma, dma((half,)),
                dma, dma((messages(lev),)), dma((8,)), dma((8,)), dma, dma,
                dma, dma, dma, dma,
            ],
            compiler_params=pltpu.CompilerParams(collective_id=0, has_side_effects=True),
        )(
            adjoint_in.reshape(lev, spec * rows, cols),
            state.reshape(nwin, lev, spec * rows, cols),
            inverses.transpose(0, 2, 1, 3).reshape(steps, spec * lev, spec), courant_lon, courant_lat,
            emission.reshape(spec * rows, cols), region_id, stiffness,
        )
        out, grad = pl.pallas_call(
            finish,
            out_shape=(
                jax.ShapeDtypeStruct(out.shape, bf16),
                jax.ShapeDtypeStruct(grad.shape, f32),
            ),
            in_specs=[any_space] * 2,
            out_specs=(any_space, any_space),
            scratch_shapes=[dma((2,))],
        )(*(pltpu.with_memory_space_constraint(x, pltpu.VMEM) for x in (out, grad)))
        return out.reshape(adjoint_in.shape), grad

    in_specs = (
        P(None, None, "lat", "lon"),
        P(None, None, None, "lat", "lon"),
        P(),
        P("lat", "lon"),
        P("lat", "lon"),
        P(None, "lat", "lon"),
        P("lat", "lon"),
        P(None, "lat", "lon"),
    )
    out_specs = (P(None, None, "lat", "lon"), P(("lat", "lon"), None))
    return jax.shard_map(
        per_device, mesh=mesh, in_specs=in_specs, out_specs=out_specs, check_vma=False
    )
```

```python
import functools

import jax
import jax.numpy as jnp
from jax import lax
from jax.experimental import pallas as pl
from jax.experimental.pallas import tpu as pltpu
from jax.sharding import PartitionSpec as P

MESH = pl.DeviceIdType.MESH
OWN1, OWN0, GHOST = 0, 1, 2


def relayed(level, window=0):
    return level // 2 % 2 == 1 or (window == 1 and level == 1)


def even_order(lev):
    half = lev // 2
    passed = [l for l in range(half) if relayed(l)]
    passed_merged = [l for l in range(half, lev) if relayed(l)]
    return [
        ("first", list(range(half + 1, lev))),
        ("relay", 0, passed[:1]),
        ("chem", 1, [(OWN1, l) for l in range(half + 1, lev)]),
        ("relay", 0, passed[1:]),
        ("state", 2, half - 1),
        ("first", list(range(half + 1))),
        ("chem", 2, [(OWN1, l) for l in range(half) if not relayed(l)]),
        ("relay", 0, passed_merged),
        ("state", half - 1, half),
        ("move", 1),
        ("chem", 3, [(OWN1, l) for l in passed + [half]]),
        ("move", 2),
        ("send", [l for l in range(half + 1, lev) if not relayed(l)]),
        ("relay", 1, passed_merged),
        ("move", 3),
        ("chem", 0, [(OWN0, l) for l in range(half) if not relayed(l)]),
        ("relay", 1, [l for l in range(half) if relayed(l, 1) and not relayed(l)]),
        ("relay", 1, passed),
        ("chem", 0, [(OWN0, l) for l in passed]),
        ("turn",),
        ("chem", 0, [(OWN0, l) for l in range(half, lev) if not relayed(l)]),
        ("drain",),
        ("chem", 0, [(OWN0, l) for l in passed_merged]),
    ]


def odd_order(lev):
    half = lev // 2
    assert half == 4
    m = half
    batches = [
        [(OWN1, 0)], [(OWN1, 1)], [(GHOST, m), (OWN1, 2)], [(OWN1, 3), (OWN1, m)],
        [(GHOST, m + 1), (OWN1, m + 1)], [(GHOST, m + 2), (OWN1, m + 2)], [(GHOST, m + 3), (OWN1, m + 3)],
    ]

    def chem(n):
        return ("chem", n, batches[n - 1])

    return [
        ("first", [0]), chem(1), ("first", [1]), chem(2), ("first", [2, m]), chem(3), ("move", 1),
        ("first", [3]), chem(4), ("move", 2), ("first", [m + 1, m + 2, m + 3]), ("move", 3),
        chem(5), ("move", 4),        chem(6), chem(7), ("move", 5),
        ("chem", 0, [(OWN0, 0)]),
        ("move", 6), ("move", 7),
        ("chem", 0, [(OWN0, 1), (OWN0, m)]),
        ("turn",),
        ("chem", 0, [(OWN0, m + 1), (OWN0, m + 2)]),
        ("drain",),
        ("chem", 0, [(OWN0, 2), (OWN0, 3), (OWN0, m + 3)]),
    ]


def messages(lev):
    return 1 + max(op[1] for op in even_order(lev) + odd_order(lev) if op[0] == "chem")


def kernel(
    n_lat, n_lon,
    adj_hbm, state_hbm, inv_hbm, clon_hbm, clat_hbm, em_hbm, reg_hbm, stiff_hbm,
    outbuf, grad_ref,
    adj, state, inv, clon_ref, clat_ref, em_ref, reg_ref, stiff_ref, tall, mats, both,
    lamb, pbuf, vout, vin, relay, zin, st_out, st_in, cout, cin, nclon, nclat, neclat, sclon, sclat, eclat, gstiff, corner_end, corner_in, corner,
    tmp, fin, coef, mixed, part, inbox1, turn, inbox2,
    adj_sem, state_sem, inv_sem, small_sem, vs, vr, rr, fs, zr, ss, sr, cs, cr, ks, kr, ds, dr, s1, r1, s2, r2,
):
    lev, rows2, cols = adj.shape
    nwin = state.shape[0]
    steps = inv.shape[0]
    spec = rows2 // 2
    half = lev // 2
    lat, lon = lax.axis_index("lat"), lax.axis_index("lon")
    odd = lax.rem(lat, 2) == 1
    even = lax.rem(lat, 2) == 0
    north = jnp.maximum(lat - 1, 0)
    north2 = jnp.maximum(lat - 2, 0)
    south = jnp.minimum(lat + 1, n_lat - 1)
    west = lax.rem(lon + n_lon - 1, n_lon)
    east = lax.rem(lon + 1, n_lon)
    has_north = lat > 0
    has_south = lat < n_lat - 1
    sends_ghost = lat >= 2
    passes_on = lat + 2 < n_lat
    first_pair = lat < 2
    later_pair = lat >= 2
    passing = [u for u in range(2 * lev) if relayed(u % lev, u // lev)]
    plans = {0: even_order(lev), 1: odd_order(lev)}

    barrier = pltpu.get_barrier_semaphore()

    def greet(to):
        pl.semaphore_signal(barrier, inc=1, device_id=to, device_id_type=MESH)

    for k in range(1, n_lon):
        greet((lat, lax.rem(lon + k, n_lon)))
    for k in range(1, n_lat):
        greet((lax.rem(lat + k, n_lat), lon))

    @pl.when(has_south)
    def _():
        greet((south, west))
        greet((south, east))

    @pl.when(has_north)
    def _():
        greet((north, east))
        greet((north, west))

    adj_load = pltpu.make_async_copy(adj_hbm, adj, adj_sem)
    small = [
        pltpu.make_async_copy(src, dst, small_sem.at[n])
        for n, (src, dst) in enumerate((
            (clon_hbm, clon_ref), (clat_hbm, clat_ref), (stiff_hbm, stiff_ref),
            (reg_hbm, reg_ref), (em_hbm, em_ref)))
    ]
    state_loads = [
        pltpu.make_async_copy(state_hbm.at[w], state.at[w], state_sem.at[w]) for w in range(nwin)
    ]
    inv_load = pltpu.make_async_copy(inv_hbm, inv, inv_sem)
    for load in small[:2] + [adj_load, state_loads[nwin - 1], inv_load] + small[2:] + state_loads[:nwin - 1]:
        load.start()

    lane = lax.broadcasted_iota(jnp.int32, (spec, cols), 1)

    def slot_of(kind, level):
        return {OWN1: level, OWN0: lev + level, GHOST: 2 * lev + level - half}[kind]

    def after_chem(kind, level):
        return slot_of(OWN0 if kind == OWN1 else GHOST, level)

    def weights(which, names):
        return [coef[which, k, 0:1, :] for k in names]

    def remote(src, dst, send, recv, to):
        return pltpu.make_async_remote_copy(
            src_ref=src, dst_ref=dst, send_sem=send, recv_sem=recv, device_id=to, device_id_type=MESH)

    def leaves(u):
        return (lamb if u < lev else vout).at[u]

    def direct(u):
        return remote(leaves(u), vin.at[u], vs, vr.at[u], (north, lon))

    def to_relay(u):
        n = passing.index(u)
        return remote(leaves(u), relay.at[n], vs, rr.at[n], (north2, lon))

    def forward(u):
        return remote(relay.at[passing.index(u)], vin.at[u], fs, vr.at[u], (south, lon))

    def ghost_out(level):
        u, n = slot_of(GHOST, level), level - half
        return remote(vout.at[u], zin.at[n], vs, zr.at[n], (north2, lon))

    def state_out(n):
        return remote(st_out.at[n], st_in.at[n], ss, sr.at[n], (south, lon))

    def col_copy(n):
        return remote(cout.at[n], cin.at[n], cs, cr.at[n], (lat, west))

    rows_out = [
        remote(clon_ref, nclon, ks.at[0], kr.at[0], (south, lon)),
        remote(clat_ref, nclat, ks.at[1], kr.at[1], (south, lon)),
        remote(clat_ref, neclat, ks.at[2], kr.at[2], (south, west)),
    ]
    rows_north = [
        remote(clon_ref, sclon, ks.at[5], kr.at[5], (north, lon)),
        remote(clat_ref, sclat, ks.at[6], kr.at[6], (north, lon)),
    ]
    rows_west = remote(clat_ref, eclat, ks.at[7], kr.at[7], (lat, west))
    corner_out = remote(corner_end, corner_in, ds, dr, (north, west))
    stiff_out = remote(stiff_ref, gstiff, ks.at[3], kr.at[3], (south, lon))
    mix_out = remote(coef.at[0, pl.ds(5, 4)], coef.at[1, pl.ds(5, 4)], ks.at[4], kr.at[4], (south, lon))

    def after(x):
        return pltpu.roll(x, cols - 1, 1)

    def pack(n, slots):
        message = None
        for i, (u, which) in enumerate(slots):
            c0, n0, o0, c1, o1 = weights(which, range(5))
            row0, row1 = lamb[u, 0], lamb[u, 1]
            new0 = c0 * row0 + n0 * row1 + o0 * after(row0)
            new1 = c1 * row1 + o1 * after(row1)
            for j, x in enumerate((row0, row1, new0, new1)):
                at = 4 * i + j
                message = x if at == 0 else jnp.where(lane == at, pltpu.roll(x, at, 1), message)
        cout[n] = message

    def move(u, which, n, i, combine):
        c0, n0, o0, c1, o1, al, be, ga, de = weights(which, range(9))
        row0, row1, message = lamb[u, 0], lamb[u, 1], cin[n]

        def shift(x, j):
            edge = message if 4 * i + j == 0 else pltpu.roll(message, cols - 4 * i - j, 1)
            return after(jnp.where(lane == 0, edge, x))

        right0, right1 = shift(row0, 0), shift(row1, 1)
        new0 = c0 * row0 + n0 * row1 + o0 * right0
        new1 = c1 * row1 + o1 * right1
        pbuf[u, 0] = c0 * new0 + n0 * new1 + o0 * shift(new0, 2)
        pbuf[u, 1] = c1 * new1 + o1 * shift(new1, 3)
        if not combine:
            return None
        v0 = al * row0
        v1 = be * row0 + ga * row1 + de * right0
        return v0, v1

    def own_sends(side, u):
        level = u % lev
        if side == 1:
            if u == half:
                return direct(u), later_pair
            return None if u < lev and level > half else (direct(u), None)
        return (to_relay(u) if relayed(level, u // lev) else direct(u)), has_north

    def when(condition, do):
        if condition is None:
            do()
        else:
            pl.when(condition)(do)

    def transport(side, n, i, kind, level):
        u = slot_of(kind, level)
        combine = kind != OWN1 or (side == 1 and level >= half)
        with jax.named_scope("move"):
            both = move(u, 1 if kind == GHOST else 0, n, i, combine)
            if combine:
                merged = side == 1 and kind == OWN0 and level >= half
                if merged and level > half:
                    ghost = slot_of(GHOST, level)
                    both = both[0] + pbuf[ghost, 0], both[1] + pbuf[ghost, 1]
                vout[u, 0], vout[u, 1] = both
                if merged and level == half:
                    @pl.when(first_pair)
                    def _():
                        ghost = slot_of(GHOST, level)
                        for r in range(2):
                            vout[u, r] = vout[u, r] + pbuf[ghost, r]
        if kind == GHOST:
            if level > half:
                when(sends_ghost, lambda: ghost_out(level).start())
        elif kind == OWN0 and not (side == 0 and level > half and not relayed(level)):
            send(side, u)

    def send(side, u):
        leaving = own_sends(side, u)
        if leaving is not None:
            when(leaving[1], lambda: leaving[0].start())

    def arrived(level):
        al, be, ga, de = [mixed[k, 0:1, :] for k in range(4)]
        row0, row1, message = vin[level, 0], vin[level, 1], corner[...]
        edge = message if level == 0 else pltpu.roll(message, cols - 4 * level, 1)
        right0 = after(jnp.where(lane == 0, edge, row0))
        return al * row0, be * row0 + ga * row1 + de * right0

    def gather(side, kind, level, i):
        u = slot_of(kind, level)
        if kind == GHOST:
            n = level - half
            with jax.named_scope("w_st"):
                when(None if n else first_pair, lambda: state_out(n).wait_recv())
            if n == 0:
                stiff_out.wait_recv()
            x, y, live = [vout[level, r] for r in range(2)], [st_in[n, r] for r in range(2)], gstiff[level]
        else:
            if side == 1:
                @pl.when(has_south)
                def _():
                    with jax.named_scope("w_vin"):
                        direct(u).wait_recv()
                    extra = kind == OWN0 and level > half
                    if extra:
                        with jax.named_scope("w_z"):
                            ghost_out(level).wait_recv()
                    adds = arrived(level) if kind == OWN1 else [vin[u, r] for r in range(2)]
                    for r in range(2):
                        both = adds[r] + zin[level - half, r] if extra else adds[r]
                        pbuf[u, r] = pbuf[u, r] + both
                x = [pbuf[u, r] for r in range(2)]
            elif kind == OWN0 or level < half:
                with jax.named_scope("w_vin"):
                    direct(u).wait_recv()
                adds = arrived(level) if kind == OWN1 else [vin[u, r] for r in range(2)]
                x = [pbuf[u, r] + adds[r] for r in range(2)]
            else:
                if level == half:
                    @pl.when(later_pair)
                    def _():
                        with jax.named_scope("w_vin"):
                            direct(u).wait_recv()
                        adds = arrived(level)
                        for r in range(2):
                            pbuf[u, r] = pbuf[u, r] + adds[r]
                x = [pbuf[u, r] for r in range(2)]
            tmp[i] = state[nwin - 1 if kind == OWN1 else 0, level].astype(jnp.float32)
            y, live = [tmp[i, pl.ds(r, spec, stride=2), :] for r in range(2)], stiff_ref[level]
        return (
            jnp.concatenate(x, axis=1), jnp.concatenate(y, axis=1),
            jnp.concatenate([live[0:1], live[1:2]], axis=1),
        )

    def chem(levels, gathered):
        flats, ys, lives = zip(*gathered)

        def dot(mat, xs):
            return [
                jnp.dot(a, x.astype(jnp.bfloat16), preferred_element_type=jnp.float32) for a, x in zip(mat, xs)]

        v1 = dot([mats[steps - 1, level] for level in levels], flats)
        for s in reversed(range(steps)):
            mat = [mats[s, level] for level in levels]
            v2 = dot(mat, [v * y for v, y in zip(v1, ys)])
            r2 = [v * y for v, y in zip(v2, ys)]
            v3 = dot(mat, r2)
            some = [0.4 * x + 0.3 * a + 0.2 * b for x, a, b in zip(flats, v1, v2)]
            if s:
                v1 = [
                    a + b for a, b in zip(
                        dot([mats[s - 1, level] for level in levels],
                            [jnp.where(live > s, x, flat) for x, flat, live in zip(some, flats, lives)]),
                        dot([both[s - 1, level] for level in levels],
                            [jnp.where(live > s, r, 0.0) for r, live in zip(r2, lives)]))]
            flats = [
                jnp.where(live > s, x + 0.1 * c, flat) for x, c, flat, live in zip(some, v3, flats, lives)
            ]
        return flats

    def spread(k):
        to = lax.rem(lon + k, n_lon)
        return remote(part.at[to], inbox1.at[k - 1], s1, r1, (lat, to))

    def spread_all():
        n = pl.ds(0, n_lon - 1)
        return remote(part.at[n], inbox1.at[n], s1, r1, (lat, west))

    def spread2(k):
        to = lax.rem(lat + k, n_lat)
        return remote(turn.at[to], inbox2.at[k - 1], s2, r2, (to, lon))

    def spread2_all():
        n = pl.ds(0, n_lat - 1)
        return remote(turn.at[n], inbox2.at[n], s2, r2, (north, lon))

    def regions():
        lat8 = part.shape[1]
        contrib = jnp.concatenate([
            em_ref[pl.ds(r, spec, stride=2), :]
            * (lamb[lev, r] + fin[:, r * cols:(r + 1) * cols])
            for r in range(2)], axis=1)
        where_from = jnp.concatenate([reg_ref[0:1, :], reg_ref[1:2, :]], axis=1)
        shape = (n_lon * lat8, 2 * cols)
        column = jnp.concatenate([jnp.full((lat8, 2 * cols), c, jnp.int32) for c in range(n_lon)], axis=0)
        band = lax.broadcasted_iota(jnp.int32, (lat8, 2 * cols), 0)
        band = jnp.concatenate([band] * n_lon, axis=0)
        onehot = (jnp.broadcast_to(where_from, shape) == band * n_lon + column).astype(jnp.float32)
        sums = lax.dot_general(
            onehot, contrib, (((1,), (1,)), ((), ())),
            precision=lax.Precision.HIGHEST, preferred_element_type=jnp.float32)
        for c in range(n_lon):
            part[c] = sums[c * lat8:(c + 1) * lat8]
        for k in range(1, n_lon):
            spread(k).start()

    def regions_turn():
        total = part[lon]
        spread_all().wait_recv()
        for k in range(n_lon - 1):
            total = total + inbox1[k]
        for b in range(n_lat):
            turn[b] = total[b:b + 1]
        for k in range(1, n_lat):
            spread2(k).start()

    def regions_end():
        total = turn[lat]
        spread2_all().wait_recv()
        for k in range(n_lat - 1):
            total = total + inbox2[k]
        grad_ref[...] = total

    def drain(side, sent):
        n = 1 + len(sent)
        remote(cout.at[pl.ds(0, n)], cin.at[pl.ds(0, n)], cs, cr.at[0], (lat, west)).wait_send()

        def left(n):
            remote(lamb.at[pl.ds(0, n)], vin.at[pl.ds(0, n)], vs, vr.at[0], (north, lon)).wait_send()

        if side == 1:
            left(lev + half)

            @pl.when(later_pair)
            def _():
                left(1)

            @pl.when(sends_ghost)
            def _():
                left(half - 1)
        else:
            @pl.when(has_north)
            def _():
                left(2 * lev)
            stiff_out.wait_send()
            mix_out.wait_send()
            n = pl.ds(0, half - 1)
            remote(st_out.at[n], st_in.at[n], ss, sr.at[0], (south, lon)).wait_send()
            when(first_pair, lambda: state_out(0).wait_send())
        rows_west.wait_send()

        @pl.when(has_north)
        def _():
            corner_out.wait_send()
            for copy in rows_north:
                copy.wait_send()

        @pl.when(has_south)
        def _():
            for copy in rows_out:
                copy.wait_send()

    def play(side):
        sent = {}
        for op in plans[side]:
            if op[0] == "chem":
                n, items = op[1:]
                gathered = [gather(side, kind, level, i) for i, (kind, level) in enumerate(items)]
                with jax.named_scope("chem"):
                    flats = chem([level for _, level in items], gathered)
                if n:
                    slots = []
                    for (kind, level), flat in zip(items, flats):
                        u = after_chem(kind, level)
                        for r in range(2):
                            lamb[u, r] = flat[:, r * cols:(r + 1) * cols]
                        slots.append((u, 1 if kind == GHOST else 0))
                    with jax.named_scope("pack"):
                        pack(n, slots)
                    col_copy(n).start()
                    sent[n] = [(OWN0 if kind == OWN1 else GHOST, level) for kind, level in items]
                else:
                    for i, ((kind, level), flat) in enumerate(zip(items, flats)):
                        for r in range(2):
                            tmp[i, pl.ds(r, spec, stride=2), :] = flat[:, r * cols:(r + 1) * cols]
                        outbuf[level] = tmp[i].astype(jnp.bfloat16)
                        if level == 0:
                            fin[...] = flat
                            with jax.named_scope("regions"):
                                regions()
            elif op[0] == "send":
                for level in op[1]:
                    send(side, lev + level)
            elif op[0] == "first":
                for level in op[1]:
                    transport(side, 0, level, OWN1, level)
            elif op[0] == "move":
                n = op[1]
                with jax.named_scope("w_col"):
                    col_copy(n).wait_recv()
                if side == 1 and n == 3:
                    mix_out.wait_recv()
                for i, (kind, level) in enumerate(sent[n]):
                    transport(side, n, i, kind, level)
            elif op[0] == "relay":
                w, passed = op[1:]

                @pl.when(passes_on)
                def _(w=w, passed=passed):
                    for level in passed:
                        u = w * lev + level
                        with jax.named_scope("w_relay"):
                            to_relay(u).wait_recv()
                        forward(u).start()
            elif op[0] == "state":
                for k in range(op[1], op[2]):
                    give_state(k)
            elif op[0] == "drain":
                drain(side, sent)
            else:
                with jax.named_scope("turn"):
                    regions_turn()

        if side == 0:
            @pl.when(passes_on)
            def _():
                remote(relay, relay, fs, rr.at[0], (south, lon)).wait_send()

    for load in small[:2]:
        load.wait()
    for r in range(2):
        clon, clat = clon_ref[r:r + 1, :], clat_ref[r:r + 1, :]
        coef[0, 3 * r] = jnp.broadcast_to(1.0 - clon - clat, (8, cols))
        if r == 0:
            coef[0, 1] = jnp.broadcast_to(clat, (8, cols))
        coef[0, 2 + 2 * r] = jnp.broadcast_to(clon, (8, cols))

    adj_load.wait()
    small[2].wait()
    for level in range(lev):
        tmp[level % 4] = adj[level].astype(jnp.float32)
        for r in range(2):
            lamb[level, r] = tmp[level % 4, pl.ds(r, spec, stride=2), :]
    with jax.named_scope("pack"):
        pack(0, [(level, 0) for level in range(lev)])
        corner_end[...] = jnp.concatenate(
            [cout[0], jnp.zeros((cols - spec, cols), jnp.float32)], axis=0).T[:4 * lev]
    with jax.named_scope("w_barrier"):
        pl.semaphore_wait(
            barrier, n_lon - 1 + n_lat - 1 + 2 * has_north.astype(jnp.int32) + 2 * has_south.astype(jnp.int32))

    @pl.when(has_south)
    def _():
        for copy in rows_out:
            copy.start()

    @pl.when(has_north)
    def _():
        for copy in rows_north:
            copy.start()
    rows_west.start()

    @pl.when(even)
    def _():
        stiff_out.start()
        when(has_north, lambda: corner_out.start())
        send(0, 0)
        send(0, 2)

    @pl.when(odd)
    def _():
        corner_out.start()
        send(1, 0)
    col_copy(0).start()

    def give_state(n, condition=None):
        def do():
            tmp[n % 4] = state[nwin - 1, half + n].astype(jnp.float32)
            for r in range(2):
                st_out[n, r] = tmp[n % 4, pl.ds(r, spec, stride=2), :]
            state_out(n).start()

        when(condition, do)

    state_loads[nwin - 1].wait()

    @pl.when(even)
    def _():
        for level in range(1, half):
            if level != 2:
                send(0, level)
        give_state(0, first_pair)
        give_state(1, first_pair)
        send(0, half)
        for level in range(half, lev):
            if relayed(level):
                send(0, level)

    @pl.when(odd)
    def _():
        for level in range(1, half + 1):
            send(1, level)

    inv_load.wait()
    with jax.named_scope("mats"):
        for s in range(steps):
            tall[...] = inv[s].astype(jnp.float32)
            for level in range(lev):
                mats[s, level] = tall[pl.ds(level, spec, stride=lev), :].T.astype(jnp.bfloat16)
    with jax.named_scope("both"):
        for s in range(1, steps):
            for level in range(lev):
                both[s - 1, level] = (0.1 * jnp.dot(
                    mats[s - 1, level], mats[s, level], preferred_element_type=jnp.float32)).astype(jnp.bfloat16)
    for load in small[3:]:
        load.wait()
    for w in range(nwin - 1):
        state_loads[w].wait()
    first_lane = lax.broadcasted_iota(jnp.int32, (8, cols), 1) == 0

    def beside(row, next_row):
        row, next_row = jnp.broadcast_to(row, (8, cols)), jnp.broadcast_to(next_row, (8, cols))
        return after(jnp.where(first_lane, next_row, row))

    @pl.when(has_north)
    def _():
        for copy in rows_out:
            copy.wait_recv()
        c0, o0, n0 = coef[0, 0], coef[0, 2], coef[0, 1]
        for r in range(2):
            clon, clat = nclon[r:r + 1, :], nclat[r:r + 1, :]
            coef[1, 3 * r] = jnp.broadcast_to(1.0 - clon - clat, (8, cols))
            if r == 0:
                coef[1, 1] = jnp.broadcast_to(clat, (8, cols))
            coef[1, 2 + 2 * r] = jnp.broadcast_to(clon, (8, cols))
        below = jnp.broadcast_to(nclat[1:2, :], (8, cols))
        coef[0, 5] = coef[1, 1] * below
        coef[0, 6] = below * (coef[1, 3] + c0)
        coef[0, 7] = below * n0
        coef[0, 8] = below * o0 + coef[1, 4] * beside(nclat[1:2, :], neclat[1:2, :])

    @pl.when(jnp.logical_not(has_north))
    def _():
        for k in range(5, 9):
            coef[0, k] = jnp.zeros((8, cols), jnp.float32)

    rows_west.wait_recv()

    @pl.when(has_south)
    def _():
        for copy in rows_north:
            copy.wait_recv()
        clon, clat = sclon[0:1, :], sclat[0:1, :]
        below = jnp.broadcast_to(clat_ref[1:2, :], (8, cols))
        mixed[0] = coef[0, 1] * below
        mixed[1] = below * (coef[0, 3] + jnp.broadcast_to(1.0 - clon - clat, (8, cols)))
        mixed[2] = below * jnp.broadcast_to(clat, (8, cols))
        mixed[3] = below * jnp.broadcast_to(clon, (8, cols)) + coef[0, 4] * beside(clat_ref[1:2, :], eclat[1:2, :])

    @pl.when(even)
    def _():
        mix_out.start()
        give_state(1, later_pair)
        for level in range(half + 1, lev):
            if not relayed(level):
                send(0, level)

    @pl.when(has_south)
    def _():
        with jax.named_scope("w_corner"):
            corner_out.wait_recv()
        corner[...] = jnp.concatenate(
            [corner_in[...], jnp.zeros((cols - 4 * lev, cols), jnp.float32)], axis=0).T[:spec]

    with jax.named_scope("w_col"):
        col_copy(0).wait_recv()

    @pl.when(even)
    def _():
        play(0)

    @pl.when(odd)
    def _():
        play(1)

    with jax.named_scope("reg_end"):
        regions_end()
    spread_all().wait_send()
    spread2_all().wait_send()


def finish(held_ref, grad_ref, out_hbm, grad_hbm, sems):
    copies = [
        pltpu.make_async_copy(held_ref, out_hbm, sems.at[0]),
        pltpu.make_async_copy(grad_ref, grad_hbm, sems.at[1]),
    ]
    for copy in copies:
        copy.start()
    for copy in copies:
        copy.wait()


def solution(mesh):
    n_lat, n_lon = mesh.shape["lat"], mesh.shape["lon"]
    assert n_lat % 2 == 0

    def per_device(adjoint_in, state, inverses, courant_lon, courant_lat, emission, region_id, stiffness):
        lev, spec, rows, cols = adjoint_in.shape
        nwin, steps = state.shape[0], inverses.shape[0]
        assert nwin == 2 and rows == 2
        half = lev // 2
        slots = nwin * lev + half
        passed = sum(relayed(level, w) for level in range(lev) for w in range(nwin))
        lat8 = -(-n_lat // 8) * 8
        f32, bf16 = jnp.float32, jnp.bfloat16
        any_space = pl.BlockSpec(memory_space=pl.ANY)
        vmem = pl.BlockSpec(memory_space=pltpu.VMEM)
        dma = pltpu.SemaphoreType.DMA

        def blocks(n):
            return pltpu.VMEM((n, rows, spec, cols), f32)

        out, grad = pl.pallas_call(
            functools.partial(kernel, n_lat, n_lon),
            out_shape=(
                pltpu.VMEM((lev, rows * spec, cols), bf16),
                pltpu.VMEM((1, spec), f32),
            ),
            in_specs=[any_space] * 8,
            out_specs=(vmem, vmem),
            scratch_shapes=[
                pltpu.VMEM((lev, rows * spec, cols), bf16),
                pltpu.VMEM((nwin, lev, rows * spec, cols), bf16),
                pltpu.VMEM((steps, spec * lev, spec), bf16),
                pltpu.VMEM(courant_lon.shape, f32),
                pltpu.VMEM(courant_lat.shape, f32),
                pltpu.VMEM((spec * rows, cols), f32),
                pltpu.VMEM(region_id.shape, jnp.int32),
                pltpu.VMEM(stiffness.shape, jnp.int32),
                pltpu.VMEM((spec * lev, spec), f32),
                pltpu.VMEM(inverses.shape, bf16),
                pltpu.VMEM((steps - 1,) + inverses.shape[1:], bf16),
                blocks(slots), blocks(slots), blocks(slots),
                blocks(nwin * lev), blocks(passed), blocks(half), blocks(half), blocks(half),
                pltpu.VMEM((messages(lev), spec, cols), f32),
                pltpu.VMEM((messages(lev), spec, cols), f32),
                pltpu.VMEM(courant_lon.shape, f32),
                pltpu.VMEM(courant_lat.shape, f32),
                pltpu.VMEM(courant_lat.shape, f32),
                pltpu.VMEM(courant_lon.shape, f32),
                pltpu.VMEM(courant_lat.shape, f32),
                pltpu.VMEM(courant_lat.shape, f32),
                pltpu.VMEM(stiffness.shape, jnp.int32),
                pltpu.VMEM((4 * lev, cols), f32),
                pltpu.VMEM((4 * lev, cols), f32),
                pltpu.VMEM((spec, cols), f32),
                pltpu.VMEM((4, rows * spec, cols), f32),
                pltpu.VMEM((spec, rows * cols), f32),
                pltpu.VMEM((2, 9, 8, cols), f32),
                pltpu.VMEM((4, 8, cols), f32),
                pltpu.VMEM((n_lon, lat8, spec), f32),
                pltpu.VMEM((n_lon, lat8, spec), f32),
                pltpu.VMEM((n_lat, 1, spec), f32),
                pltpu.VMEM((n_lat, 1, spec), f32),
                dma, dma((nwin,)), dma, dma((5,)),
                dma, dma((nwin * lev,)), dma((passed,)), dma, dma((half,)),
                dma, dma((half,)),
                dma, dma((messages(lev),)), dma((8,)), dma((8,)), dma, dma,
                dma, dma, dma, dma,
            ],
            compiler_params=pltpu.CompilerParams(collective_id=0, has_side_effects=True),
        )(
            adjoint_in.reshape(lev, spec * rows, cols),
            state.reshape(nwin, lev, spec * rows, cols),
            inverses.transpose(0, 2, 1, 3).reshape(steps, spec * lev, spec), courant_lon, courant_lat,
            emission.reshape(spec * rows, cols), region_id, stiffness,
        )
        out, grad = pl.pallas_call(
            finish,
            out_shape=(
                jax.ShapeDtypeStruct(out.shape, bf16),
                jax.ShapeDtypeStruct(grad.shape, f32),
            ),
            in_specs=[any_space] * 2,
            out_specs=(any_space, any_space),
            scratch_shapes=[dma((2,))],
        )(*(pltpu.with_memory_space_constraint(x, pltpu.VMEM) for x in (out, grad)))
        return out.reshape(adjoint_in.shape), grad

    in_specs = (
        P(None, None, "lat", "lon"),
        P(None, None, None, "lat", "lon"),
        P(),
        P("lat", "lon"),
        P("lat", "lon"),
        P(None, "lat", "lon"),
        P("lat", "lon"),
        P(None, "lat", "lon"),
    )
    out_specs = (P(None, None, "lat", "lon"), P(("lat", "lon"), None))
    return jax.shard_map(
        per_device, mesh=mesh, in_specs=in_specs, out_specs=out_specs, check_vma=False
    )
```

```python
import functools

import jax
import jax.numpy as jnp
from jax import lax
from jax.experimental import pallas as pl
from jax.experimental.pallas import tpu as pltpu
from jax.sharding import PartitionSpec as P

MESH = pl.DeviceIdType.MESH
OWN1, OWN0, GHOST = 0, 1, 2


def relayed(level, window=0):
    return level // 2 % 2 == 1 or (window == 1 and level == 1)


def even_order(lev):
    half = lev // 2
    passed = [l for l in range(half) if relayed(l)]
    passed_merged = [l for l in range(half, lev) if relayed(l)]
    return [
        ("first", list(range(half + 1, lev))),
        ("relay", 0, passed[:1]),
        ("chem", 1, [(OWN1, l) for l in range(half + 1, lev)]),
        ("relay", 0, passed[1:]),
        ("state", 2, half - 1),
        ("first", list(range(half + 1))),
        ("chem", 2, [(OWN1, l) for l in range(half) if not relayed(l)]),
        ("relay", 0, passed_merged),
        ("state", half - 1, half),
        ("move", 1),
        ("chem", 3, [(OWN1, l) for l in passed + [half]]),
        ("move", 2),
        ("send", [l for l in range(half + 1, lev) if not relayed(l)]),
        ("relay", 1, passed_merged),
        ("move", 3),
        ("chem", 0, [(OWN0, l) for l in range(half) if not relayed(l)]),
        ("relay", 1, [l for l in range(half) if relayed(l, 1) and not relayed(l)]),
        ("relay", 1, passed),
        ("chem", 0, [(OWN0, l) for l in passed]),
        ("turn",),
        ("chem", 0, [(OWN0, l) for l in range(half, lev) if not relayed(l)]),
        ("chem", 0, [(OWN0, l) for l in passed_merged[:-1]]),
        ("drain",),
        ("chem", 0, [(OWN0, l) for l in passed_merged[-1:]]),
        ("end",),
    ]


def odd_order(lev):
    half = lev // 2
    assert half == 4
    m = half
    batches = [
        [(OWN1, 0)], [(OWN1, 1)], [(GHOST, m), (OWN1, 2)], [(OWN1, 3), (OWN1, m)],
        [(GHOST, m + 1), (OWN1, m + 1)], [(GHOST, m + 2), (OWN1, m + 2)], [(GHOST, m + 3), (OWN1, m + 3)],
    ]

    def chem(n):
        return ("chem", n, batches[n - 1])

    return [
        ("first", [0]), chem(1), ("first", [1]), chem(2), ("first", [2, m]), chem(3), ("move", 1),
        ("first", [3]), chem(4), ("move", 2), ("first", [m + 1, m + 2, m + 3]), ("move", 3),
        chem(5), ("move", 4),        chem(6), chem(7), ("move", 5),
        ("chem", 0, [(OWN0, 0)]),
        ("move", 6), ("move", 7),
        ("chem", 0, [(OWN0, 1), (OWN0, m)]),
        ("turn",),
        ("chem", 0, [(OWN0, m + 1), (OWN0, m + 2)]),
        ("drain",),
        ("end",),
        ("chem", 0, [(OWN0, 2), (OWN0, 3), (OWN0, m + 3)]),
    ]


def corners(lev):
    return {
        level: (op[1], i)
        for op in odd_order(lev) if op[0] == "chem"
        for i, (kind, level) in enumerate(op[2]) if kind == OWN1 and level < lev // 2
    }


def messages(lev):
    return 1 + max(op[1] for op in even_order(lev) + odd_order(lev) if op[0] == "chem")


def kernel(
    n_lat, n_lon,
    adj_hbm, state_hbm, inv_hbm, clon_hbm, clat_hbm, em_hbm, reg_hbm, stiff_hbm,
    outbuf, grad_ref,
    adj, state, inv, clon_ref, clat_ref, em_ref, reg_ref, stiff_ref, tall, mats, both,
    lamb, pbuf, vout, vin, relay, zin, st_out, st_in, cout, cin, nclon, nclat, neclat, sclon, sclat, eclat, gstiff, corner_all, late_end, late_in, corner_end, corner_in, corner,
    tmp, fin, coef, mixed, part, inbox1, turn, inbox2,
    adj_sem, state_sem, inv_sem, small_sem, vs, vr, rr, fs, zr, ss, sr, cs, cr, ks, kr, ds, dr, ds2, dr2, s1, r1, s2, r2,
):
    lev, rows2, cols = adj.shape
    nwin = state.shape[0]
    steps = inv.shape[0]
    spec = rows2 // 2
    half = lev // 2
    lat, lon = lax.axis_index("lat"), lax.axis_index("lon")
    odd = lax.rem(lat, 2) == 1
    even = lax.rem(lat, 2) == 0
    north = jnp.maximum(lat - 1, 0)
    north2 = jnp.maximum(lat - 2, 0)
    south = jnp.minimum(lat + 1, n_lat - 1)
    west = lax.rem(lon + n_lon - 1, n_lon)
    east = lax.rem(lon + 1, n_lon)
    has_north = lat > 0
    has_south = lat < n_lat - 1
    sends_ghost = lat >= 2
    passes_on = lat + 2 < n_lat
    first_pair = lat < 2
    later_pair = lat >= 2
    passing = [u for u in range(2 * lev) if relayed(u % lev, u // lev)]
    plans = {0: even_order(lev), 1: odd_order(lev)}

    barrier = pltpu.get_barrier_semaphore()

    def greet(to):
        pl.semaphore_signal(barrier, inc=1, device_id=to, device_id_type=MESH)

    for k in range(1, n_lon):
        greet((lat, lax.rem(lon + k, n_lon)))
    for k in range(1, n_lat):
        greet((lax.rem(lat + k, n_lat), lon))

    @pl.when(has_south)
    def _():
        greet((south, west))
        greet((south, east))

    @pl.when(has_north)
    def _():
        greet((north, east))
        greet((north, west))

    adj_load = pltpu.make_async_copy(adj_hbm, adj, adj_sem)
    small = [
        pltpu.make_async_copy(src, dst, small_sem.at[n])
        for n, (src, dst) in enumerate((
            (clon_hbm, clon_ref), (clat_hbm, clat_ref), (stiff_hbm, stiff_ref),
            (reg_hbm, reg_ref), (em_hbm, em_ref)))
    ]
    state_loads = [
        pltpu.make_async_copy(state_hbm.at[w], state.at[w], state_sem.at[w]) for w in range(nwin)
    ]
    inv_load = pltpu.make_async_copy(inv_hbm, inv, inv_sem)
    for load in small[:2] + [adj_load, state_loads[nwin - 1], inv_load] + small[2:] + state_loads[:nwin - 1]:
        load.start()

    lane = lax.broadcasted_iota(jnp.int32, (spec, cols), 1)

    def slot_of(kind, level):
        return {OWN1: level, OWN0: lev + level, GHOST: 2 * lev + level - half}[kind]

    def after_chem(kind, level):
        return slot_of(OWN0 if kind == OWN1 else GHOST, level)

    def weights(which, names):
        return [coef[which, k, 0:1, :] for k in names]

    def remote(src, dst, send, recv, to):
        return pltpu.make_async_remote_copy(
            src_ref=src, dst_ref=dst, send_sem=send, recv_sem=recv, device_id=to, device_id_type=MESH)

    def leaves(u, raw=False):
        return (lamb if u < lev or raw else vout).at[u]

    def direct(u, raw=False):
        return remote(leaves(u, raw), vin.at[u], vs, vr.at[u], (north, lon))

    def to_relay(u):
        n = passing.index(u)
        return remote(leaves(u), relay.at[n], vs, rr.at[n], (north2, lon))

    def forward(u):
        return remote(relay.at[passing.index(u)], vin.at[u], fs, vr.at[u], (south, lon))

    def ghost_out(level):
        u, n = slot_of(GHOST, level), level - half
        return remote(vout.at[u], zin.at[n], vs, zr.at[n], (north2, lon))

    def state_out(n):
        return remote(st_out.at[n], st_in.at[n], ss, sr.at[n], (south, lon))

    def col_copy(n):
        return remote(cout.at[n], cin.at[n], cs, cr.at[n], (lat, west))

    rows_out = [
        remote(clon_ref, nclon, ks.at[0], kr.at[0], (south, lon)),
        remote(clat_ref, nclat, ks.at[1], kr.at[1], (south, lon)),
        remote(clat_ref, neclat, ks.at[2], kr.at[2], (south, west)),
    ]
    rows_north = [
        remote(clon_ref, sclon, ks.at[5], kr.at[5], (north, lon)),
        remote(clat_ref, sclat, ks.at[6], kr.at[6], (north, lon)),
    ]
    rows_west = remote(clat_ref, eclat, ks.at[7], kr.at[7], (lat, west))
    corner_out = remote(corner_end, corner_in, ds, dr, (north, west))
    stiff_out = remote(stiff_ref, gstiff, ks.at[3], kr.at[3], (south, lon))
    mix_out = remote(coef.at[0, pl.ds(5, 4)], coef.at[1, pl.ds(5, 4)], ks.at[4], kr.at[4], (south, lon))

    def after(x):
        return pltpu.roll(x, cols - 1, 1)

    def pack(n, slots):
        message = None
        for i, (u, which) in enumerate(slots):
            c0, n0, o0, c1, o1 = weights(which, range(5))
            row0, row1 = lamb[u, 0], lamb[u, 1]
            new0 = c0 * row0 + n0 * row1 + o0 * after(row0)
            new1 = c1 * row1 + o1 * after(row1)
            for j, x in enumerate((row0, row1, new0, new1)):
                at = 4 * i + j
                message = x if at == 0 else jnp.where(lane == at, pltpu.roll(x, at, 1), message)
        cout[n] = message

    def move(u, which, n, i, combine):
        c0, n0, o0, c1, o1, al, be, ga, de = weights(which, range(9))
        row0, row1, message = lamb[u, 0], lamb[u, 1], cin[n]

        def shift(x, j):
            edge = message if 4 * i + j == 0 else pltpu.roll(message, cols - 4 * i - j, 1)
            return after(jnp.where(lane == 0, edge, x))

        right0, right1 = shift(row0, 0), shift(row1, 1)
        new0 = c0 * row0 + n0 * row1 + o0 * right0
        new1 = c1 * row1 + o1 * right1
        pbuf[u, 0] = c0 * new0 + n0 * new1 + o0 * shift(new0, 2)
        pbuf[u, 1] = c1 * new1 + o1 * shift(new1, 3)
        if not combine:
            return None
        v0 = al * row0
        v1 = be * row0 + ga * row1 + de * right0
        return v0, v1

    def own_sends(side, u):
        level = u % lev
        if side == 1:
            if u == half:
                return direct(u), later_pair
            return None if u < lev and level > half else (direct(u, level < half), None)
        return (to_relay(u) if relayed(level, u // lev) else direct(u)), has_north

    def when(condition, do):
        if condition is None:
            do()
        else:
            pl.when(condition)(do)

    def transport(side, n, i, kind, level):
        u = slot_of(kind, level)
        raw = side == 1 and kind == OWN0 and level < half
        combine = (kind != OWN1 or (side == 1 and level >= half)) and not raw
        with jax.named_scope("move"):
            both = move(u, 1 if kind == GHOST else 0, n, i, combine)
            if combine:
                merged = side == 1 and kind == OWN0 and level >= half
                if merged and level > half:
                    ghost = slot_of(GHOST, level)
                    both = both[0] + pbuf[ghost, 0], both[1] + pbuf[ghost, 1]
                vout[u, 0], vout[u, 1] = both
                if merged and level == half:
                    @pl.when(first_pair)
                    def _():
                        ghost = slot_of(GHOST, level)
                        for r in range(2):
                            vout[u, r] = vout[u, r] + pbuf[ghost, r]
        if kind == GHOST:
            if level > half:
                when(sends_ghost, lambda: ghost_out(level).start())
        elif kind == OWN0 and not raw and not (side == 0 and level > half and not relayed(level)):
            send(side, u)

    def send(side, u):
        leaving = own_sends(side, u)
        if leaving is not None:
            when(leaving[1], lambda: leaving[0].start())

    def corner_late(n):
        return remote(late_end.at[n], late_in.at[n], ds2, dr2.at[n], (north, west))

    def arrived(level, u=None):
        al, be, ga, de = [mixed[k, 0:1, :] for k in range(4)]
        if u is None:
            u, message, at = level, corner[...], level
        else:
            n, i = corners(lev)[level]
            corner_late(n - 1).wait_recv()
            message, at = jnp.concatenate(
                [late_in[n - 1], jnp.zeros((cols - 8, cols), jnp.float32)], axis=0).T[:spec], 4 * i
        row0, row1 = vin[u, 0], vin[u, 1]
        edge = message if at == 0 else pltpu.roll(message, cols - at, 1)
        right0 = after(jnp.where(lane == 0, edge, row0))
        return al * row0, be * row0 + ga * row1 + de * right0

    def gather(side, kind, level, i):
        u = slot_of(kind, level)
        if kind == GHOST:
            n = level - half
            with jax.named_scope("w_st"):
                when(None if n else first_pair, lambda: state_out(n).wait_recv())
            if n == 0:
                stiff_out.wait_recv()
            x, y, live = [vout[level, r] for r in range(2)], [st_in[n, r] for r in range(2)], gstiff[level]
        else:
            if side == 1:
                @pl.when(has_south)
                def _():
                    with jax.named_scope("w_vin"):
                        direct(u).wait_recv()
                    extra = kind == OWN0 and level > half
                    if extra:
                        with jax.named_scope("w_z"):
                            ghost_out(level).wait_recv()
                    adds = arrived(level) if kind == OWN1 else [vin[u, r] for r in range(2)]
                    for r in range(2):
                        both = adds[r] + zin[level - half, r] if extra else adds[r]
                        pbuf[u, r] = pbuf[u, r] + both
                x = [pbuf[u, r] for r in range(2)]
            elif kind == OWN0 or level < half:
                with jax.named_scope("w_vin"):
                    direct(u).wait_recv()
                if kind == OWN1:
                    adds = arrived(level)
                elif level < half:
                    adds = arrived(level, u)
                else:
                    adds = [vin[u, r] for r in range(2)]
                x = [pbuf[u, r] + adds[r] for r in range(2)]
            else:
                if level == half:
                    @pl.when(later_pair)
                    def _():
                        with jax.named_scope("w_vin"):
                            direct(u).wait_recv()
                        adds = arrived(level)
                        for r in range(2):
                            pbuf[u, r] = pbuf[u, r] + adds[r]
                x = [pbuf[u, r] for r in range(2)]
            tmp[i] = state[nwin - 1 if kind == OWN1 else 0, level].astype(jnp.float32)
            y, live = [tmp[i, pl.ds(r, spec, stride=2), :] for r in range(2)], stiff_ref[level]
        return (
            jnp.concatenate(x, axis=1), jnp.concatenate(y, axis=1),
            jnp.concatenate([live[0:1], live[1:2]], axis=1),
        )

    def chem(levels, gathered):
        flats, ys, lives = zip(*gathered)

        def dot(mat, xs):
            return [
                jnp.dot(a, x.astype(jnp.bfloat16), preferred_element_type=jnp.float32) for a, x in zip(mat, xs)]

        v1 = dot([mats[steps - 1, level] for level in levels], flats)
        for s in reversed(range(steps)):
            mat = [mats[s, level] for level in levels]
            v2 = dot(mat, [v * y for v, y in zip(v1, ys)])
            r2 = [v * y for v, y in zip(v2, ys)]
            v3 = dot(mat, r2)
            some = [0.4 * x + 0.3 * a + 0.2 * b for x, a, b in zip(flats, v1, v2)]
            if s:
                v1 = [
                    a + b for a, b in zip(
                        dot([mats[s - 1, level] for level in levels],
                            [jnp.where(live > s, x, flat) for x, flat, live in zip(some, flats, lives)]),
                        dot([both[s - 1, level] for level in levels],
                            [jnp.where(live > s, r, 0.0) for r, live in zip(r2, lives)]))]
            flats = [
                jnp.where(live > s, x + 0.1 * c, flat) for x, c, flat, live in zip(some, v3, flats, lives)
            ]
        return flats

    def spread(k):
        to = lax.rem(lon + k, n_lon)
        return remote(part.at[to], inbox1.at[k - 1], s1, r1, (lat, to))

    def spread_all():
        n = pl.ds(0, n_lon - 1)
        return remote(part.at[n], inbox1.at[n], s1, r1, (lat, west))

    def spread2(k):
        to = lax.rem(lat + k, n_lat)
        return remote(turn.at[to], inbox2.at[k - 1], s2, r2, (to, lon))

    def spread2_all():
        n = pl.ds(0, n_lat - 1)
        return remote(turn.at[n], inbox2.at[n], s2, r2, (north, lon))

    def regions():
        lat8 = part.shape[1]
        contrib = jnp.concatenate([
            em_ref[pl.ds(r, spec, stride=2), :]
            * (lamb[lev, r] + fin[:, r * cols:(r + 1) * cols])
            for r in range(2)], axis=1)
        where_from = jnp.concatenate([reg_ref[0:1, :], reg_ref[1:2, :]], axis=1)
        shape = (n_lon * lat8, 2 * cols)
        column = jnp.concatenate([jnp.full((lat8, 2 * cols), c, jnp.int32) for c in range(n_lon)], axis=0)
        band = lax.broadcasted_iota(jnp.int32, (lat8, 2 * cols), 0)
        band = jnp.concatenate([band] * n_lon, axis=0)
        onehot = (jnp.broadcast_to(where_from, shape) == band * n_lon + column).astype(jnp.float32)
        sums = lax.dot_general(
            onehot, contrib, (((1,), (1,)), ((), ())),
            precision=lax.Precision.HIGHEST, preferred_element_type=jnp.float32)
        for c in range(n_lon):
            part[c] = sums[c * lat8:(c + 1) * lat8]
        for k in range(1, n_lon):
            spread(k).start()

    def regions_turn():
        total = part[lon]
        spread_all().wait_recv()
        for k in range(n_lon - 1):
            total = total + inbox1[k]
        for b in range(n_lat):
            turn[b] = total[b:b + 1]
        for k in range(1, n_lat):
            spread2(k).start()

    def regions_end():
        total = turn[lat]
        spread2_all().wait_recv()
        for k in range(n_lat - 1):
            total = total + inbox2[k]
        grad_ref[...] = total

    def drain(side, sent):
        n = 1 + len(sent)
        remote(cout.at[pl.ds(0, n)], cin.at[pl.ds(0, n)], cs, cr.at[0], (lat, west)).wait_send()

        def left(n):
            remote(lamb.at[pl.ds(0, n)], vin.at[pl.ds(0, n)], vs, vr.at[0], (north, lon)).wait_send()

        if side == 1:
            left(lev + half)
            remote(late_end, late_in, ds2, dr2.at[0], (north, west)).wait_send()

            @pl.when(later_pair)
            def _():
                left(1)

            @pl.when(sends_ghost)
            def _():
                left(half - 1)
        else:
            @pl.when(has_north)
            def _():
                left(2 * lev)
            stiff_out.wait_send()
            mix_out.wait_send()
            n = pl.ds(0, half - 1)
            remote(st_out.at[n], st_in.at[n], ss, sr.at[0], (south, lon)).wait_send()
            when(first_pair, lambda: state_out(0).wait_send())
        rows_west.wait_send()

        @pl.when(has_north)
        def _():
            corner_out.wait_send()
            for copy in rows_north:
                copy.wait_send()

        @pl.when(has_south)
        def _():
            for copy in rows_out:
                copy.wait_send()

    def play(side):
        sent = {}
        for op in plans[side]:
            if op[0] == "chem":
                n, items = op[1:]
                gathered = [gather(side, kind, level, i) for i, (kind, level) in enumerate(items)]
                with jax.named_scope("chem"):
                    flats = chem([level for _, level in items], gathered)
                if n:
                    slots = []
                    for (kind, level), flat in zip(items, flats):
                        u = after_chem(kind, level)
                        for r in range(2):
                            lamb[u, r] = flat[:, r * cols:(r + 1) * cols]
                        slots.append((u, 1 if kind == GHOST else 0))
                        if side == 1 and kind == OWN1 and level < half:
                            send(side, u)
                    with jax.named_scope("pack"):
                        pack(n, slots)
                    col_copy(n).start()
                    if side == 1 and n in [m for m, _ in corners(lev).values()]:
                        late_end[n - 1] = jnp.concatenate(
                            [cout[n], jnp.zeros((cols - spec, cols), jnp.float32)], axis=0).T[:8]
                        corner_late(n - 1).start()
                    sent[n] = [(OWN0 if kind == OWN1 else GHOST, level) for kind, level in items]
                else:
                    for i, ((kind, level), flat) in enumerate(zip(items, flats)):
                        for r in range(2):
                            tmp[i, pl.ds(r, spec, stride=2), :] = flat[:, r * cols:(r + 1) * cols]
                        outbuf[level] = tmp[i].astype(jnp.bfloat16)
                        if level == 0:
                            fin[...] = flat
                            with jax.named_scope("regions"):
                                regions()
            elif op[0] == "send":
                for level in op[1]:
                    send(side, lev + level)
            elif op[0] == "first":
                for level in op[1]:
                    transport(side, 0, level, OWN1, level)
            elif op[0] == "move":
                n = op[1]
                with jax.named_scope("w_col"):
                    col_copy(n).wait_recv()
                if side == 1 and n == 3:
                    mix_out.wait_recv()
                for i, (kind, level) in enumerate(sent[n]):
                    transport(side, n, i, kind, level)
            elif op[0] == "relay":
                w, passed = op[1:]

                @pl.when(passes_on)
                def _(w=w, passed=passed):
                    for level in passed:
                        u = w * lev + level
                        with jax.named_scope("w_relay"):
                            to_relay(u).wait_recv()
                        forward(u).start()
            elif op[0] == "state":
                for k in range(op[1], op[2]):
                    give_state(k)
            elif op[0] == "drain":
                drain(side, sent)
            elif op[0] == "end":
                with jax.named_scope("reg_end"):
                    regions_end()
                spread_all().wait_send()
                spread2_all().wait_send()
            else:
                with jax.named_scope("turn"):
                    regions_turn()

        if side == 0:
            @pl.when(passes_on)
            def _():
                remote(relay, relay, fs, rr.at[0], (south, lon)).wait_send()

    for load in small[:2]:
        load.wait()
    for r in range(2):
        clon, clat = clon_ref[r:r + 1, :], clat_ref[r:r + 1, :]
        coef[0, 3 * r] = jnp.broadcast_to(1.0 - clon - clat, (8, cols))
        if r == 0:
            coef[0, 1] = jnp.broadcast_to(clat, (8, cols))
        coef[0, 2 + 2 * r] = jnp.broadcast_to(clon, (8, cols))

    adj_load.wait()
    small[2].wait()
    for level in range(lev):
        tmp[level % 4] = adj[level].astype(jnp.float32)
        for r in range(2):
            lamb[level, r] = tmp[level % 4, pl.ds(r, spec, stride=2), :]
    with jax.named_scope("pack"):
        pack(0, [(level, 0) for level in range(lev)])
        corner_all[...] = jnp.concatenate(
            [cout[0], jnp.zeros((cols - spec, cols), jnp.float32)], axis=0).T[:4 * lev]
        corner_end[...] = corner_all[pl.ds(0, lev, stride=4), :]
    with jax.named_scope("w_barrier"):
        pl.semaphore_wait(
            barrier, n_lon - 1 + n_lat - 1 + 2 * has_north.astype(jnp.int32) + 2 * has_south.astype(jnp.int32))

    @pl.when(has_south)
    def _():
        for copy in rows_out:
            copy.start()

    @pl.when(has_north)
    def _():
        for copy in rows_north:
            copy.start()
    rows_west.start()

    @pl.when(even)
    def _():
        stiff_out.start()
        when(has_north, lambda: corner_out.start())
        send(0, 0)
        send(0, 2)

    @pl.when(odd)
    def _():
        corner_out.start()
        send(1, 0)
    col_copy(0).start()

    def give_state(n, condition=None):
        def do():
            tmp[n % 4] = state[nwin - 1, half + n].astype(jnp.float32)
            for r in range(2):
                st_out[n, r] = tmp[n % 4, pl.ds(r, spec, stride=2), :]
            state_out(n).start()

        when(condition, do)

    state_loads[nwin - 1].wait()

    @pl.when(even)
    def _():
        for level in range(1, half):
            if level != 2:
                send(0, level)
        give_state(0, first_pair)
        give_state(1, first_pair)
        send(0, half)
        for level in range(half, lev):
            if relayed(level):
                send(0, level)

    @pl.when(odd)
    def _():
        for level in range(1, half + 1):
            send(1, level)

    inv_load.wait()
    with jax.named_scope("mats"):
        for s in range(steps):
            tall[...] = inv[s].astype(jnp.float32)
            for level in range(lev):
                mats[s, level] = tall[pl.ds(level, spec, stride=lev), :].T.astype(jnp.bfloat16)
    with jax.named_scope("both"):
        for s in range(1, steps):
            for level in range(lev):
                both[s - 1, level] = (0.1 * jnp.dot(
                    mats[s - 1, level], mats[s, level], preferred_element_type=jnp.float32)).astype(jnp.bfloat16)
    for load in small[3:]:
        load.wait()
    for w in range(nwin - 1):
        state_loads[w].wait()
    first_lane = lax.broadcasted_iota(jnp.int32, (8, cols), 1) == 0

    def beside(row, next_row):
        row, next_row = jnp.broadcast_to(row, (8, cols)), jnp.broadcast_to(next_row, (8, cols))
        return after(jnp.where(first_lane, next_row, row))

    @pl.when(has_north)
    def _():
        for copy in rows_out:
            copy.wait_recv()
        c0, o0, n0 = coef[0, 0], coef[0, 2], coef[0, 1]
        for r in range(2):
            clon, clat = nclon[r:r + 1, :], nclat[r:r + 1, :]
            coef[1, 3 * r] = jnp.broadcast_to(1.0 - clon - clat, (8, cols))
            if r == 0:
                coef[1, 1] = jnp.broadcast_to(clat, (8, cols))
            coef[1, 2 + 2 * r] = jnp.broadcast_to(clon, (8, cols))
        below = jnp.broadcast_to(nclat[1:2, :], (8, cols))
        coef[0, 5] = coef[1, 1] * below
        coef[0, 6] = below * (coef[1, 3] + c0)
        coef[0, 7] = below * n0
        coef[0, 8] = below * o0 + coef[1, 4] * beside(nclat[1:2, :], neclat[1:2, :])

    @pl.when(jnp.logical_not(has_north))
    def _():
        for k in range(5, 9):
            coef[0, k] = jnp.zeros((8, cols), jnp.float32)

    rows_west.wait_recv()

    @pl.when(has_south)
    def _():
        for copy in rows_north:
            copy.wait_recv()
        clon, clat = sclon[0:1, :], sclat[0:1, :]
        below = jnp.broadcast_to(clat_ref[1:2, :], (8, cols))
        mixed[0] = coef[0, 1] * below
        mixed[1] = below * (coef[0, 3] + jnp.broadcast_to(1.0 - clon - clat, (8, cols)))
        mixed[2] = below * jnp.broadcast_to(clat, (8, cols))
        mixed[3] = below * jnp.broadcast_to(clon, (8, cols)) + coef[0, 4] * beside(clat_ref[1:2, :], eclat[1:2, :])

    @pl.when(even)
    def _():
        mix_out.start()
        give_state(1, later_pair)
        for level in range(half + 1, lev):
            if not relayed(level):
                send(0, level)

    @pl.when(has_south)
    def _():
        with jax.named_scope("w_corner"):
            corner_out.wait_recv()
        corner[...] = jnp.concatenate(
            [corner_in[...], jnp.zeros((cols - lev, cols), jnp.float32)], axis=0).T[:spec]

    with jax.named_scope("w_col"):
        col_copy(0).wait_recv()

    @pl.when(even)
    def _():
        play(0)

    @pl.when(odd)
    def _():
        play(1)


def finish(held_ref, grad_ref, out_hbm, grad_hbm, sems):
    copies = [
        pltpu.make_async_copy(held_ref, out_hbm, sems.at[0]),
        pltpu.make_async_copy(grad_ref, grad_hbm, sems.at[1]),
    ]
    for copy in copies:
        copy.start()
    for copy in copies:
        copy.wait()


def solution(mesh):
    n_lat, n_lon = mesh.shape["lat"], mesh.shape["lon"]
    assert n_lat % 2 == 0

    def per_device(adjoint_in, state, inverses, courant_lon, courant_lat, emission, region_id, stiffness):
        lev, spec, rows, cols = adjoint_in.shape
        nwin, steps = state.shape[0], inverses.shape[0]
        assert nwin == 2 and rows == 2
        half = lev // 2
        slots = nwin * lev + half
        passed = sum(relayed(level, w) for level in range(lev) for w in range(nwin))
        lat8 = -(-n_lat // 8) * 8
        f32, bf16 = jnp.float32, jnp.bfloat16
        any_space = pl.BlockSpec(memory_space=pl.ANY)
        vmem = pl.BlockSpec(memory_space=pltpu.VMEM)
        dma = pltpu.SemaphoreType.DMA

        def blocks(n):
            return pltpu.VMEM((n, rows, spec, cols), f32)

        out, grad = pl.pallas_call(
            functools.partial(kernel, n_lat, n_lon),
            out_shape=(
                pltpu.VMEM((lev, rows * spec, cols), bf16),
                pltpu.VMEM((1, spec), f32),
            ),
            in_specs=[any_space] * 8,
            out_specs=(vmem, vmem),
            scratch_shapes=[
                pltpu.VMEM((lev, rows * spec, cols), bf16),
                pltpu.VMEM((nwin, lev, rows * spec, cols), bf16),
                pltpu.VMEM((steps, spec * lev, spec), bf16),
                pltpu.VMEM(courant_lon.shape, f32),
                pltpu.VMEM(courant_lat.shape, f32),
                pltpu.VMEM((spec * rows, cols), f32),
                pltpu.VMEM(region_id.shape, jnp.int32),
                pltpu.VMEM(stiffness.shape, jnp.int32),
                pltpu.VMEM((spec * lev, spec), f32),
                pltpu.VMEM(inverses.shape, bf16),
                pltpu.VMEM((steps - 1,) + inverses.shape[1:], bf16),
                blocks(slots), blocks(slots), blocks(slots),
                blocks(nwin * lev), blocks(passed), blocks(half), blocks(half), blocks(half),
                pltpu.VMEM((messages(lev), spec, cols), f32),
                pltpu.VMEM((messages(lev), spec, cols), f32),
                pltpu.VMEM(courant_lon.shape, f32),
                pltpu.VMEM(courant_lat.shape, f32),
                pltpu.VMEM(courant_lat.shape, f32),
                pltpu.VMEM(courant_lon.shape, f32),
                pltpu.VMEM(courant_lat.shape, f32),
                pltpu.VMEM(courant_lat.shape, f32),
                pltpu.VMEM(stiffness.shape, jnp.int32),
                pltpu.VMEM((4 * lev, cols), f32),
                pltpu.VMEM((half, 8, cols), f32),
                pltpu.VMEM((half, 8, cols), f32),
                pltpu.VMEM((lev, cols), f32),
                pltpu.VMEM((lev, cols), f32),
                pltpu.VMEM((spec, cols), f32),
                pltpu.VMEM((4, rows * spec, cols), f32),
                pltpu.VMEM((spec, rows * cols), f32),
                pltpu.VMEM((2, 9, 8, cols), f32),
                pltpu.VMEM((4, 8, cols), f32),
                pltpu.VMEM((n_lon, lat8, spec), f32),
                pltpu.VMEM((n_lon, lat8, spec), f32),
                pltpu.VMEM((n_lat, 1, spec), f32),
                pltpu.VMEM((n_lat, 1, spec), f32),
                dma, dma((nwin,)), dma, dma((5,)),
                dma, dma((nwin * lev,)), dma((passed,)), dma, dma((half,)),
                dma, dma((half,)),
                dma, dma((messages(lev),)), dma((8,)), dma((8,)), dma, dma, dma, dma((half,)),
                dma, dma, dma, dma,
            ],
            compiler_params=pltpu.CompilerParams(collective_id=0, has_side_effects=True),
        )(
            adjoint_in.reshape(lev, spec * rows, cols),
            state.reshape(nwin, lev, spec * rows, cols),
            inverses.transpose(0, 2, 1, 3).reshape(steps, spec * lev, spec), courant_lon, courant_lat,
            emission.reshape(spec * rows, cols), region_id, stiffness,
        )
        out, grad = pl.pallas_call(
            finish,
            out_shape=(
                jax.ShapeDtypeStruct(out.shape, bf16),
                jax.ShapeDtypeStruct(grad.shape, f32),
            ),
            in_specs=[any_space] * 2,
            out_specs=(any_space, any_space),
            scratch_shapes=[dma((2,))],
        )(*(pltpu.with_memory_space_constraint(x, pltpu.VMEM) for x in (out, grad)))
        return out.reshape(adjoint_in.shape), grad

    in_specs = (
        P(None, None, "lat", "lon"),
        P(None, None, None, "lat", "lon"),
        P(),
        P("lat", "lon"),
        P("lat", "lon"),
        P(None, "lat", "lon"),
        P("lat", "lon"),
        P(None, "lat", "lon"),
    )
    out_specs = (P(None, None, "lat", "lon"), P(("lat", "lon"), None))
    return jax.shard_map(
        per_device, mesh=mesh, in_specs=in_specs, out_specs=out_specs, check_vma=False
    )
```

```python
import functools

import jax
import jax.numpy as jnp
from jax import lax
from jax.experimental import pallas as pl
from jax.experimental.pallas import tpu as pltpu
from jax.sharding import PartitionSpec as P

MESH = pl.DeviceIdType.MESH
OWN1, OWN0, GHOST = 0, 1, 2


def relayed(level, window=0):
    return level // 2 % 2 == 1 or (window == 1 and level == 1)


def even_order(lev):
    half = lev // 2
    passed = [l for l in range(half) if relayed(l)]
    passed_merged = [l for l in range(half, lev) if relayed(l)]
    return [
        ("first", list(range(half + 1, lev))),
        ("relay", 0, passed[:1]),
        ("chem", 1, [(OWN1, l) for l in range(half + 1, lev)]),
        ("relay", 0, passed[1:]),
        ("state", 2, half - 1),
        ("first", list(range(half + 1))),
        ("chem", 2, [(OWN1, l) for l in range(half) if not relayed(l)]),
        ("relay", 0, passed_merged),
        ("state", half - 1, half),
        ("move", 1),
        ("chem", 3, [(OWN1, l) for l in passed + [half]]),
        ("move", 2),
        ("send", [l for l in range(half + 1, lev) if not relayed(l)]),
        ("relay", 1, passed_merged),
        ("move", 3),
        ("chem", 0, [(OWN0, l) for l in range(half) if not relayed(l)]),
        ("relay", 1, [l for l in range(half) if relayed(l, 1) and not relayed(l)]),
        ("relay", 1, passed),
        ("chem", 0, [(OWN0, l) for l in passed]),
        ("turn",),
        ("chem", 0, [(OWN0, l) for l in range(half, lev) if not relayed(l)]),
        ("chem", 0, [(OWN0, l) for l in passed_merged[:-1]]),
        ("drain",),
        ("chem", 0, [(OWN0, l) for l in passed_merged[-1:]]),
        ("end",),
    ]


def odd_order(lev):
    half = lev // 2
    assert half == 4
    m = half
    batches = [
        [(OWN1, 0)], [(OWN1, 1)], [(GHOST, m), (OWN1, 2)], [(OWN1, 3), (OWN1, m)],
        [(GHOST, m + 1), (OWN1, m + 1)], [(GHOST, m + 2), (OWN1, m + 2)], [(GHOST, m + 3), (OWN1, m + 3)],
    ]

    def chem(n):
        return ("chem", n, batches[n - 1])

    return [
        ("first", [0]), chem(1), ("first", [1]), chem(2), ("first", [2, m]), chem(3), ("move", 1),
        ("first", [3]), chem(4), ("move", 2), ("first", [m + 1, m + 2, m + 3]), ("move", 3),
        chem(5), ("move", 4),        chem(6), chem(7), ("move", 5),
        ("chem", 0, [(OWN0, 0)]),
        ("move", 6), ("move", 7),
        ("chem", 0, [(OWN0, 1), (OWN0, m)]),
        ("turn",),
        ("chem", 0, [(OWN0, m + 1), (OWN0, m + 2)]),
        ("drain",),
        ("end",),
        ("chem", 0, [(OWN0, 2), (OWN0, 3), (OWN0, m + 3)]),
    ]


def corners(lev):
    return {
        level: (op[1], i)
        for op in odd_order(lev) if op[0] == "chem"
        for i, (kind, level) in enumerate(op[2]) if kind == OWN1 and level < lev // 2
    }


def messages(lev):
    return 1 + max(op[1] for op in even_order(lev) + odd_order(lev) if op[0] == "chem")


def kernel(
    n_lat, n_lon,
    adj_hbm, state_hbm, inv_hbm, clon_hbm, clat_hbm, em_hbm, reg_hbm, stiff_hbm,
    outbuf, grad_ref,
    adj, state, inv, clon_ref, clat_ref, em_ref, reg_ref, stiff_ref, tall, mats, both,
    lamb, pbuf, vout, vin, relay, zin, st_out, st_in, cout, cin, nclon, nclat, neclat, sclon, sclat, eclat, gstiff, corner_all, late_end, late_in, corner_end, corner_in, corner,
    tmp, fin, coef, mixed, part, inbox1, turn, inbox2,
    adj_sem, state_sem, inv_sem, small_sem, vs, vr, rr, fs, ss, cs, cr, ks, kr, ds, dr, ds2, dr2, s1, r1, s2, r2,
):
    lev, rows2, cols = adj.shape
    nwin = state.shape[0]
    steps = inv.shape[0]
    spec = rows2 // 2
    half = lev // 2
    lat, lon = lax.axis_index("lat"), lax.axis_index("lon")
    odd = lax.rem(lat, 2) == 1
    even = lax.rem(lat, 2) == 0
    north = jnp.maximum(lat - 1, 0)
    north2 = jnp.maximum(lat - 2, 0)
    south = jnp.minimum(lat + 1, n_lat - 1)
    west = lax.rem(lon + n_lon - 1, n_lon)
    east = lax.rem(lon + 1, n_lon)
    has_north = lat > 0
    has_south = lat < n_lat - 1
    sends_ghost = lat >= 2
    passes_on = lat + 2 < n_lat
    first_pair = lat < 2
    later_pair = lat >= 2
    passing = [u for u in range(2 * lev) if relayed(u % lev, u // lev)]
    plans = {0: even_order(lev), 1: odd_order(lev)}

    barrier = pltpu.get_barrier_semaphore()

    def greet(to):
        pl.semaphore_signal(barrier, inc=1, device_id=to, device_id_type=MESH)

    for k in range(1, n_lon):
        greet((lat, lax.rem(lon + k, n_lon)))
    for k in range(1, n_lat):
        greet((lax.rem(lat + k, n_lat), lon))

    @pl.when(has_south)
    def _():
        greet((south, west))
        greet((south, east))

    @pl.when(has_north)
    def _():
        greet((north, east))
        greet((north, west))

    adj_load = pltpu.make_async_copy(adj_hbm, adj, adj_sem)
    small = [
        pltpu.make_async_copy(src, dst, small_sem.at[n])
        for n, (src, dst) in enumerate((
            (clon_hbm, clon_ref), (clat_hbm, clat_ref), (stiff_hbm, stiff_ref),
            (reg_hbm, reg_ref), (em_hbm, em_ref)))
    ]
    state_loads = [
        pltpu.make_async_copy(state_hbm.at[w], state.at[w], state_sem.at[w]) for w in range(nwin)
    ]
    inv_load = pltpu.make_async_copy(inv_hbm, inv, inv_sem)
    for load in small[:2] + [adj_load, state_loads[nwin - 1], inv_load] + small[2:] + state_loads[:nwin - 1]:
        load.start()

    lane = lax.broadcasted_iota(jnp.int32, (spec, cols), 1)

    def slot_of(kind, level):
        return {OWN1: level, OWN0: lev + level, GHOST: 2 * lev + level - half}[kind]

    def after_chem(kind, level):
        return slot_of(OWN0 if kind == OWN1 else GHOST, level)

    def weights(which, names):
        return [coef[which, k, 0:1, :] for k in names]

    def remote(src, dst, send, recv, to):
        return pltpu.make_async_remote_copy(
            src_ref=src, dst_ref=dst, send_sem=send, recv_sem=recv, device_id=to, device_id_type=MESH)

    def leaves(u, raw=False):
        return (lamb if u < lev or raw else vout).at[u]

    def direct(u, raw=False):
        return remote(leaves(u, raw), vin.at[u], vs, vr.at[u], (north, lon))

    def to_relay(u):
        n = passing.index(u)
        return remote(leaves(u), relay.at[n], vs, rr.at[n], (north2, lon))

    def forward(u):
        return remote(relay.at[passing.index(u)], vin.at[u], fs, vr.at[u], (south, lon))

    def ghost_out(level):
        u, n = slot_of(GHOST, level), level - half
        return remote(vout.at[u], zin.at[n], vs, rr.at[half + n], (north2, lon))

    def state_out(n):
        return remote(st_out.at[n], st_in.at[n], ss, rr.at[n], (south, lon))

    def col_copy(n):
        return remote(cout.at[n], cin.at[n], cs, cr.at[n], (lat, west))

    rows_out = [
        remote(clon_ref, nclon, ks.at[0], kr.at[0], (south, lon)),
        remote(clat_ref, nclat, ks.at[0], kr.at[0], (south, lon)),
        remote(clat_ref, neclat, ks.at[0], kr.at[0], (south, west)),
    ]
    rows_north = [
        remote(clon_ref, sclon, ks.at[0], kr.at[1], (north, lon)),
        remote(clat_ref, sclat, ks.at[0], kr.at[1], (north, lon)),
    ]
    rows_west = remote(clat_ref, eclat, ks.at[0], kr.at[2], (lat, west))
    corner_out = remote(corner_end, corner_in, ds, dr, (north, west))

    def row_copies(n, recv):
        return remote(stiff_ref.at[pl.ds(0, n)], gstiff.at[pl.ds(0, n)], ks.at[0], kr.at[recv], (south, lon))

    stiff_out = remote(stiff_ref, gstiff, ks.at[1], kr.at[3], (south, lon))
    mix_out = remote(coef.at[0, pl.ds(5, 4)], coef.at[1, pl.ds(5, 4)], ks.at[2], kr.at[4], (south, lon))

    def after(x):
        return pltpu.roll(x, cols - 1, 1)

    def pack(n, slots):
        message = None
        for i, (u, which) in enumerate(slots):
            c0, n0, o0, c1, o1 = weights(which, range(5))
            row0, row1 = lamb[u, 0], lamb[u, 1]
            new0 = c0 * row0 + n0 * row1 + o0 * after(row0)
            new1 = c1 * row1 + o1 * after(row1)
            for j, x in enumerate((row0, row1, new0, new1)):
                at = 4 * i + j
                message = x if at == 0 else jnp.where(lane == at, pltpu.roll(x, at, 1), message)
        cout[n] = message

    def move(u, which, n, i, combine):
        c0, n0, o0, c1, o1, al, be, ga, de = weights(which, range(9))
        row0, row1, message = lamb[u, 0], lamb[u, 1], cin[n]

        def shift(x, j):
            edge = message if 4 * i + j == 0 else pltpu.roll(message, cols - 4 * i - j, 1)
            return after(jnp.where(lane == 0, edge, x))

        right0, right1 = shift(row0, 0), shift(row1, 1)
        new0 = c0 * row0 + n0 * row1 + o0 * right0
        new1 = c1 * row1 + o1 * right1
        pbuf[u, 0] = c0 * new0 + n0 * new1 + o0 * shift(new0, 2)
        pbuf[u, 1] = c1 * new1 + o1 * shift(new1, 3)
        if not combine:
            return None
        v0 = al * row0
        v1 = be * row0 + ga * row1 + de * right0
        return v0, v1

    def own_sends(side, u):
        level = u % lev
        if side == 1:
            if u == half:
                return direct(u), later_pair
            return None if u < lev and level > half else (direct(u, level < half), None)
        return (to_relay(u) if relayed(level, u // lev) else direct(u)), has_north

    def when(condition, do):
        if condition is None:
            do()
        else:
            pl.when(condition)(do)

    def transport(side, n, i, kind, level):
        u = slot_of(kind, level)
        raw = side == 1 and kind == OWN0 and level < half
        combine = (kind != OWN1 or (side == 1 and level >= half)) and not raw
        with jax.named_scope("move"):
            both = move(u, 1 if kind == GHOST else 0, n, i, combine)
            if combine:
                merged = side == 1 and kind == OWN0 and level >= half
                if merged and level > half:
                    ghost = slot_of(GHOST, level)
                    both = both[0] + pbuf[ghost, 0], both[1] + pbuf[ghost, 1]
                vout[u, 0], vout[u, 1] = both
                if merged and level == half:
                    @pl.when(first_pair)
                    def _():
                        ghost = slot_of(GHOST, level)
                        for r in range(2):
                            vout[u, r] = vout[u, r] + pbuf[ghost, r]
        if kind == GHOST:
            if level > half:
                when(sends_ghost, lambda: ghost_out(level).start())
        elif kind == OWN0 and not raw and not (side == 0 and level > half and not relayed(level)):
            send(side, u)

    def send(side, u):
        leaving = own_sends(side, u)
        if leaving is not None:
            when(leaving[1], lambda: leaving[0].start())

    def corner_late(n):
        return remote(late_end.at[n], late_in.at[n], ds2, dr2.at[n], (north, west))

    def arrived(level, u=None):
        al, be, ga, de = [mixed[k, 0:1, :] for k in range(4)]
        if u is None:
            u, message, at = level, corner[...], level
        else:
            n, i = corners(lev)[level]
            corner_late(n - 1).wait_recv()
            message, at = jnp.concatenate(
                [late_in[n - 1], jnp.zeros((cols - 8, cols), jnp.float32)], axis=0).T[:spec], 4 * i
        row0, row1 = vin[u, 0], vin[u, 1]
        edge = message if at == 0 else pltpu.roll(message, cols - at, 1)
        right0 = after(jnp.where(lane == 0, edge, row0))
        return al * row0, be * row0 + ga * row1 + de * right0

    def gather(side, kind, level, i):
        u = slot_of(kind, level)
        if kind == GHOST:
            n = level - half
            with jax.named_scope("w_st"):
                when(None if n else first_pair, lambda: state_out(n).wait_recv())
            if n == 0:
                stiff_out.wait_recv()
            x, y, live = [vout[level, r] for r in range(2)], [st_in[n, r] for r in range(2)], gstiff[level]
        else:
            if side == 1:
                @pl.when(has_south)
                def _():
                    with jax.named_scope("w_vin"):
                        direct(u).wait_recv()
                    extra = kind == OWN0 and level > half
                    if extra:
                        with jax.named_scope("w_z"):
                            ghost_out(level).wait_recv()
                    adds = arrived(level) if kind == OWN1 else [vin[u, r] for r in range(2)]
                    for r in range(2):
                        both = adds[r] + zin[level - half, r] if extra else adds[r]
                        pbuf[u, r] = pbuf[u, r] + both
                x = [pbuf[u, r] for r in range(2)]
            elif kind == OWN0 or level < half:
                with jax.named_scope("w_vin"):
                    direct(u).wait_recv()
                if kind == OWN1:
                    adds = arrived(level)
                elif level < half:
                    adds = arrived(level, u)
                else:
                    adds = [vin[u, r] for r in range(2)]
                x = [pbuf[u, r] + adds[r] for r in range(2)]
            else:
                if level == half:
                    @pl.when(later_pair)
                    def _():
                        with jax.named_scope("w_vin"):
                            direct(u).wait_recv()
                        adds = arrived(level)
                        for r in range(2):
                            pbuf[u, r] = pbuf[u, r] + adds[r]
                x = [pbuf[u, r] for r in range(2)]
            tmp[i] = state[nwin - 1 if kind == OWN1 else 0, level].astype(jnp.float32)
            y, live = [tmp[i, pl.ds(r, spec, stride=2), :] for r in range(2)], stiff_ref[level]
        return (
            jnp.concatenate(x, axis=1), jnp.concatenate(y, axis=1),
            jnp.concatenate([live[0:1], live[1:2]], axis=1),
        )

    def chem(levels, gathered):
        flats, ys, lives = zip(*gathered)

        def dot(mat, xs):
            return [
                jnp.dot(a, x.astype(jnp.bfloat16), preferred_element_type=jnp.float32) for a, x in zip(mat, xs)]

        v1 = dot([mats[steps - 1, level] for level in levels], flats)
        for s in reversed(range(steps)):
            mat = [mats[s, level] for level in levels]
            v2 = dot(mat, [v * y for v, y in zip(v1, ys)])
            r2 = [v * y for v, y in zip(v2, ys)]
            v3 = dot(mat, r2)
            some = [0.4 * x + 0.3 * a + 0.2 * b for x, a, b in zip(flats, v1, v2)]
            if s:
                v1 = [
                    a + b for a, b in zip(
                        dot([mats[s - 1, level] for level in levels],
                            [jnp.where(live > s, x, flat) for x, flat, live in zip(some, flats, lives)]),
                        dot([both[s - 1, level] for level in levels],
                            [jnp.where(live > s, r, 0.0) for r, live in zip(r2, lives)]))]
            flats = [
                jnp.where(live > s, x + 0.1 * c, flat) for x, c, flat, live in zip(some, v3, flats, lives)
            ]
        return flats

    def spread(k):
        to = lax.rem(lon + k, n_lon)
        return remote(part.at[to], inbox1.at[k - 1], s1, r1, (lat, to))

    def spread_all():
        n = pl.ds(0, n_lon - 1)
        return remote(part.at[n], inbox1.at[n], s1, r1, (lat, west))

    def spread2(k):
        to = lax.rem(lat + k, n_lat)
        return remote(turn.at[to], inbox2.at[k - 1], s2, r2, (to, lon))

    def spread2_all():
        n = pl.ds(0, n_lat - 1)
        return remote(turn.at[n], inbox2.at[n], s2, r2, (north, lon))

    def regions():
        lat8 = part.shape[1]
        contrib = jnp.concatenate([
            em_ref[pl.ds(r, spec, stride=2), :]
            * (lamb[lev, r] + fin[:, r * cols:(r + 1) * cols])
            for r in range(2)], axis=1)
        where_from = jnp.concatenate([reg_ref[0:1, :], reg_ref[1:2, :]], axis=1)
        shape = (n_lon * lat8, 2 * cols)
        column = jnp.concatenate([jnp.full((lat8, 2 * cols), c, jnp.int32) for c in range(n_lon)], axis=0)
        band = lax.broadcasted_iota(jnp.int32, (lat8, 2 * cols), 0)
        band = jnp.concatenate([band] * n_lon, axis=0)
        onehot = (jnp.broadcast_to(where_from, shape) == band * n_lon + column).astype(jnp.float32)
        sums = lax.dot_general(
            onehot, contrib, (((1,), (1,)), ((), ())),
            precision=lax.Precision.HIGHEST, preferred_element_type=jnp.float32)
        for c in range(n_lon):
            part[c] = sums[c * lat8:(c + 1) * lat8]
        for k in range(1, n_lon):
            spread(k).start()

    def regions_turn():
        total = part[lon]
        spread_all().wait_recv()
        for k in range(n_lon - 1):
            total = total + inbox1[k]
        for b in range(n_lat):
            turn[b] = total[b:b + 1]
        for k in range(1, n_lat):
            spread2(k).start()

    def regions_end():
        total = turn[lat]
        spread2_all().wait_recv()
        for k in range(n_lat - 1):
            total = total + inbox2[k]
        grad_ref[...] = total

    def drain(side, sent):
        n = 1 + len(sent)
        remote(cout.at[pl.ds(0, n)], cin.at[pl.ds(0, n)], cs, cr.at[0], (lat, west)).wait_send()

        def left(n):
            remote(lamb.at[pl.ds(0, n)], vin.at[pl.ds(0, n)], vs, vr.at[0], (north, lon)).wait_send()

        if side == 1:
            left(lev + half)
            remote(late_end, late_in, ds2, dr2.at[0], (north, west)).wait_send()

            @pl.when(later_pair)
            def _():
                left(1)

            @pl.when(sends_ghost)
            def _():
                left(half - 1)
        else:
            @pl.when(has_north)
            def _():
                left(2 * lev)
            stiff_out.wait_send()
            mix_out.wait_send()
            n = pl.ds(0, half - 1)
            remote(st_out.at[n], st_in.at[n], ss, rr.at[0], (south, lon)).wait_send()
            when(first_pair, lambda: state_out(0).wait_send())
        rows_west.wait_send()

        @pl.when(has_north)
        def _():
            corner_out.wait_send()
            row_copies(len(rows_north), 1).wait_send()

        @pl.when(has_south)
        def _():
            row_copies(len(rows_out), 0).wait_send()

    def play(side):
        sent = {}
        for op in plans[side]:
            if op[0] == "chem":
                n, items = op[1:]
                gathered = [gather(side, kind, level, i) for i, (kind, level) in enumerate(items)]
                with jax.named_scope("chem"):
                    flats = chem([level for _, level in items], gathered)
                if n:
                    slots = []
                    for (kind, level), flat in zip(items, flats):
                        u = after_chem(kind, level)
                        for r in range(2):
                            lamb[u, r] = flat[:, r * cols:(r + 1) * cols]
                        slots.append((u, 1 if kind == GHOST else 0))
                        if side == 1 and kind == OWN1 and level < half:
                            send(side, u)
                    with jax.named_scope("pack"):
                        pack(n, slots)
                    col_copy(n).start()
                    if side == 1 and n in [m for m, _ in corners(lev).values()]:
                        late_end[n - 1] = jnp.concatenate(
                            [cout[n], jnp.zeros((cols - spec, cols), jnp.float32)], axis=0).T[:8]
                        corner_late(n - 1).start()
                    sent[n] = [(OWN0 if kind == OWN1 else GHOST, level) for kind, level in items]
                else:
                    for i, ((kind, level), flat) in enumerate(zip(items, flats)):
                        for r in range(2):
                            tmp[i, pl.ds(r, spec, stride=2), :] = flat[:, r * cols:(r + 1) * cols]
                        outbuf[level] = tmp[i].astype(jnp.bfloat16)
                        if level == 0:
                            fin[...] = flat
                            with jax.named_scope("regions"):
                                regions()
            elif op[0] == "send":
                for level in op[1]:
                    send(side, lev + level)
            elif op[0] == "first":
                for level in op[1]:
                    transport(side, 0, level, OWN1, level)
            elif op[0] == "move":
                n = op[1]
                with jax.named_scope("w_col"):
                    col_copy(n).wait_recv()
                if side == 1 and n == 3:
                    mix_out.wait_recv()
                for i, (kind, level) in enumerate(sent[n]):
                    transport(side, n, i, kind, level)
            elif op[0] == "relay":
                w, passed = op[1:]

                @pl.when(passes_on)
                def _(w=w, passed=passed):
                    for level in passed:
                        u = w * lev + level
                        with jax.named_scope("w_relay"):
                            to_relay(u).wait_recv()
                        forward(u).start()
            elif op[0] == "state":
                for k in range(op[1], op[2]):
                    give_state(k)
            elif op[0] == "drain":
                drain(side, sent)
            elif op[0] == "end":
                with jax.named_scope("reg_end"):
                    regions_end()
                spread_all().wait_send()
                spread2_all().wait_send()
            else:
                with jax.named_scope("turn"):
                    regions_turn()

        if side == 0:
            @pl.when(passes_on)
            def _():
                remote(relay, relay, fs, rr.at[0], (south, lon)).wait_send()

    for load in small[:2]:
        load.wait()
    for r in range(2):
        clon, clat = clon_ref[r:r + 1, :], clat_ref[r:r + 1, :]
        coef[0, 3 * r] = jnp.broadcast_to(1.0 - clon - clat, (8, cols))
        if r == 0:
            coef[0, 1] = jnp.broadcast_to(clat, (8, cols))
        coef[0, 2 + 2 * r] = jnp.broadcast_to(clon, (8, cols))

    adj_load.wait()
    small[2].wait()
    for level in range(lev):
        tmp[level % 4] = adj[level].astype(jnp.float32)
        for r in range(2):
            lamb[level, r] = tmp[level % 4, pl.ds(r, spec, stride=2), :]
    with jax.named_scope("pack"):
        pack(0, [(level, 0) for level in range(lev)])
        corner_all[...] = jnp.concatenate(
            [cout[0], jnp.zeros((cols - spec, cols), jnp.float32)], axis=0).T[:4 * lev]
        corner_end[...] = corner_all[pl.ds(0, lev, stride=4), :]
    with jax.named_scope("w_barrier"):
        pl.semaphore_wait(
            barrier, n_lon - 1 + n_lat - 1 + 2 * has_north.astype(jnp.int32) + 2 * has_south.astype(jnp.int32))

    @pl.when(has_south)
    def _():
        for copy in rows_out:
            copy.start()

    @pl.when(has_north)
    def _():
        for copy in rows_north:
            copy.start()
    rows_west.start()

    @pl.when(even)
    def _():
        stiff_out.start()
        when(has_north, lambda: corner_out.start())
        send(0, 0)
        send(0, 2)

    @pl.when(odd)
    def _():
        corner_out.start()
        send(1, 0)
    col_copy(0).start()

    def give_state(n, condition=None):
        def do():
            tmp[n % 4] = state[nwin - 1, half + n].astype(jnp.float32)
            for r in range(2):
                st_out[n, r] = tmp[n % 4, pl.ds(r, spec, stride=2), :]
            state_out(n).start()

        when(condition, do)

    state_loads[nwin - 1].wait()

    @pl.when(even)
    def _():
        for level in range(1, half):
            if level != 2:
                send(0, level)
        give_state(0, first_pair)
        give_state(1, first_pair)
        send(0, half)
        for level in range(half, lev):
            if relayed(level):
                send(0, level)

    @pl.when(odd)
    def _():
        for level in range(1, half + 1):
            send(1, level)

    inv_load.wait()
    with jax.named_scope("mats"):
        for s in range(steps):
            tall[...] = inv[s].astype(jnp.float32)
            for level in range(lev):
                mats[s, level] = tall[pl.ds(level, spec, stride=lev), :].T.astype(jnp.bfloat16)
    with jax.named_scope("both"):
        for s in range(1, steps):
            for level in range(lev):
                both[s - 1, level] = (0.1 * jnp.dot(
                    mats[s - 1, level], mats[s, level], preferred_element_type=jnp.float32)).astype(jnp.bfloat16)
    for load in small[3:]:
        load.wait()
    for w in range(nwin - 1):
        state_loads[w].wait()
    first_lane = lax.broadcasted_iota(jnp.int32, (8, cols), 1) == 0

    def beside(row, next_row):
        row, next_row = jnp.broadcast_to(row, (8, cols)), jnp.broadcast_to(next_row, (8, cols))
        return after(jnp.where(first_lane, next_row, row))

    @pl.when(has_north)
    def _():
        row_copies(len(rows_out), 0).wait_recv()
        c0, o0, n0 = coef[0, 0], coef[0, 2], coef[0, 1]
        for r in range(2):
            clon, clat = nclon[r:r + 1, :], nclat[r:r + 1, :]
            coef[1, 3 * r] = jnp.broadcast_to(1.0 - clon - clat, (8, cols))
            if r == 0:
                coef[1, 1] = jnp.broadcast_to(clat, (8, cols))
            coef[1, 2 + 2 * r] = jnp.broadcast_to(clon, (8, cols))
        below = jnp.broadcast_to(nclat[1:2, :], (8, cols))
        coef[0, 5] = coef[1, 1] * below
        coef[0, 6] = below * (coef[1, 3] + c0)
        coef[0, 7] = below * n0
        coef[0, 8] = below * o0 + coef[1, 4] * beside(nclat[1:2, :], neclat[1:2, :])

    @pl.when(jnp.logical_not(has_north))
    def _():
        for k in range(5, 9):
            coef[0, k] = jnp.zeros((8, cols), jnp.float32)

    rows_west.wait_recv()

    @pl.when(has_south)
    def _():
        row_copies(len(rows_north), 1).wait_recv()
        clon, clat = sclon[0:1, :], sclat[0:1, :]
        below = jnp.broadcast_to(clat_ref[1:2, :], (8, cols))
        mixed[0] = coef[0, 1] * below
        mixed[1] = below * (coef[0, 3] + jnp.broadcast_to(1.0 - clon - clat, (8, cols)))
        mixed[2] = below * jnp.broadcast_to(clat, (8, cols))
        mixed[3] = below * jnp.broadcast_to(clon, (8, cols)) + coef[0, 4] * beside(clat_ref[1:2, :], eclat[1:2, :])

    @pl.when(even)
    def _():
        mix_out.start()
        give_state(1, later_pair)
        for level in range(half + 1, lev):
            if not relayed(level):
                send(0, level)

    @pl.when(has_south)
    def _():
        with jax.named_scope("w_corner"):
            corner_out.wait_recv()
        corner[...] = jnp.concatenate(
            [corner_in[...], jnp.zeros((cols - lev, cols), jnp.float32)], axis=0).T[:spec]

    with jax.named_scope("w_col"):
        col_copy(0).wait_recv()

    @pl.when(even)
    def _():
        play(0)

    @pl.when(odd)
    def _():
        play(1)


def finish(held_ref, grad_ref, out_hbm, grad_hbm, sems):
    copies = [
        pltpu.make_async_copy(held_ref, out_hbm, sems.at[0]),
        pltpu.make_async_copy(grad_ref, grad_hbm, sems.at[1]),
    ]
    for copy in copies:
        copy.start()
    for copy in copies:
        copy.wait()


def solution(mesh):
    n_lat, n_lon = mesh.shape["lat"], mesh.shape["lon"]
    assert n_lat % 2 == 0

    def per_device(adjoint_in, state, inverses, courant_lon, courant_lat, emission, region_id, stiffness):
        lev, spec, rows, cols = adjoint_in.shape
        nwin, steps = state.shape[0], inverses.shape[0]
        assert nwin == 2 and rows == 2
        half = lev // 2
        slots = nwin * lev + half
        passed = sum(relayed(level, w) for level in range(lev) for w in range(nwin))
        lat8 = -(-n_lat // 8) * 8
        f32, bf16 = jnp.float32, jnp.bfloat16
        any_space = pl.BlockSpec(memory_space=pl.ANY)
        vmem = pl.BlockSpec(memory_space=pltpu.VMEM)
        dma = pltpu.SemaphoreType.DMA

        def blocks(n):
            return pltpu.VMEM((n, rows, spec, cols), f32)

        out, grad = pl.pallas_call(
            functools.partial(kernel, n_lat, n_lon),
            out_shape=(
                pltpu.VMEM((lev, rows * spec, cols), bf16),
                pltpu.VMEM((1, spec), f32),
            ),
            in_specs=[any_space] * 8,
            out_specs=(vmem, vmem),
            scratch_shapes=[
                pltpu.VMEM((lev, rows * spec, cols), bf16),
                pltpu.VMEM((nwin, lev, rows * spec, cols), bf16),
                pltpu.VMEM((steps, spec * lev, spec), bf16),
                pltpu.VMEM(courant_lon.shape, f32),
                pltpu.VMEM(courant_lat.shape, f32),
                pltpu.VMEM((spec * rows, cols), f32),
                pltpu.VMEM(region_id.shape, jnp.int32),
                pltpu.VMEM(stiffness.shape, jnp.int32),
                pltpu.VMEM((spec * lev, spec), f32),
                pltpu.VMEM(inverses.shape, bf16),
                pltpu.VMEM((steps - 1,) + inverses.shape[1:], bf16),
                blocks(slots), blocks(slots), blocks(slots),
                blocks(nwin * lev), blocks(passed), blocks(half), blocks(half), blocks(half),
                pltpu.VMEM((messages(lev), spec, cols), f32),
                pltpu.VMEM((messages(lev), spec, cols), f32),
                pltpu.VMEM(courant_lon.shape, f32),
                pltpu.VMEM(courant_lat.shape, f32),
                pltpu.VMEM(courant_lat.shape, f32),
                pltpu.VMEM(courant_lon.shape, f32),
                pltpu.VMEM(courant_lat.shape, f32),
                pltpu.VMEM(courant_lat.shape, f32),
                pltpu.VMEM(stiffness.shape, jnp.int32),
                pltpu.VMEM((4 * lev, cols), f32),
                pltpu.VMEM((half, 8, cols), f32),
                pltpu.VMEM((half, 8, cols), f32),
                pltpu.VMEM((lev, cols), f32),
                pltpu.VMEM((lev, cols), f32),
                pltpu.VMEM((spec, cols), f32),
                pltpu.VMEM((4, rows * spec, cols), f32),
                pltpu.VMEM((spec, rows * cols), f32),
                pltpu.VMEM((2, 9, 8, cols), f32),
                pltpu.VMEM((4, 8, cols), f32),
                pltpu.VMEM((n_lon, lat8, spec), f32),
                pltpu.VMEM((n_lon, lat8, spec), f32),
                pltpu.VMEM((n_lat, 1, spec), f32),
                pltpu.VMEM((n_lat, 1, spec), f32),
                dma, dma((nwin,)), dma, dma((5,)),
                dma, dma((nwin * lev,)), dma((max(passed, 2 * half),)), dma,
                dma,
                dma, dma((messages(lev),)), dma((3,)), dma((5,)), dma, dma, dma, dma((half,)),
                dma, dma, dma, dma,
            ],
            compiler_params=pltpu.CompilerParams(collective_id=0, has_side_effects=True),
        )(
            adjoint_in.reshape(lev, spec * rows, cols),
            state.reshape(nwin, lev, spec * rows, cols),
            inverses.transpose(0, 2, 1, 3).reshape(steps, spec * lev, spec), courant_lon, courant_lat,
            emission.reshape(spec * rows, cols), region_id, stiffness,
        )
        out, grad = pl.pallas_call(
            finish,
            out_shape=(
                jax.ShapeDtypeStruct(out.shape, bf16),
                jax.ShapeDtypeStruct(grad.shape, f32),
            ),
            in_specs=[any_space] * 2,
            out_specs=(any_space, any_space),
            scratch_shapes=[dma((2,))],
        )(*(pltpu.with_memory_space_constraint(x, pltpu.VMEM) for x in (out, grad)))
        return out.reshape(adjoint_in.shape), grad

    in_specs = (
        P(None, None, "lat", "lon"),
        P(None, None, None, "lat", "lon"),
        P(),
        P("lat", "lon"),
        P("lat", "lon"),
        P(None, "lat", "lon"),
        P("lat", "lon"),
        P(None, "lat", "lon"),
    )
    out_specs = (P(None, None, "lat", "lon"), P(("lat", "lon"), None))
    return jax.shard_map(
        per_device, mesh=mesh, in_specs=in_specs, out_specs=out_specs, check_vma=False
    )
```
